32 devices in a mesh: replica: 8 (over z, x), shard: 4 (over y, core).
Axes of the slice: x: 2, y: 2, z: 4, core: 2. Of those that a mesh axis runs over, the one named last changes fastest.
Arguments:
- deltas: bfloat16 [8, 2048, 8192], P('replica', 'shard')
- master: float32 [2048, 8192], P('shard', 'replica'), may hold values from -6 to 6
- momentum: float32 [2048, 8192], P('shard', 'replica'), may hold values from -6 to 6
- block_owner: int32 [8, 1], replicated, may hold values from 0 to 3; in each aligned block of 8 rows (0 to 7, 8 to 15, ...) at most 4 rows name the same one
Outputs:
- master_out: float32 [2048, 8192], P('shard', 'replica')
- momentum_out: float32 [2048, 8192], P('shard', 'replica')
- params: bfloat16 [1024, 8192], P(None, 'replica')
The draws below stay inside these ranges and needn't reach their ends.
Inputs may be any that keep to these rules, and one draw needn't show every extreme that they name: `block_owner`: every shard owns at least one block and at most 4; some shard owns exactly 4. Rows of slots that are not live hold arbitrary deltas.
All inputs are finite; a program needn't handle non-finite values.
Results may differ from the reference program's by a relative error of at most 0.01.
Values may be sent and summed in bfloat16 or wider, within the bound.
A program may use at most 128 MiB of HBM per device.

```python
import math
import jax
import jax.numpy as jnp
import numpy as np
from jax import lax

D = 8192
BLOCK_ROWS = 128
SLOTS = 4
BLOCKS = 8
N_REPLICA = 8
N_SHARD = 4


def draw_deltas(key, part):
    rows = N_SHARD * SLOTS * BLOCK_ROWS
    base = jax.random.normal(key, (N_REPLICA, rows, D), jnp.float32)
    ramp = jnp.exp(jnp.log(3.0) * jnp.arange(rows, dtype=jnp.float32) / max(rows - 1, 1))
    rising = jnp.exp(jnp.log(3.0) * jnp.arange(N_REPLICA, dtype=jnp.float32) / max(N_REPLICA - 1, 1))
    column_ramp = jnp.exp(jnp.log(3.0) * jnp.arange(D, dtype=jnp.float32) / max(D - 1, 1))
    values = base * column_ramp[None, None, :]
    return (4.0 * values * ramp[None, :, None] * rising[:, None, None]).astype(jnp.bfloat16)


def levels(key, shape, cuts, smallest, largest):
    level, own = 1.0, jax.random.fold_in(key, 6)
    for dim, blocks in cuts:
        draws = jnp.exp(jax.random.uniform(jax.random.fold_in(own, dim), (blocks,), jnp.float32, smallest / len(cuts), largest / len(cuts)))
        level = level * jnp.repeat(draws, shape[dim] // blocks).reshape([-1 if axis == dim else 1 for axis in range(len(shape))])
    return level


def shared_out(own_key, own, number, rows, count, top, reach, slope):
    sequence = jax.random.permutation(own_key, count)
    packed, usual = load_shares(count, rows * top, reach, slope, True), load_shares(count, rows * top, reach, slope, False)
    places = jnp.arange(count)

    def named(lengths, offset_by):
        used = int((lengths > 0).sum())
        fixed = max(1, used // 4)
        moved = fixed + (places - fixed + offset_by * (used - fixed)) % max(1, count - fixed)
        return jnp.zeros((count,), jnp.int32).at[sequence[jnp.where(places < fixed, places, moved)]].set(jnp.asarray(lengths, jnp.int32))

    lengths = jnp.where(number % 4 == 0, named(packed, number // 4), named(usual, number - number // 4 - 1))
    mixed = jax.random.permutation(jax.random.fold_in(own, 3), count)
    giver, sink = mixed[0:count // 2 * 2:2], mixed[1:count // 2 * 2:2]
    slack = jnp.minimum(lengths[giver] - 1, reach - lengths[sink]) // 2
    slack = jnp.where((giver == sequence[0]) | (sink == sequence[0]) | (lengths[sink] == 0), 0, jnp.maximum(slack, 0))
    moved = jax.random.randint(jax.random.fold_in(own, 4), (count // 2,), 0, 1 << 20) % (slack + 1)
    lengths = lengths.at[giver].add(-moved).at[sink].add(moved)
    items = jnp.searchsorted(jnp.cumsum(lengths), jnp.arange(rows * top), side="right").astype(jnp.int32)
    table = items.reshape(top, rows).T
    table = table[jax.random.permutation(jax.random.fold_in(own, 1), rows)]
    offset_by = jax.random.randint(jax.random.fold_in(own, 2), (rows, 1), 0, top)
    return jnp.take_along_axis(table, (jnp.arange(top)[None, :] + offset_by) % top, axis=1)


def load_shares(number_of, total, reach, skew, full):
    loads = [(1 << 20) // math.isqrt(grade ** skew) + 1 for grade in range(1, number_of + 1)]
    largest = reach if full else min(reach, max(-(-total // number_of), total * loads[0] // sum(loads)))
    least = 1 if total - largest >= number_of - 1 else 0
    given, spare = [largest] + [least] * (number_of - 1), total - largest - least * (number_of - 1)
    while spare > 0:
        candidates = [i for i in range(1, number_of) if given[i] < largest] or [i for i in range(1, number_of) if given[i] < reach]
        whole, left = sum([loads[i] for i in candidates]), spare
        for i in candidates:
            more = min(reach - given[i], max(1, left * loads[i] // whole), spare)
            given[i] = given[i] + more
            spare = spare - more
    return np.array(given)


def normal_values(key, extent, deviation, most, cuts=(), held_as=jnp.bfloat16):
    gain = levels(key, extent, cuts, -0.22, 0.18) if cuts else 1.0
    result = jax.random.normal(key, extent, jnp.float32) * deviation * gain
    return jnp.minimum(jnp.maximum(result, -most), most).astype(held_as)


def setup_inputs(seed: int = 0) -> dict:
    arg_keys = jax.random.split(jax.random.key(seed), 5)
    deltas = draw_deltas(jax.random.fold_in(arg_keys[4], 71), 0)
    master = normal_values(arg_keys[1], (N_SHARD * SLOTS * BLOCK_ROWS, D), 1.0, 6.0, ((0, 4), (1, 8)), jnp.float32)
    momentum = normal_values(arg_keys[2], (N_SHARD * SLOTS * BLOCK_ROWS, D), 1.0, 6.0, ((0, 4), (1, 8)), jnp.float32)
    block_owner_keys = jax.random.split(jax.random.fold_in(arg_keys[3], 1), BLOCKS // BLOCKS)
    block_owner_turns = jax.random.permutation(jax.random.fold_in(arg_keys[3], 3), BLOCKS // BLOCKS)
    block_owner = jax.vmap(lambda own, number: shared_out(jax.random.fold_in(arg_keys[3], 2), own, number, BLOCKS, N_SHARD, 1, SLOTS, 2))(block_owner_keys, block_owner_turns).reshape((BLOCKS, 1))
    return dict(deltas=deltas, master=master, momentum=momentum, block_owner=block_owner)


def reference(deltas, master, momentum, block_owner):
    owner = block_owner[:, 0]
    shard_ids = jnp.arange(N_SHARD, dtype=jnp.int32)
    counts = lax.optimization_barrier(jnp.sum((owner[None, :] == shard_ids[:, None]).astype(jnp.int32), axis=1))
    live = jnp.arange(SLOTS, dtype=jnp.int32)[None, :] < counts[:, None]
    live_rows = jnp.repeat(live.reshape(-1), BLOCK_ROWS)[:, None]

    def add_one(total, piece):
        return (total + piece.astype(jnp.float32), None)
    summed, _ = lax.scan(add_one, jnp.zeros(master.shape, jnp.float32), deltas)
    avg = jnp.where(live_rows, summed / N_REPLICA, jnp.float32(0.0))
    total = jnp.sum(avg * avg)
    limit = 0.5 * jnp.sqrt(jnp.float32(BLOCKS * BLOCK_ROWS * D))
    factor = jnp.minimum(jnp.float32(1.0), limit / (jnp.sqrt(total) + 1e-06))
    grad = factor * avg
    momentum_out = jnp.where(live_rows, 0.9 * momentum + grad, momentum)
    master_out = jnp.where(live_rows, master - 0.7 * (grad + 0.9 * momentum_out), master)
    index = jnp.arange(BLOCKS, dtype=jnp.int32)
    same = (owner[None, :] == owner[:, None]) & (index[None, :] < index[:, None])
    before = lax.optimization_barrier(jnp.sum(same.astype(jnp.int32), axis=1))
    flat = (owner * SLOTS + before).astype(jnp.int32)
    blocks = master_out.reshape(N_SHARD * SLOTS, BLOCK_ROWS, D)[flat]
    params = blocks.astype(jnp.bfloat16).reshape(BLOCKS * BLOCK_ROWS, D)
    return (master_out, momentum_out, params)
```

```python
import functools

import jax
import jax.numpy as jnp
from jax import lax
from jax.experimental import pallas as pl
from jax.experimental.pallas import tpu as pltpu
from jax.sharding import PartitionSpec as P

BLOCK_ROWS = 128
SLOTS = 4
F32 = jnp.float32
BF16 = jnp.bfloat16
VMEM_LIMIT = 56 * 1024 * 1024


def remote(src, dst, send, recv, device):
    return pltpu.make_async_remote_copy(
        src_ref=src, dst_ref=dst, send_sem=send, recv_sem=recv,
        device_id=device, device_id_type=pl.DeviceIdType.MESH,
    )


def shard_count(owner, shard):
    return sum(jnp.where(owner[0, b] == shard, 1, 0) for b in range(owner.shape[1]))


def spread(condition, shape):
    return jnp.broadcast_to(jnp.where(condition, 1, 0), shape) != 0


def sync_kernel(
    R, S, rows, rc,
    owner, deltas, master, momentum,
    sums, bases, tot,
    dv, p3, yt, ms, mm, base, xin, pair, zin, mine, norm, nbuf, sbuf,
    ld, lm, p3_s, p3_r, t_s, t_r, x_s, x_r, z_s, z_r, l_s, c_s, c_r, y_s, y_r, f_s, f_r,
    bl_s, bc_s, bc_r, by_s, by_r, bf_s, bf_r, n_s, n_r, m_s, m_r,
):
    width = deltas.shape[2]
    cols = width // R
    Z, O = R // 2, S // 2
    per = BLOCK_ROWS // rc
    half = BLOCK_ROWS // 2
    chunks = rows // rc
    quad = rows < SLOTS * BLOCK_ROWS
    whole = rows // BLOCK_ROWS
    direct = whole * per
    top = whole * BLOCK_ROWS
    me_r, me_s = lax.axis_index("replica"), lax.axis_index("shard")
    z, x = me_r // 2, me_r % 2
    o, core = me_s // 2, me_s % 2
    x_peer = z * 2 + 1 - x
    twin = o * 2 + 1 - core

    barrier = pltpu.get_barrier_semaphore()
    for i in range(1, R):
        pl.semaphore_signal(barrier, inc=1, device_id=((me_r + i) % R, me_s), device_id_type=pl.DeviceIdType.MESH)
    for i in range(1, S):
        pl.semaphore_signal(barrier, inc=1, device_id=(me_r, (me_s + i) % S), device_id_type=pl.DeviceIdType.MESH)

    def load(k):
        part = pl.ds(k * BLOCK_ROWS, BLOCK_ROWS)
        return pltpu.make_async_copy(deltas.at[0, part, :], dv.at[part, :], ld.at[k])

    if quad:
        load(whole).start()
    for k in range(whole):
        load(k).start()
    load_master = pltpu.make_async_copy(master, ms, lm.at[0])
    load_momentum = pltpu.make_async_copy(momentum, mm, lm.at[1])
    load_master.start()
    load_momentum.start()
    mine_count = jnp.sum(jnp.where(owner[...] == me_s, 1, 0), axis=1, keepdims=True)
    twin_count = jnp.sum(jnp.where(owner[...] == twin, 1, 0), axis=1, keepdims=True)
    heavy = jnp.maximum(mine_count, twin_count) >= SLOTS
    pl.semaphore_wait(barrier, R + S - 2)

    def rows_of(c):
        return pl.ds(pl.multiple_of(c * rc, rc), rc)

    def columns(c, j, side):
        return pl.ds(pl.multiple_of((((z + 1 + j) % Z) * 2 + side) * cols, cols), cols)

    def x_copy(source, c, j):
        return remote(
            source.at[rows_of(c), columns(c, j, 1 - x)], xin.at[c, j], x_s.at[c, j], x_r.at[c, j], (x_peer, me_s)
        )

    def z_copy(c, j):
        return remote(
            pair.at[c, j], zin.at[c, j], z_s.at[c, j], z_r.at[c, j], (((z + 1 + j) % Z) * 2 + x, me_s)
        )

    def c_copy(c):
        return remote(mine.at[c], sums.at[me_s, c], c_s.at[c], c_r.at[c], (me_r, twin))

    def l_copy(c):
        return pltpu.make_async_copy(mine.at[c], sums.at[me_s, c], l_s.at[c])

    def y_copy(i, c):
        return remote(
            mine.at[c], sums.at[me_s, c], y_s.at[i - 1, c], y_r.at[i - 1, c], (me_r, ((o + i) % O) * 2 + core)
        )

    def f_copy(i, c):
        source = ((o + O - i) % O) * 2 + core
        return remote(sums.at[source, c], sums.at[source, c], f_s.at[i - 1, c], f_r.at[i - 1, c], (me_r, twin))

    def by_copy(i):
        return remote(base, bases.at[me_s], by_s.at[i - 1], by_r.at[i - 1], (me_r, ((o + i) % O) * 2 + core))

    def bf_copy(i):
        source = ((o + O - i) % O) * 2 + core
        return remote(bases.at[source], bases.at[source], bf_s.at[i - 1], bf_r.at[i - 1], (me_r, twin))

    def third_copy(h):
        return remote(
            deltas.at[0, pl.ds((SLOTS - 1) * BLOCK_ROWS + h * half, half), :],
            p3.at[pl.ds(h * half, half), :], p3_s.at[h], p3_r.at[h], (me_r, twin),
        )

    def t_copy():
        return remote(dv.at[pl.ds(top + half, half), :], yt, t_s, t_r, (me_r, ((o + 1) % O) * 2 + core))

    def base_twin():
        return remote(base, bases.at[me_s], bc_s, bc_r, (me_r, twin))

    def base_local():
        return pltpu.make_async_copy(base, bases.at[me_s], bl_s)

    def start_x(source, low, high):
        @pl.loop(low, high)
        def _(c):
            for j in range(Z):
                x_copy(source, c, j).start()

    def pick(condition, other, start, other_start):
        @pl.loop(0, half // 16)
        def _(r):
            keep = spread(condition, (16, 1024))
            for q in range(width // 1024):
                at = (pl.ds(pl.multiple_of(start + r * 16, 16), 16), pl.ds(q * 1024, 1024))
                there = (pl.ds(pl.multiple_of(other_start + r * 16, 16), 16), pl.ds(q * 1024, 1024))
                dv[at] = jnp.where(keep, dv[at].astype(F32), other[there].astype(F32)).astype(BF16)

    if quad:
        third_copy(1).start()
        third_copy(0).start()
    start_x(deltas.at[0], 0, direct)
    norm[0] = jnp.zeros((8, 128), F32)

    def send_third():
        load(whole).wait()
        third_copy(1).wait_recv()
        pick(mine_count >= SLOTS, p3, top + half, half)
        t_copy().start()

    def make_base():
        load_master.wait()
        load_momentum.wait()

        @pl.loop(0, SLOTS * BLOCK_ROWS // 16)
        def _(r):
            at = pl.ds(pl.multiple_of(r * 16, 16), 16)
            base[at, :] = (ms[at, :] - 0.567 * mm[at, :]).astype(BF16)

        for i in range(1, O):
            by_copy(i).start()
        base_twin().start()
        base_local().start()

    def add_pair(c):
        @pl.when(c % per == 0)
        def _():
            @pl.when(c < direct)
            def _():
                load(c // per).wait()

        for j in range(Z):
            x_copy(deltas.at[0], c, j).wait_recv()
            pair[c, j] = (xin[c, j].astype(F32) + dv[rows_of(c), columns(c, j, x)].astype(F32)).astype(BF16)
            if j < Z - 1:
                z_copy(c, j).start()

    def add_line(c):
        for j in range(Z - 1):
            z_copy(c, j).wait_recv()
        place = jnp.where(c >= direct, -1, c // per) if quad else c // per
        live = spread(place < mine_count, (8, 128))
        part = jnp.zeros((8, 128), F32)
        for r in range(0, rc, 16):
            total = pair[c, Z - 1, r:r + 16, :].astype(F32)
            for j in range(Z - 1):
                total = total + zin[c, j, r:r + 16, :].astype(F32)
            total = total / R
            mine[c, r:r + 16, :] = total.astype(BF16)
            for h in range(0, 16, 8):
                for q in range(0, cols, 128):
                    v = total[h:h + 8, q:q + 128]
                    part = part + v * v
        norm[0] = norm[0] + jnp.where(live, part, 0.0)
        for i in range(1, O):
            y_copy(i, c).start()
        c_copy(c).start()
        l_copy(c).start()

    def forward(c):
        for i in range(1, O):
            y_copy(i, c).wait_recv()
            f_copy(i, c).start()

    lag = 4

    @pl.loop(0, chunks + lag)
    def _(t):
        @pl.when(t < chunks)
        def _():
            add_pair(t)

        @pl.when(t >= lag)
        def _():
            add_line(t - lag)

        @pl.when(t == 2)
        def _():
            make_base()

        if quad:
            @pl.when(t == 0)
            def _():
                send_third()

            @pl.when(t == direct - direct // 4)
            def _():
                third_copy(0).wait_recv()
                pick(mine_count >= SLOTS, p3, top, 0)
                t_copy().wait_recv()
                pick(heavy, yt, top, 0)
                start_x(dv, direct, chunks)

    def n_copy(i):
        return remote(norm.at[0], nbuf.at[i - 1], n_s.at[i - 1], n_r.at[i - 1], ((me_r + i) % R, me_s))

    def m_copy(i):
        return remote(norm.at[1], sbuf.at[i - 1], m_s.at[i - 1], m_r.at[i - 1], (me_r, (me_s + i) % S))

    for i in range(1, R):
        n_copy(i).start()
    for i in range(1, O):
        by_copy(i).wait_recv()
        bf_copy(i).start()

    @pl.loop(0, chunks - 2)
    def _(c):
        forward(c)
        for j in range(Z):
            x_copy(deltas.at[0], c, j).wait_send()
        for j in range(Z - 1):
            z_copy(c, j).wait_send()

    total = norm[0]
    for i in range(1, R):
        n_copy(i).wait_recv()
        total = total + nbuf[i - 1]
    norm[1] = total
    for i in range(1, S):
        m_copy(i).start()

    @pl.loop(chunks - 2, chunks)
    def _(c):
        forward(c)

    for i in range(1, S):
        m_copy(i).wait_recv()
        total = total + sbuf[i - 1]
    tot[...] = total

    if quad:
        third_copy(0).wait_send()
        third_copy(1).wait_send()
        t_copy().wait_send()
    base_local().wait()
    base_twin().wait()
    for i in range(1, O):
        by_copy(i).wait_send()
        bf_copy(i).wait()
    for i in range(1, R):
        n_copy(i).wait_send()
    for i in range(1, S):
        m_copy(i).wait_send()

    @pl.loop(chunks - 2, chunks)
    def _(c):
        for j in range(Z):
            x_copy(deltas.at[0], c, j).wait_send()
        for j in range(Z - 1):
            z_copy(c, j).wait_send()

    @pl.loop(0, chunks)
    def _(c):
        l_copy(c).wait()
        c_copy(c).wait()
        for i in range(1, O):
            y_copy(i, c).wait_send()
            f_copy(i, c).wait()


def finish_kernel(
    R, units,
    owner_in, tot, master, momentum, sums, bases,
    master_out, momentum_out, params,
    owner, owner_s, ms, mm, su, pb, ps,
    a_s, b_s, u_s, p_s, q_s, oa_s, ob_s, op_s,
):
    blocks = owner.shape[1]
    cols = master.shape[1]
    half = BLOCK_ROWS // 2
    me_s = lax.axis_index("shard")
    get_owner = pltpu.make_async_copy(owner_in, owner, owner_s)
    get_owner.start()

    def unit(shard, place, h):
        if units == 2 * SLOTS:
            return shard * units + 2 * place + h
        moved = shard + jnp.where(place == SLOTS - 1, 1 - 2 * (shard % 2), 0)
        if h:
            moved = moved + jnp.where(moved // 2 == 0, 2, -2)
        return jnp.where(place < 2, shard * units + 2 * place + h, moved * units + units - 1)

    def slot_rows(j):
        return pl.ds(pl.multiple_of(j * BLOCK_ROWS, BLOCK_ROWS), BLOCK_ROWS)

    def get_slot(j):
        return [
            pltpu.make_async_copy(master.at[slot_rows(j)], ms.at[slot_rows(j)], a_s.at[j]),
            pltpu.make_async_copy(momentum.at[slot_rows(j)], mm.at[slot_rows(j)], b_s.at[j]),
        ] + [
            pltpu.make_async_copy(sums.at[unit(me_s, j, h)], su.at[2 * j + h], u_s.at[2 * j + h]) for h in range(2)
        ]

    def put_slot(j):
        return [
            pltpu.make_async_copy(ms.at[slot_rows(j)], master_out.at[slot_rows(j)], oa_s.at[j]),
            pltpu.make_async_copy(mm.at[slot_rows(j)], momentum_out.at[slot_rows(j)], ob_s.at[j]),
        ]

    def get_block(b):
        shard = owner[0, b]
        place = sum(jnp.where(jnp.logical_and(owner[0, k] == shard, k < b), 1, 0) for k in range(blocks))
        return [pltpu.make_async_copy(bases.at[shard * SLOTS + place], pb.at[b], p_s.at[b])] + [
            pltpu.make_async_copy(sums.at[unit(shard, place, h)], ps.at[2 * b + h], q_s.at[2 * b + h])
            for h in range(2)
        ]

    def put_block(b):
        return pltpu.make_async_copy(pb.at[b], params.at[slot_rows(b)], op_s.at[b])

    @pl.loop(0, SLOTS)
    def _(j):
        for copy in get_slot(j):
            copy.start()

    get_owner.wait()
    count = shard_count(owner, me_s)

    @pl.loop(0, blocks)
    def _(b):
        for copy in get_block(b):
            copy.start()

    total = jnp.sum(jnp.sum(tot[...], axis=1, keepdims=True), axis=0, keepdims=True)
    limit = 0.5 * jnp.sqrt(jnp.full((1, 1), blocks * BLOCK_ROWS * R * cols, F32))
    factor = jnp.minimum(1.0, limit / (jnp.sqrt(total) + 1e-06))

    @pl.loop(0, SLOTS)
    def _(j):
        for copy in get_slot(j):
            copy.wait()

        @pl.when(j < count)
        def _():
            for h in range(2):
                @pl.loop(0, half // 16)
                def _(r):
                    at = pl.ds(pl.multiple_of(j * BLOCK_ROWS + h * half + r * 16, 16), 16)
                    grad = factor * su[2 * j + h, pl.ds(pl.multiple_of(r * 16, 16), 16), :].astype(F32)
                    fresh = 0.9 * mm[at, :] + grad
                    mm[at, :] = fresh
                    ms[at, :] = ms[at, :] - 0.7 * (grad + 0.9 * fresh)

        for copy in put_slot(j):
            copy.start()

    @pl.loop(0, blocks)
    def _(b):
        for copy in get_block(b):
            copy.wait()
        for h in range(2):
            @pl.loop(0, half // 16)
            def _(r):
                at = pl.ds(pl.multiple_of(h * half + r * 16, 16), 16)
                grad = factor * ps[2 * b + h, pl.ds(pl.multiple_of(r * 16, 16), 16), :].astype(F32)
                pb[b, at, :] = (pb[b, at, :].astype(F32) - 1.33 * grad).astype(BF16)

        put_block(b).start()

    @pl.loop(0, SLOTS)
    def _(j):
        for copy in put_slot(j):
            copy.wait()

    @pl.loop(0, blocks)
    def _(b):
        put_block(b).wait()


def on_device(deltas, master, momentum, block_owner):
    R, S = lax.axis_size("replica"), lax.axis_size("shard")
    width, cols = deltas.shape[2], master.shape[1]
    blocks = block_owner.shape[0]
    block_owner = block_owner.reshape(1, blocks)
    half = BLOCK_ROWS // 2
    quad = S == 4 and blocks - SLOTS - (S - 2) <= 2
    rows = 2 * BLOCK_ROWS + half if quad else SLOTS * BLOCK_ROWS
    rc = half
    while rc > 16 and (rows // (rc // 2)) * R <= 160:
        rc //= 2
    chunks = rows // rc
    units = rows // half
    Z, O = R // 2, S // 2
    loads = rows // BLOCK_ROWS + (1 if quad else 0)

    dma = pltpu.SemaphoreType.DMA
    vmem = pltpu.VMEM
    anywhere = pl.BlockSpec(memory_space=pl.ANY)
    in_vmem = pl.BlockSpec(memory_space=pltpu.VMEM)
    in_smem = pl.BlockSpec(memory_space=pltpu.SMEM)
    ys, zs = max(O - 1, 1), max(Z - 1, 1)
    sums, bases, tot = pl.pallas_call(
        functools.partial(sync_kernel, R, S, rows, rc),
        out_shape=(
            jax.ShapeDtypeStruct((S, chunks, rc, cols), BF16),
            jax.ShapeDtypeStruct((S,) + master.shape, BF16),
            jax.ShapeDtypeStruct((8, 128), F32),
        ),
        in_specs=[in_vmem, anywhere, anywhere, anywhere],
        out_specs=(anywhere, anywhere, in_vmem),
        scratch_shapes=[
            vmem((loads * BLOCK_ROWS, width), BF16),
            vmem((BLOCK_ROWS, width) if quad else (16, 128), BF16),
            vmem((half, width) if quad else (16, 128), BF16),
            vmem(master.shape, F32),
            vmem(master.shape, F32),
            vmem(master.shape, BF16),
            vmem((chunks, Z, rc, cols), BF16),
            vmem((chunks, Z, rc, cols), BF16),
            vmem((chunks, zs, rc, cols), BF16),
            vmem((chunks, rc, cols), BF16),
            vmem((2, 8, 128), F32),
            vmem((R - 1, 8, 128), F32),
            vmem((S - 1, 8, 128), F32),
            dma((loads,)), dma((2,)), dma((2,)), dma((2,)), dma, dma,
            dma((chunks, Z)), dma((chunks, Z)),
            dma((chunks, zs)), dma((chunks, zs)),
            dma((chunks,)), dma((chunks,)), dma((chunks,)),
            dma((ys, chunks)), dma((ys, chunks)), dma((ys, chunks)), dma((ys, chunks)),
            dma, dma, dma,
            dma((ys,)), dma((ys,)), dma((ys,)), dma((ys,)),
            dma((R - 1,)), dma((R - 1,)), dma((S - 1,)), dma((S - 1,)),
        ],
        compiler_params=pltpu.CompilerParams(
            collective_id=0, has_side_effects=True, vmem_limit_bytes=VMEM_LIMIT
        ),
        name="sync",
    )(block_owner, deltas, master, momentum)

    return tuple(pl.pallas_call(
        functools.partial(finish_kernel, R, units),
        out_shape=(
            jax.ShapeDtypeStruct(master.shape, F32),
            jax.ShapeDtypeStruct(master.shape, F32),
            jax.ShapeDtypeStruct((blocks * BLOCK_ROWS, cols), BF16),
        ),
        in_specs=[in_vmem, in_vmem] + [anywhere] * 4,
        out_specs=(anywhere,) * 3,
        scratch_shapes=[
            pltpu.SMEM((1, blocks), jnp.int32), dma,
            vmem(master.shape, F32),
            vmem(master.shape, F32),
            vmem((2 * SLOTS, half, cols), BF16),
            vmem((blocks, BLOCK_ROWS, cols), BF16),
            vmem((2 * blocks, half, cols), BF16),
            dma((SLOTS,)), dma((SLOTS,)), dma((2 * SLOTS,)), dma((blocks,)), dma((2 * blocks,)),
            dma((SLOTS,)), dma((SLOTS,)), dma((blocks,)),
        ],
        compiler_params=pltpu.CompilerParams(vmem_limit_bytes=VMEM_LIMIT),
        name="finish",
    )(block_owner, tot, master, momentum, sums.reshape(S * units, half, cols),
      bases.reshape(S * SLOTS, BLOCK_ROWS, cols)))


def solution(mesh):
    return jax.shard_map(
        on_device,
        mesh=mesh,
        in_specs=(P("replica", "shard", None), P("shard", "replica"), P("shard", "replica"), P()),
        out_specs=(P("shard", "replica"), P("shard", "replica"), P(None, "replica")),
        check_vma=False,
    )
```

```python
import functools

import jax
import jax.numpy as jnp
from jax import lax
from jax.experimental import pallas as pl
from jax.experimental.pallas import tpu as pltpu
from jax.sharding import PartitionSpec as P

BLOCK_ROWS = 128
SLOTS = 4
F32 = jnp.float32
BF16 = jnp.bfloat16
VMEM_LIMIT = 56 * 1024 * 1024


def remote(src, dst, send, recv, device):
    return pltpu.make_async_remote_copy(
        src_ref=src, dst_ref=dst, send_sem=send, recv_sem=recv,
        device_id=device, device_id_type=pl.DeviceIdType.MESH,
    )


def shard_count(owner, shard):
    return sum(jnp.where(owner[0, b] == shard, 1, 0) for b in range(owner.shape[1]))


def spread(condition, shape):
    return jnp.broadcast_to(jnp.where(condition, 1, 0), shape) != 0


def sync_kernel(
    R, S, rows, rc,
    owner, deltas, master, momentum,
    sums, bases, tot,
    dv, p3, yt, ms, mm, base, xin, pair, zin, mine, norm, nbuf, sbuf,
    ld, lm, p3_s, p3_r, t_s, t_r, x_s, x_r, z_s, z_r, l_s, c_s, c_r, y_s, y_r, f_s, f_r,
    bl_s, bc_s, bc_r, by_s, by_r, bf_s, bf_r, n_s, n_r, m_s, m_r,
):
    width = deltas.shape[2]
    cols = width // R
    Z, O = R // 2, S // 2
    per = BLOCK_ROWS // rc
    half = BLOCK_ROWS // 2
    chunks = rows // rc
    quad = rows < SLOTS * BLOCK_ROWS
    whole = rows // BLOCK_ROWS
    direct = whole * per
    top = whole * BLOCK_ROWS
    me_r, me_s = lax.axis_index("replica"), lax.axis_index("shard")
    z, x = me_r // 2, me_r % 2
    o, core = me_s // 2, me_s % 2
    x_peer = z * 2 + 1 - x
    twin = o * 2 + 1 - core

    barrier = pltpu.get_barrier_semaphore()
    for i in range(1, R):
        pl.semaphore_signal(barrier, inc=1, device_id=((me_r + i) % R, me_s), device_id_type=pl.DeviceIdType.MESH)
    for i in range(1, S):
        pl.semaphore_signal(barrier, inc=1, device_id=(me_r, (me_s + i) % S), device_id_type=pl.DeviceIdType.MESH)

    def load(k):
        part = pl.ds(k * BLOCK_ROWS, BLOCK_ROWS)
        return pltpu.make_async_copy(deltas.at[0, part, :], dv.at[part, :], ld.at[k])

    if quad:
        load(whole).start()
    for k in range(whole):
        load(k).start()
    load_master = pltpu.make_async_copy(master, ms, lm.at[0])
    load_momentum = pltpu.make_async_copy(momentum, mm, lm.at[1])
    load_master.start()
    load_momentum.start()
    mine_count = jnp.sum(jnp.where(owner[...] == me_s, 1, 0), axis=1, keepdims=True)
    twin_count = jnp.sum(jnp.where(owner[...] == twin, 1, 0), axis=1, keepdims=True)
    heavy = jnp.maximum(mine_count, twin_count) >= SLOTS
    pl.semaphore_wait(barrier, R + S - 2)

    def rows_of(c):
        return pl.ds(pl.multiple_of(c * rc, rc), rc)

    def columns(c, j, side):
        return pl.ds(pl.multiple_of((((z + 1 + j) % Z) * 2 + side) * cols, cols), cols)

    def x_copy(source, c, j):
        return remote(
            source.at[rows_of(c), columns(c, j, 1 - x)], xin.at[c, j], x_s.at[c, j], x_r.at[c, j], (x_peer, me_s)
        )

    def z_copy(c, j):
        return remote(
            pair.at[c, j], zin.at[c, j], z_s.at[c, j], z_r.at[c, j], (((z + 1 + j) % Z) * 2 + x, me_s)
        )

    def c_copy(c):
        return remote(mine.at[c], sums.at[me_s, c], c_s.at[c], c_r.at[c], (me_r, twin))

    def l_copy(c):
        return pltpu.make_async_copy(mine.at[c], sums.at[me_s, c], l_s.at[c])

    def y_copy(i, c):
        return remote(
            mine.at[c], sums.at[me_s, c], y_s.at[i - 1, c], y_r.at[i - 1, c], (me_r, ((o + i) % O) * 2 + core)
        )

    def f_copy(i, c):
        source = ((o + O - i) % O) * 2 + core
        return remote(sums.at[source, c], sums.at[source, c], f_s.at[i - 1, c], f_r.at[i - 1, c], (me_r, twin))

    def by_copy(i):
        return remote(base, bases.at[me_s], by_s.at[i - 1], by_r.at[i - 1], (me_r, ((o + i) % O) * 2 + core))

    def bf_copy(i):
        source = ((o + O - i) % O) * 2 + core
        return remote(bases.at[source], bases.at[source], bf_s.at[i - 1], bf_r.at[i - 1], (me_r, twin))

    def third_copy(h):
        return remote(
            deltas.at[0, pl.ds((SLOTS - 1) * BLOCK_ROWS + h * half, half), :],
            p3.at[pl.ds(h * half, half), :], p3_s.at[h], p3_r.at[h], (me_r, twin),
        )

    def t_copy():
        return remote(dv.at[pl.ds(top + half, half), :], yt, t_s, t_r, (me_r, ((o + 1) % O) * 2 + core))

    def base_twin():
        return remote(base, bases.at[me_s], bc_s, bc_r, (me_r, twin))

    def base_local():
        return pltpu.make_async_copy(base, bases.at[me_s], bl_s)

    def start_x(source, low, high):
        @pl.loop(low, high)
        def _(c):
            for j in range(Z):
                x_copy(source, c, j).start()

    def pick(condition, other, start, other_start):
        @pl.loop(0, half // 16)
        def _(r):
            keep = spread(condition, (16, 1024))
            for q in range(width // 1024):
                at = (pl.ds(pl.multiple_of(start + r * 16, 16), 16), pl.ds(q * 1024, 1024))
                there = (pl.ds(pl.multiple_of(other_start + r * 16, 16), 16), pl.ds(q * 1024, 1024))
                dv[at] = jnp.where(keep, dv[at].astype(F32), other[there].astype(F32)).astype(BF16)

    if quad:
        third_copy(1).start()
        third_copy(0).start()
    start_x(deltas.at[0], 0, direct)
    norm[0] = jnp.zeros((8, 128), F32)

    def send_third():
        load(whole).wait()
        third_copy(1).wait_recv()
        pick(mine_count >= SLOTS, p3, top + half, half)
        t_copy().start()

    def make_base():
        load_master.wait()
        load_momentum.wait()

        @pl.loop(0, SLOTS * BLOCK_ROWS // 16)
        def _(r):
            at = pl.ds(pl.multiple_of(r * 16, 16), 16)
            base[at, :] = (ms[at, :] - 0.567 * mm[at, :]).astype(BF16)

        for i in range(1, O):
            by_copy(i).start()
        base_twin().start()
        base_local().start()

    def add_pair(c):
        @pl.when(c % per == 0)
        def _():
            @pl.when(c < direct)
            def _():
                load(c // per).wait()

        for j in range(Z):
            x_copy(deltas.at[0], c, j).wait_recv()
            pair[c, j] = (xin[c, j].astype(F32) + dv[rows_of(c), columns(c, j, x)].astype(F32)).astype(BF16)
            if j < Z - 1:
                z_copy(c, j).start()

    def add_line(c):
        for j in range(Z - 1):
            z_copy(c, j).wait_recv()
        place = jnp.where(c >= direct, -1, c // per) if quad else c // per
        live = spread(place < mine_count, (8, 128))
        part = jnp.zeros((8, 128), F32)
        for r in range(0, rc, 16):
            total = pair[c, Z - 1, r:r + 16, :].astype(F32)
            for j in range(Z - 1):
                total = total + zin[c, j, r:r + 16, :].astype(F32)
            total = total / R
            mine[c, r:r + 16, :] = total.astype(BF16)
            for h in range(0, 16, 8):
                for q in range(0, cols, 128):
                    v = total[h:h + 8, q:q + 128]
                    part = part + v * v
        norm[0] = norm[0] + jnp.where(live, part, 0.0)
        for i in range(1, O):
            y_copy(i, c).start()
        c_copy(c).start()
        l_copy(c).start()

    def forward(c):
        for i in range(1, O):
            y_copy(i, c).wait_recv()
            f_copy(i, c).start()

    lag = 4

    @pl.loop(0, chunks + lag)
    def _(t):
        @pl.when(t < chunks)
        def _():
            add_pair(t)

        @pl.when(t >= lag)
        def _():
            add_line(t - lag)

        @pl.when(t == 2)
        def _():
            make_base()

        if quad:
            @pl.when(t == 0)
            def _():
                send_third()

            @pl.when(t == direct - direct // 4)
            def _():
                third_copy(0).wait_recv()
                pick(mine_count >= SLOTS, p3, top, 0)
                t_copy().wait_recv()
                pick(heavy, yt, top, 0)
                start_x(dv, direct, chunks)

    def n_copy(i):
        return remote(norm.at[0], nbuf.at[i - 1], n_s.at[i - 1], n_r.at[i - 1], ((me_r + i) % R, me_s))

    def m_copy(i):
        return remote(norm.at[1], sbuf.at[i - 1], m_s.at[i - 1], m_r.at[i - 1], (me_r, (me_s + i) % S))

    for i in range(1, R):
        n_copy(i).start()
    for i in range(1, O):
        by_copy(i).wait_recv()
        bf_copy(i).start()

    @pl.loop(0, chunks - 2)
    def _(c):
        forward(c)
        for j in range(Z):
            x_copy(deltas.at[0], c, j).wait_send()
        for j in range(Z - 1):
            z_copy(c, j).wait_send()

    total = norm[0]
    for i in range(1, R):
        n_copy(i).wait_recv()
        total = total + nbuf[i - 1]
    norm[1] = total
    for i in range(1, S):
        m_copy(i).start()

    @pl.loop(chunks - 2, chunks)
    def _(c):
        forward(c)

    for i in range(1, S):
        m_copy(i).wait_recv()
        total = total + sbuf[i - 1]
    tot[...] = total

    if quad:
        third_copy(0).wait_send()
        third_copy(1).wait_send()
        t_copy().wait_send()
    base_local().wait()
    base_twin().wait()
    for i in range(1, O):
        by_copy(i).wait_send()
        bf_copy(i).wait()
    for i in range(1, R):
        n_copy(i).wait_send()
    for i in range(1, S):
        m_copy(i).wait_send()

    @pl.loop(chunks - 2, chunks)
    def _(c):
        for j in range(Z):
            x_copy(deltas.at[0], c, j).wait_send()
        for j in range(Z - 1):
            z_copy(c, j).wait_send()

    @pl.loop(0, chunks)
    def _(c):
        l_copy(c).wait()
        c_copy(c).wait()
        for i in range(1, O):
            y_copy(i, c).wait_send()
            f_copy(i, c).wait()


def tree_kernel(
    R, S, rows, rc, first,
    owner, deltas, master, momentum,
    sums, bases, tot,
    dv, p3, yt, ms, mm, base, b3, b3_in,
    xin, pair, zq, comb, zin, qb, combb, zinb, part_b, keep_b, xin_b, mine, norm, total_row, nbuf,
    ld, lm, p3_s, p3_r, t_s, t_r, x_s, x_r, q_s, q_r, far_s, far_r,
    qb_s, qb_r, farb_s, farb_r, xb_s, xb_r,
    l_s, c_s, c_r, y_s, y_r, f_s, f_r,
    b3_s, b3_r, bl_s, bc_s, bc_r, by_s, by_r, bf_s, bf_r, n_s, n_r,
):
    width = deltas.shape[2]
    cols = width // R
    Z = R // 2
    per = BLOCK_ROWS // rc
    half = BLOCK_ROWS // 2
    chunks = rows // rc
    whole = rows // BLOCK_ROWS
    direct = whole * per
    top = whole * BLOCK_ROWS
    me_r, me_s = lax.axis_index("replica"), lax.axis_index("shard")
    z, x = me_r // 2, me_r % 2
    o, core = me_s // 2, me_s % 2
    side = z // 2
    inner = (z + side) % 2
    outer = 1 - inner
    is_inner, is_outer = inner == 1, inner == 0
    x_peer = (z * 2 + 1 - x, me_s)
    near = ((side * 2 + 1 - z % 2) * 2 + x, me_s)
    far_outer = ((Z - 1) * (1 - side) * 2 + x, me_s)
    far_inner = ((Z - 1 - z) * 2 + x, me_s)
    twin = o * 2 + 1 - core
    twin_device = (me_r, twin)
    y_shard = (1 - o) * 2 + core
    y_device = (me_r, y_shard)

    barrier = pltpu.get_barrier_semaphore()
    me = me_r * S + me_s

    def peer(i):
        other = (me + i) % (R * S)
        return (other // S, other % S)

    for i in range(1, R * S):
        pl.semaphore_signal(barrier, inc=1, device_id=peer(i), device_id_type=pl.DeviceIdType.MESH)

    def load(k):
        part = pl.ds(k * BLOCK_ROWS, BLOCK_ROWS)
        return pltpu.make_async_copy(deltas.at[0, part, :], dv.at[part, :], ld.at[k])

    load(whole).start()
    for k in range(whole):
        load(k).start()
    load_master = pltpu.make_async_copy(master, ms, lm.at[0])
    load_momentum = pltpu.make_async_copy(momentum, mm, lm.at[1])
    load_master.start()
    load_momentum.start()
    mine_count = jnp.sum(jnp.where(owner[...] == me_s, 1, 0), axis=1, keepdims=True)
    twin_count = jnp.sum(jnp.where(owner[...] == twin, 1, 0), axis=1, keepdims=True)
    heavy = jnp.maximum(mine_count, twin_count) >= SLOTS
    norm[...] = jnp.zeros((8, 128), F32)
    pl.semaphore_wait(barrier, R * S - 1)

    def rows_of(c):
        return pl.ds(pl.multiple_of(c * rc, rc), rc)

    def columns(k, side_x):
        e = (Z - k - outer) % Z
        d = e + side * (Z - 1 - 2 * e)
        return pl.ds(pl.multiple_of((d * 2 + side_x) * cols, cols), cols)

    def x_copy(source, c, k):
        return remote(
            source.at[rows_of(c), columns(k, 1 - x)], xin.at[c, k], x_s.at[c, k], x_r.at[c, k], x_peer
        )

    def q_copy(c, k):
        slot = 2 * inner if k == 0 else k
        return remote(pair.at[c, k], zq.at[c, slot], q_s.at[c, k], q_r.at[c, slot], near)

    def q_wait(c, slot):
        remote(pair.at[c, slot], zq.at[c, slot], q_s.at[c, slot], q_r.at[c, slot], near).wait_recv()

    def far_copy(c, i):
        return remote(comb.at[c, i], zin.at[c], far_s.at[c, i], far_r.at[c], far_inner if i else far_outer)

    def half_x(v):
        return x if v else 1 - x

    def qb_copy(c, v, k):
        slot = 2 * inner if k == 0 else k
        return remote(
            deltas.at[0, rows_of(c), columns(k, half_x(v))], qb.at[c, v, slot],
            qb_s.at[c, v, k], qb_r.at[c, v, slot], near,
        )

    def qb_wait(c, v, slot):
        remote(
            combb.at[c, v, 0], qb.at[c, v, slot], qb_s.at[c, v, slot], qb_r.at[c, v, slot], near
        ).wait_recv()

    def farb_copy(c, v, i):
        return remote(
            combb.at[c, v, i], zinb.at[c, v], farb_s.at[c, v, i], farb_r.at[c, v], far_inner if i else far_outer
        )

    def xb_copy(c):
        return remote(part_b.at[c], xin_b.at[c], xb_s.at[c], xb_r.at[c], x_peer)

    def c_copy(c):
        return remote(mine.at[c], sums.at[me_s, c], c_s.at[c], c_r.at[c], twin_device)

    def l_copy(c):
        return pltpu.make_async_copy(mine.at[c], sums.at[me_s, c], l_s.at[c])

    def y_copy(c):
        return remote(mine.at[c], sums.at[me_s, c], y_s.at[c], y_r.at[c], y_device)

    def f_copy(c):
        return remote(sums.at[y_shard, c], sums.at[y_shard, c], f_s.at[c], f_r.at[c], twin_device)

    def by_copy():
        return remote(base, bases.at[me_s], by_s, by_r, y_device)

    def bf_copy():
        return remote(bases.at[y_shard], bases.at[y_shard], bf_s, bf_r, twin_device)

    def b3_copy():
        return remote(b3, b3_in, b3_s, b3_r, twin_device)

    def base_twin():
        return remote(base, bases.at[me_s], bc_s, bc_r, twin_device)

    def base_local():
        return pltpu.make_async_copy(base, bases.at[me_s], bl_s)

    def third_copy(h):
        return remote(
            deltas.at[0, pl.ds((SLOTS - 1) * BLOCK_ROWS + h * half, half), :],
            p3.at[pl.ds(h * half, half), :], p3_s.at[h], p3_r.at[h], twin_device,
        )

    def t_copy():
        return remote(dv.at[pl.ds(top + half, half), :], yt, t_s, t_r, y_device)

    def start_x(source, low, high):
        @pl.loop(low, high)
        def _(c):
            for k in range(Z):
                x_copy(source, c, k).start()

    def start_qb(c):
        for v in range(2):
            qb_copy(c, v, 0).start()

            @pl.when(is_outer)
            def _():
                for k in range(1, Z - 1):
                    qb_copy(c, v, k).start()

    def pick(condition, other, start, other_start):
        @pl.loop(0, half // 16)
        def _(r):
            keep = spread(condition, (16, 1024))
            for q in range(width // 1024):
                at = (pl.ds(pl.multiple_of(start + r * 16, 16), 16), pl.ds(q * 1024, 1024))
                there = (pl.ds(pl.multiple_of(other_start + r * 16, 16), 16), pl.ds(q * 1024, 1024))
                dv[at] = jnp.where(keep, dv[at].astype(F32), other[there].astype(F32)).astype(BF16)

    third_copy(1).start()
    third_copy(0).start()
    start_x(deltas.at[0], first, first + 1)

    @pl.loop(0, first)
    def _(c):
        start_qb(c)

    start_x(deltas.at[0], first + 1, direct)

    def send_third():
        load(whole).wait()
        third_copy(1).wait_recv()
        pick(mine_count >= SLOTS, p3, top + half, half)
        t_copy().start()

    def start_base(low, high, target, target_start):
        @pl.loop(low * BLOCK_ROWS // 16, high * BLOCK_ROWS // 16)
        def _(r):
            at = pl.ds(pl.multiple_of(r * 16, 16), 16)
            to = pl.ds(pl.multiple_of(r * 16 - target_start, 16), 16)
            target[to, :] = (ms[at, :] - 0.567 * mm[at, :]).astype(BF16)

    def make_base():
        load_master.wait()
        load_momentum.wait()
        start_base(SLOTS - 1, SLOTS, b3, (SLOTS - 1) * BLOCK_ROWS)
        b3_copy().start()
        start_base(0, SLOTS - 1, base, 0)

    def send_base():
        b3_copy().wait_recv()

        @pl.loop(0, BLOCK_ROWS // 16)
        def _(r):
            at = pl.ds(pl.multiple_of(top + r * 16, 16), 16)
            there = pl.ds(pl.multiple_of(r * 16, 16), 16)
            keep = spread(mine_count >= SLOTS, (16, cols))
            base[at, :] = jnp.where(keep, base[at, :].astype(F32), b3_in[there, :].astype(F32)).astype(BF16)

        by_copy().start()
        base_twin().start()
        base_local().start()

    def add_pair(c):
        @pl.when(jnp.logical_and(c % per == 0, c < direct))
        def _():
            load(c // per).wait()

        for k in range(Z):
            x_copy(deltas.at[0], c, k).wait_recv()
            pair[c, k] = (xin[c, k].astype(F32) + dv[rows_of(c), columns(k, x)].astype(F32)).astype(BF16)
            if k == 0:
                q_copy(c, k).start()
            elif k < Z - 1:
                @pl.when(is_outer)
                def _():
                    q_copy(c, k).start()

    def add_mid(c):
        for i in range(2):
            q_wait(c, i)
            comb[c, i] = (pair[c, 1 + i].astype(F32) + zq[c, i].astype(F32)).astype(BF16)
            far_copy(c, i).start()

    def add_mid_b(c):
        for v in range(2):
            for i in range(2):
                qb_wait(c, v, i)
                own = dv[rows_of(c), columns(1 + i, half_x(v))].astype(F32)
                combb[c, v, i] = (own + qb[c, v, i].astype(F32)).astype(BF16)
                farb_copy(c, v, i).start()

    def add_line_b(c):
        for v in range(2):
            qb_wait(c, v, 2)
            farb_copy(c, v, 0).wait_recv()
            own = dv[rows_of(c), columns(Z - 1, half_x(v))].astype(F32)
            value = own + qb[c, v, 2].astype(F32) + zinb[c, v].astype(F32)
            if v:
                keep_b[c] = value
            else:
                part_b[c] = value.astype(BF16)
                xb_copy(c).start()

    def emit(c, get):
        place = jnp.where(c >= direct, -1, c // per)
        live = spread(place < mine_count, (8, 128))
        part = jnp.zeros((8, 128), F32)
        for r in range(0, rc, 16):
            total = get(r) / R
            mine[c, r:r + 16, :] = total.astype(BF16)
            for h in range(0, 16, 8):
                for q in range(0, cols, 128):
                    v = total[h:h + 8, q:q + 128]
                    part = part + v * v
        norm[...] = norm[...] + jnp.where(live, part, 0.0)
        y_copy(c).start()
        c_copy(c).start()
        l_copy(c).start()

    def add_line(c):
        q_wait(c, 2)
        far_copy(c, 0).wait_recv()
        emit(c, lambda r: (
            pair[c, Z - 1, r:r + 16, :].astype(F32) + zq[c, 2, r:r + 16, :].astype(F32)
            + zin[c, r:r + 16, :].astype(F32)
        ))

    def add_last_b(c):
        xb_copy(c).wait_recv()
        emit(c, lambda r: keep_b[c, r:r + 16, :] + xin_b[c, r:r + 16, :].astype(F32))

    def forward(c):
        y_copy(c).wait_recv()
        f_copy(c).start()

    make_base()
    send_third()
    send_base()
    load(0).wait()

    mid_lag, line_lag = 2, 4
    steps = chunks - first
    quad_at = (direct - first) * 2 // 3

    @pl.loop(0, steps + line_lag)
    def _(t):
        @pl.when(t == direct - first)
        def _():
            @pl.loop(0, first)
            def _(c):
                add_last_b(c)

        @pl.when(t < steps)
        def _():
            add_pair(first + t)

        @pl.when(jnp.logical_and(is_inner, t < first))
        def _():
            add_mid_b(t)

        @pl.when(jnp.logical_and(t >= 2, t < 2 + first))
        def _():
            add_line_b(t - 2)

        @pl.when(jnp.logical_and(is_inner, jnp.logical_and(t >= mid_lag, t < steps + mid_lag)))
        def _():
            add_mid(first + t - mid_lag)

        @pl.when(t >= line_lag)
        def _():
            add_line(first + t - line_lag)

        @pl.when(t == quad_at)
        def _():
            third_copy(0).wait_recv()
            pick(mine_count >= SLOTS, p3, top, 0)
            t_copy().wait_recv()
            pick(heavy, yt, top, 0)
            start_x(dv, direct, chunks)

    total_row[...] = jnp.sum(norm[...], axis=0, keepdims=True)

    def n_copy(i):
        return remote(total_row, nbuf.at[i - 1], n_s.at[i - 1], n_r.at[i - 1], peer(i))

    for i in range(1, R * S):
        n_copy(i).start()
    by_copy().wait_recv()
    bf_copy().start()

    @pl.loop(first, chunks - 2)
    def _(c):
        forward(c)

    @pl.loop(0, first)
    def _(c):
        forward(c)

    @pl.loop(chunks - 2, chunks)
    def _(c):
        forward(c)

    third_copy(0).wait_send()
    third_copy(1).wait_send()
    t_copy().wait_send()
    b3_copy().wait_send()
    base_local().wait()
    base_twin().wait()

    @pl.loop(first, chunks)
    def _(c):
        for k in range(Z):
            x_copy(deltas.at[0], c, k).wait_send()
        q_copy(c, 0).wait_send()

        @pl.when(is_outer)
        def _():
            for k in range(1, Z - 1):
                q_copy(c, k).wait_send()

        @pl.when(is_inner)
        def _():
            for i in range(2):
                far_copy(c, i).wait_send()

    @pl.loop(0, first)
    def _(c):
        xb_copy(c).wait_send()
        for v in range(2):
            qb_copy(c, v, 0).wait_send()

            @pl.when(is_outer)
            def _():
                for k in range(1, Z - 1):
                    qb_copy(c, v, k).wait_send()

            @pl.when(is_inner)
            def _():
                for i in range(2):
                    farb_copy(c, v, i).wait_send()

    @pl.loop(0, chunks)
    def _(c):
        l_copy(c).wait()
        c_copy(c).wait()
        y_copy(c).wait_send()
        f_copy(c).wait()

    by_copy().wait_send()
    bf_copy().wait()
    total = total_row[...]
    for i in range(1, R * S):
        n_copy(i).wait_recv()
        total = total + nbuf[i - 1]
    tot[...] = jnp.broadcast_to(total, (8, 128)) * jnp.where(
        lax.broadcasted_iota(jnp.int32, (8, 128), 0) == 0, 1.0, 0.0
    )
    for i in range(1, R * S):
        n_copy(i).wait_send()


def finish_kernel(
    R, units, held,
    owner_in, tot, master, momentum, sums, bases,
    master_out, momentum_out, params,
    owner, owner_s, ms, mm, su, pb, ps,
    a_s, b_s, u_s, p_s, q_s, oa_s, ob_s, op_s,
):
    blocks = owner.shape[1]
    cols = master.shape[1]
    half = BLOCK_ROWS // 2
    me_s = lax.axis_index("shard")
    get_owner = pltpu.make_async_copy(owner_in, owner, owner_s)
    get_owner.start()

    def unit(shard, place, h):
        if units == 2 * SLOTS:
            return shard * units + 2 * place + h
        moved = shard + jnp.where(place == SLOTS - 1, 1 - 2 * (shard % 2), 0)
        if h:
            moved = moved + jnp.where(moved // 2 == 0, 2, -2)
        return jnp.where(place < 2, shard * units + 2 * place + h, moved * units + units - 1)

    def slot_rows(j):
        return pl.ds(pl.multiple_of(j * BLOCK_ROWS, BLOCK_ROWS), BLOCK_ROWS)

    def get_slot(j):
        return [
            pltpu.make_async_copy(master.at[slot_rows(j)], ms.at[slot_rows(j)], a_s.at[j]),
            pltpu.make_async_copy(momentum.at[slot_rows(j)], mm.at[slot_rows(j)], b_s.at[j]),
        ] + [
            pltpu.make_async_copy(sums.at[unit(me_s, j, h)], su.at[2 * j + h], u_s.at[2 * j + h]) for h in range(2)
        ]

    def put_slot(j):
        return [
            pltpu.make_async_copy(ms.at[slot_rows(j)], master_out.at[slot_rows(j)], oa_s.at[j]),
            pltpu.make_async_copy(mm.at[slot_rows(j)], momentum_out.at[slot_rows(j)], ob_s.at[j]),
        ]

    def get_block(b):
        shard = owner[0, b]
        place = sum(jnp.where(jnp.logical_and(owner[0, k] == shard, k < b), 1, 0) for k in range(blocks))
        kept = shard * held + place
        if held < SLOTS:
            kept = jnp.where(place < held, kept, (shard + 1 - 2 * (shard % 2)) * held + held - 1)
        return [pltpu.make_async_copy(bases.at[kept], pb.at[b], p_s.at[b])] + [
            pltpu.make_async_copy(sums.at[unit(shard, place, h)], ps.at[2 * b + h], q_s.at[2 * b + h])
            for h in range(2)
        ]

    def put_block(b):
        return pltpu.make_async_copy(pb.at[b], params.at[slot_rows(b)], op_s.at[b])

    @pl.loop(0, SLOTS)
    def _(j):
        for copy in get_slot(j):
            copy.start()

    get_owner.wait()
    count = shard_count(owner, me_s)

    @pl.loop(0, blocks)
    def _(b):
        for copy in get_block(b):
            copy.start()

    total = jnp.sum(jnp.sum(tot[...], axis=1, keepdims=True), axis=0, keepdims=True)
    limit = 0.5 * jnp.sqrt(jnp.full((1, 1), blocks * BLOCK_ROWS * R * cols, F32))
    factor = jnp.minimum(1.0, limit / (jnp.sqrt(total) + 1e-06))

    @pl.loop(0, SLOTS)
    def _(j):
        for copy in get_slot(j):
            copy.wait()

        @pl.when(j < count)
        def _():
            for h in range(2):
                @pl.loop(0, half // 16)
                def _(r):
                    at = pl.ds(pl.multiple_of(j * BLOCK_ROWS + h * half + r * 16, 16), 16)
                    grad = factor * su[2 * j + h, pl.ds(pl.multiple_of(r * 16, 16), 16), :].astype(F32)
                    fresh = 0.9 * mm[at, :] + grad
                    mm[at, :] = fresh
                    ms[at, :] = ms[at, :] - 0.7 * (grad + 0.9 * fresh)

        for copy in put_slot(j):
            copy.start()

    @pl.loop(0, blocks)
    def _(b):
        for copy in get_block(b):
            copy.wait()
        for h in range(2):
            @pl.loop(0, half // 16)
            def _(r):
                at = pl.ds(pl.multiple_of(h * half + r * 16, 16), 16)
                grad = factor * ps[2 * b + h, pl.ds(pl.multiple_of(r * 16, 16), 16), :].astype(F32)
                pb[b, at, :] = (pb[b, at, :].astype(F32) - 1.33 * grad).astype(BF16)

        put_block(b).start()

    @pl.loop(0, SLOTS)
    def _(j):
        for copy in put_slot(j):
            copy.wait()

    @pl.loop(0, blocks)
    def _(b):
        put_block(b).wait()


def on_device(deltas, master, momentum, block_owner):
    R, S = lax.axis_size("replica"), lax.axis_size("shard")
    width, cols = deltas.shape[2], master.shape[1]
    blocks = block_owner.shape[0]
    block_owner = block_owner.reshape(1, blocks)
    half = BLOCK_ROWS // 2
    quad = S == 4 and blocks - SLOTS - (S - 2) <= 2
    rows = 2 * BLOCK_ROWS + half if quad else SLOTS * BLOCK_ROWS
    rc = half
    while rc > 16 and (rows // (rc // 2)) * R <= 160:
        rc //= 2
    chunks = rows // rc
    units = rows // half
    Z, O = R // 2, S // 2
    loads = rows // BLOCK_ROWS + (1 if quad else 0)

    dma = pltpu.SemaphoreType.DMA
    vmem = pltpu.VMEM
    anywhere = pl.BlockSpec(memory_space=pl.ANY)
    in_vmem = pl.BlockSpec(memory_space=pltpu.VMEM)
    in_smem = pl.BlockSpec(memory_space=pltpu.SMEM)
    tree = quad and Z == 4 and O == 2
    held = SLOTS - 1 if tree else SLOTS
    if tree:
        first = chunks * 3 // 20
        piece = (rc, cols)
        sums, bases, tot = pl.pallas_call(
            functools.partial(tree_kernel, R, S, rows, rc, first),
            out_shape=(
                jax.ShapeDtypeStruct((S, chunks, rc, cols), BF16),
                jax.ShapeDtypeStruct((S, held * BLOCK_ROWS, cols), BF16),
                jax.ShapeDtypeStruct((8, 128), F32),
            ),
            in_specs=[in_vmem, anywhere, anywhere, anywhere],
            out_specs=(anywhere, anywhere, in_vmem),
            scratch_shapes=[
                vmem((loads * BLOCK_ROWS, width), BF16),
                vmem((BLOCK_ROWS, width), BF16),
                vmem((half, width), BF16),
                vmem(master.shape, F32),
                vmem(master.shape, F32),
                vmem((held * BLOCK_ROWS, cols), BF16),
                vmem((BLOCK_ROWS, cols), BF16),
                vmem((BLOCK_ROWS, cols), BF16),
                vmem((chunks, Z) + piece, BF16),
                vmem((chunks, Z) + piece, BF16),
                vmem((chunks, 3) + piece, BF16),
                vmem((chunks, 2) + piece, BF16),
                vmem((chunks,) + piece, BF16),
                vmem((first, 2, 3) + piece, BF16),
                vmem((first, 2, 2) + piece, BF16),
                vmem((first, 2) + piece, BF16),
                vmem((first,) + piece, BF16),
                vmem((first,) + piece, F32),
                vmem((first,) + piece, BF16),
                vmem((chunks,) + piece, BF16),
                vmem((8, 128), F32),
                vmem((1, 128), F32),
                vmem((R * S - 1, 1, 128), F32),
                dma((loads,)), dma((2,)), dma((2,)), dma((2,)), dma, dma,
                dma((chunks, Z)), dma((chunks, Z)),
                dma((chunks, 3)), dma((chunks, 3)),
                dma((chunks, 2)), dma((chunks,)),
                dma((first, 2, 3)), dma((first, 2, 3)),
                dma((first, 2, 2)), dma((first, 2)),
                dma((first,)), dma((first,)),
                dma((chunks,)), dma((chunks,)), dma((chunks,)),
                dma((chunks,)), dma((chunks,)), dma((chunks,)), dma((chunks,)),
                dma, dma, dma, dma, dma, dma, dma, dma, dma,
                dma((R * S - 1,)), dma((R * S - 1,)),
            ],
            compiler_params=pltpu.CompilerParams(
                collective_id=0, has_side_effects=True, vmem_limit_bytes=VMEM_LIMIT
            ),
            name="sync",
        )(block_owner, deltas, master, momentum)
    else:
        ys, zs = max(O - 1, 1), max(Z - 1, 1)
        sums, bases, tot = pl.pallas_call(
            functools.partial(sync_kernel, R, S, rows, rc),
            out_shape=(
                jax.ShapeDtypeStruct((S, chunks, rc, cols), BF16),
                jax.ShapeDtypeStruct((S,) + master.shape, BF16),
                jax.ShapeDtypeStruct((8, 128), F32),
            ),
            in_specs=[in_vmem, anywhere, anywhere, anywhere],
            out_specs=(anywhere, anywhere, in_vmem),
            scratch_shapes=[
                vmem((loads * BLOCK_ROWS, width), BF16),
                vmem((BLOCK_ROWS, width) if quad else (16, 128), BF16),
                vmem((half, width) if quad else (16, 128), BF16),
                vmem(master.shape, F32),
                vmem(master.shape, F32),
                vmem(master.shape, BF16),
                vmem((chunks, Z, rc, cols), BF16),
                vmem((chunks, Z, rc, cols), BF16),
                vmem((chunks, zs, rc, cols), BF16),
                vmem((chunks, rc, cols), BF16),
                vmem((2, 8, 128), F32),
                vmem((R - 1, 8, 128), F32),
                vmem((S - 1, 8, 128), F32),
                dma((loads,)), dma((2,)), dma((2,)), dma((2,)), dma, dma,
                dma((chunks, Z)), dma((chunks, Z)),
                dma((chunks, zs)), dma((chunks, zs)),
                dma((chunks,)), dma((chunks,)), dma((chunks,)),
                dma((ys, chunks)), dma((ys, chunks)), dma((ys, chunks)), dma((ys, chunks)),
                dma, dma, dma,
                dma((ys,)), dma((ys,)), dma((ys,)), dma((ys,)),
                dma((R - 1,)), dma((R - 1,)), dma((S - 1,)), dma((S - 1,)),
            ],
            compiler_params=pltpu.CompilerParams(
                collective_id=0, has_side_effects=True, vmem_limit_bytes=VMEM_LIMIT
            ),
            name="sync",
        )(block_owner, deltas, master, momentum)

    return tuple(pl.pallas_call(
        functools.partial(finish_kernel, R, units, held),
        out_shape=(
            jax.ShapeDtypeStruct(master.shape, F32),
            jax.ShapeDtypeStruct(master.shape, F32),
            jax.ShapeDtypeStruct((blocks * BLOCK_ROWS, cols), BF16),
        ),
        in_specs=[in_vmem, in_vmem] + [anywhere] * 4,
        out_specs=(anywhere,) * 3,
        scratch_shapes=[
            pltpu.SMEM((1, blocks), jnp.int32), dma,
            vmem(master.shape, F32),
            vmem(master.shape, F32),
            vmem((2 * SLOTS, half, cols), BF16),
            vmem((blocks, BLOCK_ROWS, cols), BF16),
            vmem((2 * blocks, half, cols), BF16),
            dma((SLOTS,)), dma((SLOTS,)), dma((2 * SLOTS,)), dma((blocks,)), dma((2 * blocks,)),
            dma((SLOTS,)), dma((SLOTS,)), dma((blocks,)),
        ],
        compiler_params=pltpu.CompilerParams(vmem_limit_bytes=VMEM_LIMIT),
        name="finish",
    )(block_owner, tot, master, momentum, sums.reshape(S * units, half, cols),
      bases.reshape(S * held, BLOCK_ROWS, cols)))


def solution(mesh):
    return jax.shard_map(
        on_device,
        mesh=mesh,
        in_specs=(P("replica", "shard", None), P("shard", "replica"), P("shard", "replica"), P()),
        out_specs=(P("shard", "replica"), P("shard", "replica"), P(None, "replica")),
        check_vma=False,
    )
```

```python
import functools

import jax
import jax.numpy as jnp
from jax import lax
from jax.experimental import pallas as pl
from jax.experimental.pallas import tpu as pltpu
from jax.sharding import PartitionSpec as P

BLOCK_ROWS = 128
SLOTS = 4
F32 = jnp.float32
BF16 = jnp.bfloat16
VMEM_LIMIT = 56 * 1024 * 1024


def remote(src, dst, send, recv, device):
    return pltpu.make_async_remote_copy(
        src_ref=src, dst_ref=dst, send_sem=send, recv_sem=recv,
        device_id=device, device_id_type=pl.DeviceIdType.MESH,
    )


def shard_count(owner, shard):
    return sum(jnp.where(owner[0, b] == shard, 1, 0) for b in range(owner.shape[1]))


def spread(condition, shape):
    return jnp.broadcast_to(jnp.where(condition, 1, 0), shape) != 0


def sync_kernel(
    R, S, rows, rc,
    owner, deltas, master, momentum,
    sums, bases, tot,
    dv, p3, yt, ms, mm, base, xin, pair, zin, mine, norm, nbuf, sbuf,
    ld, lm, p3_s, p3_r, t_s, t_r, x_s, x_r, z_s, z_r, l_s, c_s, c_r, y_s, y_r, f_s, f_r,
    bl_s, bc_s, bc_r, by_s, by_r, bf_s, bf_r, n_s, n_r, m_s, m_r,
):
    width = deltas.shape[2]
    cols = width // R
    Z, O = R // 2, S // 2
    per = BLOCK_ROWS // rc
    half = BLOCK_ROWS // 2
    chunks = rows // rc
    quad = rows < SLOTS * BLOCK_ROWS
    whole = rows // BLOCK_ROWS
    direct = whole * per
    top = whole * BLOCK_ROWS
    me_r, me_s = lax.axis_index("replica"), lax.axis_index("shard")
    z, x = me_r // 2, me_r % 2
    o, core = me_s // 2, me_s % 2
    x_peer = z * 2 + 1 - x
    twin = o * 2 + 1 - core

    barrier = pltpu.get_barrier_semaphore()
    for i in range(1, R):
        pl.semaphore_signal(barrier, inc=1, device_id=((me_r + i) % R, me_s), device_id_type=pl.DeviceIdType.MESH)
    for i in range(1, S):
        pl.semaphore_signal(barrier, inc=1, device_id=(me_r, (me_s + i) % S), device_id_type=pl.DeviceIdType.MESH)

    def load(k):
        part = pl.ds(k * BLOCK_ROWS, BLOCK_ROWS)
        return pltpu.make_async_copy(deltas.at[0, part, :], dv.at[part, :], ld.at[k])

    if quad:
        load(whole).start()
    for k in range(whole):
        load(k).start()
    load_master = pltpu.make_async_copy(master, ms, lm.at[0])
    load_momentum = pltpu.make_async_copy(momentum, mm, lm.at[1])
    load_master.start()
    load_momentum.start()
    mine_count = jnp.sum(jnp.where(owner[...] == me_s, 1, 0), axis=1, keepdims=True)
    twin_count = jnp.sum(jnp.where(owner[...] == twin, 1, 0), axis=1, keepdims=True)
    heavy = jnp.maximum(mine_count, twin_count) >= SLOTS
    pl.semaphore_wait(barrier, R + S - 2)

    def rows_of(c):
        return pl.ds(pl.multiple_of(c * rc, rc), rc)

    def columns(c, j, side):
        return pl.ds(pl.multiple_of((((z + 1 + j) % Z) * 2 + side) * cols, cols), cols)

    def x_copy(source, c, j):
        return remote(
            source.at[rows_of(c), columns(c, j, 1 - x)], xin.at[c, j], x_s.at[c, j], x_r.at[c, j], (x_peer, me_s)
        )

    def z_copy(c, j):
        return remote(
            pair.at[c, j], zin.at[c, j], z_s.at[c, j], z_r.at[c, j], (((z + 1 + j) % Z) * 2 + x, me_s)
        )

    def c_copy(c):
        return remote(mine.at[c], sums.at[me_s, c], c_s.at[c], c_r.at[c], (me_r, twin))

    def l_copy(c):
        return pltpu.make_async_copy(mine.at[c], sums.at[me_s, c], l_s.at[c])

    def y_copy(i, c):
        return remote(
            mine.at[c], sums.at[me_s, c], y_s.at[i - 1, c], y_r.at[i - 1, c], (me_r, ((o + i) % O) * 2 + core)
        )

    def f_copy(i, c):
        source = ((o + O - i) % O) * 2 + core
        return remote(sums.at[source, c], sums.at[source, c], f_s.at[i - 1, c], f_r.at[i - 1, c], (me_r, twin))

    def by_copy(i):
        return remote(base, bases.at[me_s], by_s.at[i - 1], by_r.at[i - 1], (me_r, ((o + i) % O) * 2 + core))

    def bf_copy(i):
        source = ((o + O - i) % O) * 2 + core
        return remote(bases.at[source], bases.at[source], bf_s.at[i - 1], bf_r.at[i - 1], (me_r, twin))

    def third_copy(h):
        return remote(
            deltas.at[0, pl.ds((SLOTS - 1) * BLOCK_ROWS + h * half, half), :],
            p3.at[pl.ds(h * half, half), :], p3_s.at[h], p3_r.at[h], (me_r, twin),
        )

    def t_copy():
        return remote(dv.at[pl.ds(top + half, half), :], yt, t_s, t_r, (me_r, ((o + 1) % O) * 2 + core))

    def base_twin():
        return remote(base, bases.at[me_s], bc_s, bc_r, (me_r, twin))

    def base_local():
        return pltpu.make_async_copy(base, bases.at[me_s], bl_s)

    def start_x(source, low, high):
        @pl.loop(low, high)
        def _(c):
            for j in range(Z):
                x_copy(source, c, j).start()

    def pick(condition, other, start, other_start):
        @pl.loop(0, half // 16)
        def _(r):
            keep = spread(condition, (16, 1024))
            for q in range(width // 1024):
                at = (pl.ds(pl.multiple_of(start + r * 16, 16), 16), pl.ds(q * 1024, 1024))
                there = (pl.ds(pl.multiple_of(other_start + r * 16, 16), 16), pl.ds(q * 1024, 1024))
                dv[at] = jnp.where(keep, dv[at].astype(F32), other[there].astype(F32)).astype(BF16)

    if quad:
        third_copy(1).start()
        third_copy(0).start()
    start_x(deltas.at[0], 0, direct)
    norm[0] = jnp.zeros((8, 128), F32)

    def send_third():
        load(whole).wait()
        third_copy(1).wait_recv()
        pick(mine_count >= SLOTS, p3, top + half, half)
        t_copy().start()

    def make_base():
        load_master.wait()
        load_momentum.wait()

        @pl.loop(0, SLOTS * BLOCK_ROWS // 16)
        def _(r):
            at = pl.ds(pl.multiple_of(r * 16, 16), 16)
            base[at, :] = (ms[at, :] - 0.567 * mm[at, :]).astype(BF16)

        for i in range(1, O):
            by_copy(i).start()
        base_twin().start()
        base_local().start()

    def add_pair(c):
        @pl.when(c % per == 0)
        def _():
            @pl.when(c < direct)
            def _():
                load(c // per).wait()

        for j in range(Z):
            x_copy(deltas.at[0], c, j).wait_recv()
            pair[c, j] = (xin[c, j].astype(F32) + dv[rows_of(c), columns(c, j, x)].astype(F32)).astype(BF16)
            if j < Z - 1:
                z_copy(c, j).start()

    def add_line(c):
        for j in range(Z - 1):
            z_copy(c, j).wait_recv()
        place = jnp.where(c >= direct, -1, c // per) if quad else c // per
        live = spread(place < mine_count, (8, 128))
        part = jnp.zeros((8, 128), F32)
        for r in range(0, rc, 16):
            total = pair[c, Z - 1, r:r + 16, :].astype(F32)
            for j in range(Z - 1):
                total = total + zin[c, j, r:r + 16, :].astype(F32)
            total = total / R
            mine[c, r:r + 16, :] = total.astype(BF16)
            for h in range(0, 16, 8):
                for q in range(0, cols, 128):
                    v = total[h:h + 8, q:q + 128]
                    part = part + v * v
        norm[0] = norm[0] + jnp.where(live, part, 0.0)
        for i in range(1, O):
            y_copy(i, c).start()
        c_copy(c).start()
        l_copy(c).start()

    def forward(c):
        for i in range(1, O):
            y_copy(i, c).wait_recv()
            f_copy(i, c).start()

    lag = 4

    @pl.loop(0, chunks + lag)
    def _(t):
        @pl.when(t < chunks)
        def _():
            add_pair(t)

        @pl.when(t >= lag)
        def _():
            add_line(t - lag)

        @pl.when(t == 2)
        def _():
            make_base()

        if quad:
            @pl.when(t == 0)
            def _():
                send_third()

            @pl.when(t == direct - direct // 4)
            def _():
                third_copy(0).wait_recv()
                pick(mine_count >= SLOTS, p3, top, 0)
                t_copy().wait_recv()
                pick(heavy, yt, top, 0)
                start_x(dv, direct, chunks)

    def n_copy(i):
        return remote(norm.at[0], nbuf.at[i - 1], n_s.at[i - 1], n_r.at[i - 1], ((me_r + i) % R, me_s))

    def m_copy(i):
        return remote(norm.at[1], sbuf.at[i - 1], m_s.at[i - 1], m_r.at[i - 1], (me_r, (me_s + i) % S))

    for i in range(1, R):
        n_copy(i).start()
    for i in range(1, O):
        by_copy(i).wait_recv()
        bf_copy(i).start()

    @pl.loop(0, chunks - 2)
    def _(c):
        forward(c)
        for j in range(Z):
            x_copy(deltas.at[0], c, j).wait_send()
        for j in range(Z - 1):
            z_copy(c, j).wait_send()

    total = norm[0]
    for i in range(1, R):
        n_copy(i).wait_recv()
        total = total + nbuf[i - 1]
    norm[1] = total
    for i in range(1, S):
        m_copy(i).start()

    @pl.loop(chunks - 2, chunks)
    def _(c):
        forward(c)

    for i in range(1, S):
        m_copy(i).wait_recv()
        total = total + sbuf[i - 1]
    tot[...] = total

    if quad:
        third_copy(0).wait_send()
        third_copy(1).wait_send()
        t_copy().wait_send()
    base_local().wait()
    base_twin().wait()
    for i in range(1, O):
        by_copy(i).wait_send()
        bf_copy(i).wait()
    for i in range(1, R):
        n_copy(i).wait_send()
    for i in range(1, S):
        m_copy(i).wait_send()

    @pl.loop(chunks - 2, chunks)
    def _(c):
        for j in range(Z):
            x_copy(deltas.at[0], c, j).wait_send()
        for j in range(Z - 1):
            z_copy(c, j).wait_send()

    @pl.loop(0, chunks)
    def _(c):
        l_copy(c).wait()
        c_copy(c).wait()
        for i in range(1, O):
            y_copy(i, c).wait_send()
            f_copy(i, c).wait()


def tree_kernel(
    R, S, rows, rc, first,
    owner, deltas, master, momentum,
    sums, bases, tot,
    dv, p3, yt, ms, mm, base, b3, b3_in,
    xin, pair, zq, comb, zin, qb, combb, zinb, part_b, keep_b, xin_b, mine, norm, total_row, nbuf,
    ld, lm, p3_s, p3_r, t_s, t_r, x_s, x_r, q_s, qa_r, qc_r, far_s, far_r,
    qb_s, qb_r, farb_s, farb_r, xb_s, xb_r,
    l_s, c_s, c_r, y_s, y_r, f_s, f_r,
    b3_s, b3_r, bl_s, bc_s, bc_r, by_s, by_r, bf_s, bf_r, n_s, n_r,
):
    width = deltas.shape[2]
    cols = width // R
    Z = R // 2
    per = BLOCK_ROWS // rc
    half = BLOCK_ROWS // 2
    chunks = rows // rc
    whole = rows // BLOCK_ROWS
    direct = whole * per
    top = whole * BLOCK_ROWS
    me_r, me_s = lax.axis_index("replica"), lax.axis_index("shard")
    z, x = me_r // 2, me_r % 2
    o, core = me_s // 2, me_s % 2
    side = z // 2
    inner = (z + side) % 2
    outer = 1 - inner
    is_inner, is_outer = inner == 1, inner == 0
    x_peer = (z * 2 + 1 - x, me_s)
    near = ((side * 2 + 1 - z % 2) * 2 + x, me_s)
    far_outer = ((Z - 1) * (1 - side) * 2 + x, me_s)
    far_inner = ((Z - 1 - z) * 2 + x, me_s)
    far = ((1 + inner * (Z - 2 - z) + outer * (1 - side)) * 2 + x, me_s)
    twin = o * 2 + 1 - core
    twin_device = (me_r, twin)
    y_shard = (1 - o) * 2 + core
    y_device = (me_r, y_shard)

    barrier = pltpu.get_barrier_semaphore()
    me = me_r * S + me_s

    def peer(i):
        other = (me + i) % (R * S)
        return (other // S, other % S)

    for device in (x_peer, twin_device, y_device, near, far):
        pl.semaphore_signal(barrier, inc=1, device_id=device, device_id_type=pl.DeviceIdType.MESH)

    @pl.when(is_inner)
    def _():
        pl.semaphore_signal(barrier, inc=1, device_id=far_outer, device_id_type=pl.DeviceIdType.MESH)

    def load(k):
        part = pl.ds(k * BLOCK_ROWS, BLOCK_ROWS)
        return pltpu.make_async_copy(deltas.at[0, part, :], dv.at[part, :], ld.at[k])

    load(whole).start()
    for k in range(whole):
        load(k).start()
    load_master = pltpu.make_async_copy(master, ms, lm.at[0])
    load_momentum = pltpu.make_async_copy(momentum, mm, lm.at[1])
    load_master.start()
    load_momentum.start()
    mine_count = jnp.sum(jnp.where(owner[...] == me_s, 1, 0), axis=1, keepdims=True)
    twin_count = jnp.sum(jnp.where(owner[...] == twin, 1, 0), axis=1, keepdims=True)
    heavy = jnp.maximum(mine_count, twin_count) >= SLOTS
    norm[...] = jnp.zeros((8, 128), F32)
    pl.semaphore_wait(barrier, 5 + inner)

    def rows_of(c):
        return pl.ds(pl.multiple_of(c * rc, rc), rc)

    def columns(k, side_x):
        e = (Z - k - outer) % Z
        d = e + side * (Z - 1 - 2 * e)
        return pl.ds(pl.multiple_of((d * 2 + side_x) * cols, cols), cols)

    def arrived(ref, sem):
        remote(ref, ref, n_s, sem, twin_device).wait_recv()

    def sent(ref, sem):
        remote(ref, ref, sem, n_r, twin_device).wait_send()

    def x_copy(source, c, k):
        return remote(source.at[rows_of(c), columns(k, 1 - x)], xin.at[c, k], x_s, x_r.at[c - first], x_peer)

    def start_q(c, k):
        if k == 0:
            @pl.when(is_inner)
            def _():
                remote(pair.at[c, 0], zq.at[c, 2], q_s, qc_r.at[c - first], near).start()

        @pl.when(is_outer)
        def _():
            remote(pair.at[c, k], zq.at[c, k], q_s, (qc_r if k == 2 else qa_r).at[c - first], near).start()

    def far_copy(c, i):
        return remote(comb.at[c, i], zin.at[c], far_s, far_r.at[c - first], far_inner if i else far_outer)

    def half_x(v):
        return x if v else 1 - x

    def start_qb(c):
        def start(v, k, slot):
            remote(
                deltas.at[0, rows_of(c), columns(k, half_x(v))], qb.at[c, slot, v],
                qb_s, qb_r.at[c, slot // 2], near,
            ).start()

        @pl.when(is_inner)
        def _():
            for v in range(2):
                start(v, 0, 2)

        @pl.when(is_outer)
        def _():
            for k in range(Z - 1):
                for v in range(2):
                    start(v, k, k)

    def farb_copy(c, v, i):
        return remote(combb.at[c, v, i], zinb.at[c, v], farb_s, farb_r.at[c], far_inner if i else far_outer)

    def xb_copy(c):
        return remote(part_b.at[c], xin_b.at[c], xb_s, xb_r.at[c], x_peer)

    def c_copy(c):
        return remote(mine.at[c], sums.at[me_s, c], c_s, c_r, twin_device)

    def l_copy(c):
        return pltpu.make_async_copy(mine.at[c], sums.at[me_s, c], l_s)

    def y_copy(c):
        return remote(mine.at[c], sums.at[me_s, c], y_s, y_r.at[c], y_device)

    def f_copy(c):
        return remote(sums.at[y_shard, c], sums.at[y_shard, c], f_s, f_r, twin_device)

    def by_copy():
        return remote(base, bases.at[me_s], by_s, by_r, y_device)

    def bf_copy():
        return remote(bases.at[y_shard], bases.at[y_shard], bf_s, bf_r, twin_device)

    def b3_copy():
        return remote(b3, b3_in, b3_s, b3_r, twin_device)

    def base_twin():
        return remote(base, bases.at[me_s], bc_s, bc_r, twin_device)

    def base_local():
        return pltpu.make_async_copy(base, bases.at[me_s], bl_s)

    def third_copy(h):
        return remote(
            deltas.at[0, pl.ds((SLOTS - 1) * BLOCK_ROWS + h * half, half), :],
            p3.at[pl.ds(h * half, half), :], p3_s, p3_r.at[h], twin_device,
        )

    def t_copy():
        return remote(dv.at[pl.ds(top + half, half), :], yt, t_s, t_r, y_device)

    def start_x(source, low, high):
        @pl.loop(low, high)
        def _(c):
            for k in range(Z):
                x_copy(source, c, k).start()

    def pick(condition, other, start, other_start):
        @pl.loop(0, half // 16)
        def _(r):
            keep = spread(condition, (16, 1024))
            for q in range(width // 1024):
                at = (pl.ds(pl.multiple_of(start + r * 16, 16), 16), pl.ds(q * 1024, 1024))
                there = (pl.ds(pl.multiple_of(other_start + r * 16, 16), 16), pl.ds(q * 1024, 1024))
                dv[at] = jnp.where(keep, dv[at].astype(F32), other[there].astype(F32)).astype(BF16)

    third_copy(1).start()
    third_copy(0).start()
    start_x(deltas.at[0], first, first + 1)

    @pl.loop(0, first)
    def _(c):
        start_qb(c)

    start_x(deltas.at[0], first + 1, direct)

    def send_third():
        load(whole).wait()
        third_copy(1).wait_recv()
        pick(mine_count >= SLOTS, p3, top + half, half)
        t_copy().start()

    def start_base(low, high, target, target_start):
        @pl.loop(low * BLOCK_ROWS // 16, high * BLOCK_ROWS // 16)
        def _(r):
            at = pl.ds(pl.multiple_of(r * 16, 16), 16)
            to = pl.ds(pl.multiple_of(r * 16 - target_start, 16), 16)
            target[to, :] = (ms[at, :] - 0.567 * mm[at, :]).astype(BF16)

    def make_base():
        load_master.wait()
        load_momentum.wait()
        start_base(SLOTS - 1, SLOTS, b3, (SLOTS - 1) * BLOCK_ROWS)
        b3_copy().start()
        start_base(0, SLOTS - 1, base, 0)

    def send_base():
        b3_copy().wait_recv()

        @pl.loop(0, BLOCK_ROWS // 16)
        def _(r):
            at = pl.ds(pl.multiple_of(top + r * 16, 16), 16)
            there = pl.ds(pl.multiple_of(r * 16, 16), 16)
            keep = spread(mine_count >= SLOTS, (16, cols))
            base[at, :] = jnp.where(keep, base[at, :].astype(F32), b3_in[there, :].astype(F32)).astype(BF16)

        by_copy().start()
        base_twin().start()
        base_local().start()

    def add_pair(c):
        @pl.when(jnp.logical_and(c % per == 0, c < direct))
        def _():
            load(c // per).wait()

        arrived(xin.at[c], x_r.at[c - first])
        for k in range(Z):
            pair[c, k] = (xin[c, k].astype(F32) + dv[rows_of(c), columns(k, x)].astype(F32)).astype(BF16)
            if k < Z - 1:
                start_q(c, k)

    def add_mid(c):
        arrived(zq.at[c, pl.ds(0, 2)], qa_r.at[c - first])
        for i in range(2):
            comb[c, i] = (pair[c, 1 + i].astype(F32) + zq[c, i].astype(F32)).astype(BF16)
            far_copy(c, i).start()

    def add_mid_b(c):
        arrived(qb.at[c, pl.ds(0, 2)], qb_r.at[c, 0])
        for v in range(2):
            for i in range(2):
                own = dv[rows_of(c), columns(1 + i, half_x(v))].astype(F32)
                combb[c, v, i] = (own + qb[c, i, v].astype(F32)).astype(BF16)
                farb_copy(c, v, i).start()

    def add_line_b(c):
        arrived(qb.at[c, 2], qb_r.at[c, 1])
        arrived(zinb.at[c], farb_r.at[c])
        for v in range(2):
            own = dv[rows_of(c), columns(Z - 1, half_x(v))].astype(F32)
            value = own + qb[c, 2, v].astype(F32) + zinb[c, v].astype(F32)
            if v:
                keep_b[c] = value
            else:
                part_b[c] = value.astype(BF16)

    def emit(c, get):
        place = jnp.where(c >= direct, -1, c // per)
        live = spread(place < mine_count, (8, 128))
        part = jnp.zeros((8, 128), F32)
        for r in range(0, rc, 16):
            total = get(r) / R
            mine[c, r:r + 16, :] = total.astype(BF16)
            for h in range(0, 16, 8):
                for q in range(0, cols, 128):
                    v = total[h:h + 8, q:q + 128]
                    part = part + v * v
        norm[...] = norm[...] + jnp.where(live, part, 0.0)
        y_copy(c).start()
        c_copy(c).start()
        l_copy(c).start()

    def add_line(c):
        arrived(zq.at[c, 2], qc_r.at[c - first])
        arrived(zin.at[c], far_r.at[c - first])
        emit(c, lambda r: (
            pair[c, Z - 1, r:r + 16, :].astype(F32) + zq[c, 2, r:r + 16, :].astype(F32)
            + zin[c, r:r + 16, :].astype(F32)
        ))

    def add_last_b(c):
        xb_copy(c).wait_recv()
        emit(c, lambda r: keep_b[c, r:r + 16, :] + xin_b[c, r:r + 16, :].astype(F32))

    def forward(c):
        y_copy(c).wait_recv()
        f_copy(c).start()

    make_base()
    send_third()
    send_base()
    load(0).wait()

    mid_lag, line_lag = 2, 4
    steps = chunks - first
    quad_at = (direct - first) * 2 // 3

    @pl.loop(0, steps + line_lag)
    def _(t):
        @pl.when(t < steps)
        def _():
            add_pair(first + t)

        @pl.when(jnp.logical_and(is_inner, t < first))
        def _():
            add_mid_b(t)

        @pl.when(jnp.logical_and(t >= 2, t < 2 + first))
        def _():
            add_line_b(t - 2)

        @pl.when(jnp.logical_and(is_inner, jnp.logical_and(t >= mid_lag, t < steps + mid_lag)))
        def _():
            add_mid(first + t - mid_lag)

        @pl.when(t >= line_lag)
        def _():
            add_line(first + t - line_lag)

        @pl.when(t == steps)
        def _():
            @pl.loop(0, first)
            def _(c):
                add_last_b(c)

        @pl.when(t == quad_at)
        def _():
            third_copy(0).wait_recv()
            pick(mine_count >= SLOTS, p3, top, 0)
            t_copy().wait_recv()
            pick(heavy, yt, top, 0)
            start_x(dv, direct, chunks)

            @pl.loop(0, first)
            def _(c):
                xb_copy(c).start()

    total_row[...] = jnp.sum(norm[...], axis=0, keepdims=True)

    def n_copy(i):
        return remote(total_row, nbuf.at[i - 1], n_s, n_r, peer(i))

    for i in range(1, R * S):
        n_copy(i).start()
    by_copy().wait_recv()
    bf_copy().start()

    @pl.loop(first, chunks - 2)
    def _(c):
        forward(c)

    @pl.loop(0, first)
    def _(c):
        forward(c)

    @pl.loop(chunks - 2, chunks)
    def _(c):
        forward(c)

    sent(p3, p3_s)
    t_copy().wait_send()
    b3_copy().wait_send()
    base_local().wait()
    base_twin().wait()
    ours = pl.ds(first, steps)
    sent(xin.at[ours], x_s)
    sent(xin_b, xb_s)

    @pl.when(is_outer)
    def _():
        sent(zq.at[ours], q_s)
        sent(qb, qb_s)

    @pl.when(is_inner)
    def _():
        sent(zin.at[ours], q_s)
        sent(zinb, qb_s)
        sent(comb.at[ours], far_s)
        sent(combb, farb_s)

    pltpu.make_async_copy(mine, sums.at[me_s], l_s).wait()
    sent(mine, c_s)
    sent(mine, y_s)
    sent(mine, f_s)
    arrived(sums.at[twin], c_r)
    arrived(mine, f_r)
    by_copy().wait_send()
    bf_copy().wait()
    arrived(nbuf, n_r)
    sent(nbuf, n_s)
    total = total_row[...]
    for i in range(1, R * S):
        total = total + nbuf[i - 1]
    tot[...] = jnp.broadcast_to(total, (8, 128)) * jnp.where(
        lax.broadcasted_iota(jnp.int32, (8, 128), 0) == 0, 1.0, 0.0
    )


def finish_kernel(
    R, units, held,
    owner_in, tot, master, momentum, sums, bases,
    master_out, momentum_out, params,
    owner, owner_s, ms, mm, su, pb, ps,
    a_s, b_s, u_s, p_s, q_s, oa_s, ob_s, op_s,
):
    blocks = owner.shape[1]
    cols = master.shape[1]
    half = BLOCK_ROWS // 2
    me_s = lax.axis_index("shard")
    get_owner = pltpu.make_async_copy(owner_in, owner, owner_s)
    get_owner.start()

    def unit(shard, place, h):
        if units == 2 * SLOTS:
            return shard * units + 2 * place + h
        moved = shard + jnp.where(place == SLOTS - 1, 1 - 2 * (shard % 2), 0)
        if h:
            moved = moved + jnp.where(moved // 2 == 0, 2, -2)
        return jnp.where(place < 2, shard * units + 2 * place + h, moved * units + units - 1)

    def slot_rows(j):
        return pl.ds(pl.multiple_of(j * BLOCK_ROWS, BLOCK_ROWS), BLOCK_ROWS)

    def get_slot(j):
        return [
            pltpu.make_async_copy(master.at[slot_rows(j)], ms.at[slot_rows(j)], a_s.at[j]),
            pltpu.make_async_copy(momentum.at[slot_rows(j)], mm.at[slot_rows(j)], b_s.at[j]),
        ] + [
            pltpu.make_async_copy(sums.at[unit(me_s, j, h)], su.at[2 * j + h], u_s.at[2 * j + h]) for h in range(2)
        ]

    def put_slot(j):
        return [
            pltpu.make_async_copy(ms.at[slot_rows(j)], master_out.at[slot_rows(j)], oa_s.at[j]),
            pltpu.make_async_copy(mm.at[slot_rows(j)], momentum_out.at[slot_rows(j)], ob_s.at[j]),
        ]

    def get_block(b):
        shard = owner[0, b]
        place = sum(jnp.where(jnp.logical_and(owner[0, k] == shard, k < b), 1, 0) for k in range(blocks))
        kept = shard * held + place
        if held < SLOTS:
            kept = jnp.where(place < held, kept, (shard + 1 - 2 * (shard % 2)) * held + held - 1)
        return [pltpu.make_async_copy(bases.at[kept], pb.at[b], p_s.at[b])] + [
            pltpu.make_async_copy(sums.at[unit(shard, place, h)], ps.at[2 * b + h], q_s.at[2 * b + h])
            for h in range(2)
        ]

    def put_block(b):
        return pltpu.make_async_copy(pb.at[b], params.at[slot_rows(b)], op_s.at[b])

    @pl.loop(0, SLOTS)
    def _(j):
        for copy in get_slot(j):
            copy.start()

    get_owner.wait()
    count = shard_count(owner, me_s)

    @pl.loop(0, blocks)
    def _(b):
        for copy in get_block(b):
            copy.start()

    total = jnp.sum(jnp.sum(tot[...], axis=1, keepdims=True), axis=0, keepdims=True)
    limit = 0.5 * jnp.sqrt(jnp.full((1, 1), blocks * BLOCK_ROWS * R * cols, F32))
    factor = jnp.minimum(1.0, limit / (jnp.sqrt(total) + 1e-06))

    @pl.loop(0, SLOTS)
    def _(j):
        for copy in get_slot(j):
            copy.wait()

        @pl.when(j < count)
        def _():
            for h in range(2):
                @pl.loop(0, half // 16)
                def _(r):
                    at = pl.ds(pl.multiple_of(j * BLOCK_ROWS + h * half + r * 16, 16), 16)
                    grad = factor * su[2 * j + h, pl.ds(pl.multiple_of(r * 16, 16), 16), :].astype(F32)
                    fresh = 0.9 * mm[at, :] + grad
                    mm[at, :] = fresh
                    ms[at, :] = ms[at, :] - 0.7 * (grad + 0.9 * fresh)

        for copy in put_slot(j):
            copy.start()

    @pl.loop(0, blocks)
    def _(b):
        for copy in get_block(b):
            copy.wait()
        for h in range(2):
            @pl.loop(0, half // 16)
            def _(r):
                at = pl.ds(pl.multiple_of(h * half + r * 16, 16), 16)
                grad = factor * ps[2 * b + h, pl.ds(pl.multiple_of(r * 16, 16), 16), :].astype(F32)
                pb[b, at, :] = (pb[b, at, :].astype(F32) - 1.33 * grad).astype(BF16)

        put_block(b).start()

    @pl.loop(0, SLOTS)
    def _(j):
        for copy in put_slot(j):
            copy.wait()

    @pl.loop(0, blocks)
    def _(b):
        put_block(b).wait()


def on_device(deltas, master, momentum, block_owner):
    R, S = lax.axis_size("replica"), lax.axis_size("shard")
    width, cols = deltas.shape[2], master.shape[1]
    blocks = block_owner.shape[0]
    block_owner = block_owner.reshape(1, blocks)
    half = BLOCK_ROWS // 2
    quad = S == 4 and blocks - SLOTS - (S - 2) <= 2
    rows = 2 * BLOCK_ROWS + half if quad else SLOTS * BLOCK_ROWS
    rc = half
    while rc > 16 and (rows // (rc // 2)) * R <= 160:
        rc //= 2
    chunks = rows // rc
    units = rows // half
    Z, O = R // 2, S // 2
    loads = rows // BLOCK_ROWS + (1 if quad else 0)

    dma = pltpu.SemaphoreType.DMA
    vmem = pltpu.VMEM
    anywhere = pl.BlockSpec(memory_space=pl.ANY)
    in_vmem = pl.BlockSpec(memory_space=pltpu.VMEM)
    in_smem = pl.BlockSpec(memory_space=pltpu.SMEM)
    tree = quad and Z == 4 and O == 2
    held = SLOTS - 1 if tree else SLOTS
    if tree:
        first = chunks // 5
        steps = chunks - first
        piece = (rc, cols)
        sums, bases, tot = pl.pallas_call(
            functools.partial(tree_kernel, R, S, rows, rc, first),
            out_shape=(
                jax.ShapeDtypeStruct((S, chunks, rc, cols), BF16),
                jax.ShapeDtypeStruct((S, held * BLOCK_ROWS, cols), BF16),
                jax.ShapeDtypeStruct((8, 128), F32),
            ),
            in_specs=[in_vmem, anywhere, anywhere, anywhere],
            out_specs=(anywhere, anywhere, in_vmem),
            scratch_shapes=[
                vmem((loads * BLOCK_ROWS, width), BF16),
                vmem((BLOCK_ROWS, width), BF16),
                vmem((half, width), BF16),
                vmem(master.shape, F32),
                vmem(master.shape, F32),
                vmem((held * BLOCK_ROWS, cols), BF16),
                vmem((BLOCK_ROWS, cols), BF16),
                vmem((BLOCK_ROWS, cols), BF16),
                vmem((chunks, Z) + piece, BF16),
                vmem((chunks, Z) + piece, BF16),
                vmem((chunks, 3) + piece, BF16),
                vmem((chunks, 2) + piece, BF16),
                vmem((chunks,) + piece, BF16),
                vmem((first, 3, 2) + piece, BF16),
                vmem((first, 2, 2) + piece, BF16),
                vmem((first, 2) + piece, BF16),
                vmem((first,) + piece, BF16),
                vmem((first,) + piece, F32),
                vmem((first,) + piece, BF16),
                vmem((chunks,) + piece, BF16),
                vmem((8, 128), F32),
                vmem((1, 128), F32),
                vmem((R * S - 1, 1, 128), F32),
                dma((loads,)), dma((2,)), dma, dma((2,)), dma, dma,
                dma, dma((steps,)), dma, dma((steps,)), dma((steps,)), dma, dma((steps,)),
                dma, dma((first, 2)), dma, dma((first,)), dma, dma((first,)),
                dma, dma, dma, dma, dma((chunks,)), dma, dma,
                dma, dma, dma, dma, dma, dma, dma, dma, dma, dma, dma,
            ],
            compiler_params=pltpu.CompilerParams(
                collective_id=0, has_side_effects=True, vmem_limit_bytes=VMEM_LIMIT
            ),
            name="sync",
        )(block_owner, deltas, master, momentum)
    else:
        ys, zs = max(O - 1, 1), max(Z - 1, 1)
        sums, bases, tot = pl.pallas_call(
            functools.partial(sync_kernel, R, S, rows, rc),
            out_shape=(
                jax.ShapeDtypeStruct((S, chunks, rc, cols), BF16),
                jax.ShapeDtypeStruct((S,) + master.shape, BF16),
                jax.ShapeDtypeStruct((8, 128), F32),
            ),
            in_specs=[in_vmem, anywhere, anywhere, anywhere],
            out_specs=(anywhere, anywhere, in_vmem),
            scratch_shapes=[
                vmem((loads * BLOCK_ROWS, width), BF16),
                vmem((BLOCK_ROWS, width) if quad else (16, 128), BF16),
                vmem((half, width) if quad else (16, 128), BF16),
                vmem(master.shape, F32),
                vmem(master.shape, F32),
                vmem(master.shape, BF16),
                vmem((chunks, Z, rc, cols), BF16),
                vmem((chunks, Z, rc, cols), BF16),
                vmem((chunks, zs, rc, cols), BF16),
                vmem((chunks, rc, cols), BF16),
                vmem((2, 8, 128), F32),
                vmem((R - 1, 8, 128), F32),
                vmem((S - 1, 8, 128), F32),
                dma((loads,)), dma((2,)), dma((2,)), dma((2,)), dma, dma,
                dma((chunks, Z)), dma((chunks, Z)),
                dma((chunks, zs)), dma((chunks, zs)),
                dma((chunks,)), dma((chunks,)), dma((chunks,)),
                dma((ys, chunks)), dma((ys, chunks)), dma((ys, chunks)), dma((ys, chunks)),
                dma, dma, dma,
                dma((ys,)), dma((ys,)), dma((ys,)), dma((ys,)),
                dma((R - 1,)), dma((R - 1,)), dma((S - 1,)), dma((S - 1,)),
            ],
            compiler_params=pltpu.CompilerParams(
                collective_id=0, has_side_effects=True, vmem_limit_bytes=VMEM_LIMIT
            ),
            name="sync",
        )(block_owner, deltas, master, momentum)

    return tuple(pl.pallas_call(
        functools.partial(finish_kernel, R, units, held),
        out_shape=(
            jax.ShapeDtypeStruct(master.shape, F32),
            jax.ShapeDtypeStruct(master.shape, F32),
            jax.ShapeDtypeStruct((blocks * BLOCK_ROWS, cols), BF16),
        ),
        in_specs=[in_vmem, in_vmem] + [anywhere] * 4,
        out_specs=(anywhere,) * 3,
        scratch_shapes=[
            pltpu.SMEM((1, blocks), jnp.int32), dma,
            vmem(master.shape, F32),
            vmem(master.shape, F32),
            vmem((2 * SLOTS, half, cols), BF16),
            vmem((blocks, BLOCK_ROWS, cols), BF16),
            vmem((2 * blocks, half, cols), BF16),
            dma((SLOTS,)), dma((SLOTS,)), dma((2 * SLOTS,)), dma((blocks,)), dma((2 * blocks,)),
            dma((SLOTS,)), dma((SLOTS,)), dma((blocks,)),
        ],
        compiler_params=pltpu.CompilerParams(vmem_limit_bytes=VMEM_LIMIT),
        name="finish",
    )(block_owner, tot, master, momentum, sums.reshape(S * units, half, cols),
      bases.reshape(S * held, BLOCK_ROWS, cols)))


def solution(mesh):
    return jax.shard_map(
        on_device,
        mesh=mesh,
        in_specs=(P("replica", "shard", None), P("shard", "replica"), P("shard", "replica"), P()),
        out_specs=(P("shard", "replica"), P("shard", "replica"), P(None, "replica")),
        check_vma=False,
    )
```

```python
import functools

import jax
import jax.numpy as jnp
from jax import lax
from jax.experimental import pallas as pl
from jax.experimental.pallas import tpu as pltpu
from jax.sharding import PartitionSpec as P

BLOCK_ROWS = 128
SLOTS = 4
F32 = jnp.float32
BF16 = jnp.bfloat16
VMEM_LIMIT = 56 * 1024 * 1024
SYNC_VMEM = 26 * 1024 * 1024
CLOSE_VMEM = 12 * 1024 * 1024


def remote(src, dst, send, recv, device):
    return pltpu.make_async_remote_copy(
        src_ref=src, dst_ref=dst, send_sem=send, recv_sem=recv,
        device_id=device, device_id_type=pl.DeviceIdType.MESH,
    )


def shard_count(owner, shard):
    return sum(jnp.where(owner[0, b] == shard, 1, 0) for b in range(owner.shape[1]))


def spread(condition, shape):
    return jnp.broadcast_to(jnp.where(condition, 1, 0), shape) != 0


def sync_kernel(
    R, S, rows, rc,
    owner, deltas, master, momentum,
    sums, bases, tot,
    dv, p3, yt, ms, mm, base, xin, pair, zin, mine, norm, nbuf, sbuf,
    ld, lm, p3_s, p3_r, t_s, t_r, x_s, x_r, z_s, z_r, l_s, c_s, c_r, y_s, y_r, f_s, f_r,
    bl_s, bc_s, bc_r, by_s, by_r, bf_s, bf_r, n_s, n_r, m_s, m_r,
):
    width = deltas.shape[2]
    cols = width // R
    Z, O = R // 2, S // 2
    per = BLOCK_ROWS // rc
    half = BLOCK_ROWS // 2
    chunks = rows // rc
    quad = rows < SLOTS * BLOCK_ROWS
    whole = rows // BLOCK_ROWS
    direct = whole * per
    top = whole * BLOCK_ROWS
    me_r, me_s = lax.axis_index("replica"), lax.axis_index("shard")
    z, x = me_r // 2, me_r % 2
    o, core = me_s // 2, me_s % 2
    x_peer = z * 2 + 1 - x
    twin = o * 2 + 1 - core

    barrier = pltpu.get_barrier_semaphore()
    for i in range(1, R):
        pl.semaphore_signal(barrier, inc=1, device_id=((me_r + i) % R, me_s), device_id_type=pl.DeviceIdType.MESH)
    for i in range(1, S):
        pl.semaphore_signal(barrier, inc=1, device_id=(me_r, (me_s + i) % S), device_id_type=pl.DeviceIdType.MESH)

    def load(k):
        part = pl.ds(k * BLOCK_ROWS, BLOCK_ROWS)
        return pltpu.make_async_copy(deltas.at[0, part, :], dv.at[part, :], ld.at[k])

    if quad:
        load(whole).start()
    for k in range(whole):
        load(k).start()
    load_master = pltpu.make_async_copy(master, ms, lm.at[0])
    load_momentum = pltpu.make_async_copy(momentum, mm, lm.at[1])
    load_master.start()
    load_momentum.start()
    mine_count = jnp.sum(jnp.where(owner[...] == me_s, 1, 0), axis=1, keepdims=True)
    twin_count = jnp.sum(jnp.where(owner[...] == twin, 1, 0), axis=1, keepdims=True)
    heavy = jnp.maximum(mine_count, twin_count) >= SLOTS
    pl.semaphore_wait(barrier, R + S - 2)

    def rows_of(c):
        return pl.ds(pl.multiple_of(c * rc, rc), rc)

    def columns(c, j, side):
        return pl.ds(pl.multiple_of((((z + 1 + j) % Z) * 2 + side) * cols, cols), cols)

    def x_copy(source, c, j):
        return remote(
            source.at[rows_of(c), columns(c, j, 1 - x)], xin.at[c, j], x_s.at[c, j], x_r.at[c, j], (x_peer, me_s)
        )

    def z_copy(c, j):
        return remote(
            pair.at[c, j], zin.at[c, j], z_s.at[c, j], z_r.at[c, j], (((z + 1 + j) % Z) * 2 + x, me_s)
        )

    def c_copy(c):
        return remote(mine.at[c], sums.at[me_s, c], c_s.at[c], c_r.at[c], (me_r, twin))

    def l_copy(c):
        return pltpu.make_async_copy(mine.at[c], sums.at[me_s, c], l_s.at[c])

    def y_copy(i, c):
        return remote(
            mine.at[c], sums.at[me_s, c], y_s.at[i - 1, c], y_r.at[i - 1, c], (me_r, ((o + i) % O) * 2 + core)
        )

    def f_copy(i, c):
        source = ((o + O - i) % O) * 2 + core
        return remote(sums.at[source, c], sums.at[source, c], f_s.at[i - 1, c], f_r.at[i - 1, c], (me_r, twin))

    def by_copy(i):
        return remote(base, bases.at[me_s], by_s.at[i - 1], by_r.at[i - 1], (me_r, ((o + i) % O) * 2 + core))

    def bf_copy(i):
        source = ((o + O - i) % O) * 2 + core
        return remote(bases.at[source], bases.at[source], bf_s.at[i - 1], bf_r.at[i - 1], (me_r, twin))

    def third_copy(h):
        return remote(
            deltas.at[0, pl.ds((SLOTS - 1) * BLOCK_ROWS + h * half, half), :],
            p3.at[pl.ds(h * half, half), :], p3_s.at[h], p3_r.at[h], (me_r, twin),
        )

    def t_copy():
        return remote(dv.at[pl.ds(top + half, half), :], yt, t_s, t_r, (me_r, ((o + 1) % O) * 2 + core))

    def base_twin():
        return remote(base, bases.at[me_s], bc_s, bc_r, (me_r, twin))

    def base_local():
        return pltpu.make_async_copy(base, bases.at[me_s], bl_s)

    def start_x(source, low, high):
        @pl.loop(low, high)
        def _(c):
            for j in range(Z):
                x_copy(source, c, j).start()

    def pick(condition, other, start, other_start):
        @pl.loop(0, half // 16)
        def _(r):
            keep = spread(condition, (16, 1024))
            for q in range(width // 1024):
                at = (pl.ds(pl.multiple_of(start + r * 16, 16), 16), pl.ds(q * 1024, 1024))
                there = (pl.ds(pl.multiple_of(other_start + r * 16, 16), 16), pl.ds(q * 1024, 1024))
                dv[at] = jnp.where(keep, dv[at].astype(F32), other[there].astype(F32)).astype(BF16)

    if quad:
        third_copy(1).start()
        third_copy(0).start()
    start_x(deltas.at[0], 0, direct)
    norm[0] = jnp.zeros((8, 128), F32)

    def send_third():
        load(whole).wait()
        third_copy(1).wait_recv()
        pick(mine_count >= SLOTS, p3, top + half, half)
        t_copy().start()

    def make_base():
        load_master.wait()
        load_momentum.wait()

        @pl.loop(0, SLOTS * BLOCK_ROWS // 16)
        def _(r):
            at = pl.ds(pl.multiple_of(r * 16, 16), 16)
            base[at, :] = (ms[at, :] - 0.567 * mm[at, :]).astype(BF16)

        for i in range(1, O):
            by_copy(i).start()
        base_twin().start()
        base_local().start()

    def add_pair(c):
        @pl.when(c % per == 0)
        def _():
            @pl.when(c < direct)
            def _():
                load(c // per).wait()

        for j in range(Z):
            x_copy(deltas.at[0], c, j).wait_recv()
            pair[c, j] = (xin[c, j].astype(F32) + dv[rows_of(c), columns(c, j, x)].astype(F32)).astype(BF16)
            if j < Z - 1:
                z_copy(c, j).start()

    def add_line(c):
        for j in range(Z - 1):
            z_copy(c, j).wait_recv()
        place = jnp.where(c >= direct, -1, c // per) if quad else c // per
        live = spread(place < mine_count, (8, 128))
        part = jnp.zeros((8, 128), F32)
        for r in range(0, rc, 16):
            total = pair[c, Z - 1, r:r + 16, :].astype(F32)
            for j in range(Z - 1):
                total = total + zin[c, j, r:r + 16, :].astype(F32)
            total = total / R
            mine[c, r:r + 16, :] = total.astype(BF16)
            for h in range(0, 16, 8):
                for q in range(0, cols, 128):
                    v = total[h:h + 8, q:q + 128]
                    part = part + v * v
        norm[0] = norm[0] + jnp.where(live, part, 0.0)
        for i in range(1, O):
            y_copy(i, c).start()
        c_copy(c).start()
        l_copy(c).start()

    def forward(c):
        for i in range(1, O):
            y_copy(i, c).wait_recv()
            f_copy(i, c).start()

    lag = 4

    @pl.loop(0, chunks + lag)
    def _(t):
        @pl.when(t < chunks)
        def _():
            add_pair(t)

        @pl.when(t >= lag)
        def _():
            add_line(t - lag)

        @pl.when(t == 2)
        def _():
            make_base()

        if quad:
            @pl.when(t == 0)
            def _():
                send_third()

            @pl.when(t == direct - direct // 4)
            def _():
                third_copy(0).wait_recv()
                pick(mine_count >= SLOTS, p3, top, 0)
                t_copy().wait_recv()
                pick(heavy, yt, top, 0)
                start_x(dv, direct, chunks)

    def n_copy(i):
        return remote(norm.at[0], nbuf.at[i - 1], n_s.at[i - 1], n_r.at[i - 1], ((me_r + i) % R, me_s))

    def m_copy(i):
        return remote(norm.at[1], sbuf.at[i - 1], m_s.at[i - 1], m_r.at[i - 1], (me_r, (me_s + i) % S))

    for i in range(1, R):
        n_copy(i).start()
    for i in range(1, O):
        by_copy(i).wait_recv()
        bf_copy(i).start()

    @pl.loop(0, chunks - 2)
    def _(c):
        forward(c)
        for j in range(Z):
            x_copy(deltas.at[0], c, j).wait_send()
        for j in range(Z - 1):
            z_copy(c, j).wait_send()

    total = norm[0]
    for i in range(1, R):
        n_copy(i).wait_recv()
        total = total + nbuf[i - 1]
    norm[1] = total
    for i in range(1, S):
        m_copy(i).start()

    @pl.loop(chunks - 2, chunks)
    def _(c):
        forward(c)

    for i in range(1, S):
        m_copy(i).wait_recv()
        total = total + sbuf[i - 1]
    tot[...] = total

    if quad:
        third_copy(0).wait_send()
        third_copy(1).wait_send()
        t_copy().wait_send()
    base_local().wait()
    base_twin().wait()
    for i in range(1, O):
        by_copy(i).wait_send()
        bf_copy(i).wait()
    for i in range(1, R):
        n_copy(i).wait_send()
    for i in range(1, S):
        m_copy(i).wait_send()

    @pl.loop(chunks - 2, chunks)
    def _(c):
        for j in range(Z):
            x_copy(deltas.at[0], c, j).wait_send()
        for j in range(Z - 1):
            z_copy(c, j).wait_send()

    @pl.loop(0, chunks)
    def _(c):
        l_copy(c).wait()
        c_copy(c).wait()
        for i in range(1, O):
            y_copy(i, c).wait_send()
            f_copy(i, c).wait()


def tree_kernel(
    R, S, rows, rc, first,
    owner_in, deltas, master, momentum,
    sums, bases, tot, ms, mm,
    owner, dv, p3, yt, b3, b3_in,
    xin, pair, zq, comb, zin, qb, combb, zinb, part_b, keep_b, xin_b, norm, total_row, nbuf,
    lo, ld, lm, p3_s, p3_r, t_s, t_r, x_s, x_r, q_s, qa_r, qc_r, far_s, far_r,
    qb_s, qb_r, farb_s, farb_r, xb_s, xb_r,
    c_s, c_r, y_s, y_r, f_s, f_r,
    b3_s, b3_r, bc_s, bc_r, by_s, by_r, bf_s, bf_r, n_s, n_r,
):
    width = deltas.shape[2]
    cols = width // R
    Z = R // 2
    per = BLOCK_ROWS // rc
    half = BLOCK_ROWS // 2
    chunks = rows // rc
    whole = rows // BLOCK_ROWS
    direct = whole * per
    top = whole * BLOCK_ROWS
    me_r, me_s = lax.axis_index("replica"), lax.axis_index("shard")
    z, x = me_r // 2, me_r % 2
    o, core = me_s // 2, me_s % 2
    side = z // 2
    inner = (z + side) % 2
    outer = 1 - inner
    is_inner, is_outer = inner == 1, inner == 0
    x_peer = (z * 2 + 1 - x, me_s)
    near = ((side * 2 + 1 - z % 2) * 2 + x, me_s)
    far_outer = ((Z - 1) * (1 - side) * 2 + x, me_s)
    far_inner = ((Z - 1 - z) * 2 + x, me_s)
    far = ((1 + inner * (Z - 2 - z) + outer * (1 - side)) * 2 + x, me_s)
    twin = o * 2 + 1 - core
    twin_device = (me_r, twin)
    y_shard = (1 - o) * 2 + core
    y_device = (me_r, y_shard)

    barrier = pltpu.get_barrier_semaphore()
    me = me_r * S + me_s

    def peer(i):
        other = (me + i) % (R * S)
        return (other // S, other % S)

    for device in (x_peer, twin_device, y_device, near, far):
        pl.semaphore_signal(barrier, inc=1, device_id=device, device_id_type=pl.DeviceIdType.MESH)

    @pl.when(is_inner)
    def _():
        pl.semaphore_signal(barrier, inc=1, device_id=far_outer, device_id_type=pl.DeviceIdType.MESH)

    def load(k):
        part = pl.ds(k * BLOCK_ROWS, BLOCK_ROWS)
        return pltpu.make_async_copy(deltas.at[0, part, :], dv.at[part, :], ld.at[k])

    load(whole).start()
    load_owner = pltpu.make_async_copy(owner_in, owner, lo)
    load_owner.start()
    for k in range(whole):
        load(k).start()
    load_master = pltpu.make_async_copy(master, ms, lm.at[0])
    load_momentum = pltpu.make_async_copy(momentum, mm, lm.at[1])
    load_master.start()
    load_momentum.start()
    norm[...] = jnp.zeros((8, 128), F32)
    pl.semaphore_wait(barrier, 5 + inner)
    mine, base = sums.at[me_s], bases.at[me_s]

    def rows_of(c):
        return pl.ds(pl.multiple_of(c * rc, rc), rc)

    def columns(k, side_x):
        e = (Z - k - outer) % Z
        d = e + side * (Z - 1 - 2 * e)
        return pl.ds(pl.multiple_of((d * 2 + side_x) * cols, cols), cols)

    def arrived(ref, sem):
        remote(ref, ref, n_s, sem, twin_device).wait_recv()

    def sent(ref, sem):
        remote(ref, ref, sem, n_r, twin_device).wait_send()

    def x_copy(source, c, k):
        return remote(source.at[rows_of(c), columns(k, 1 - x)], xin.at[c, k], x_s, x_r.at[c - first], x_peer)

    def start_q(c, k):
        if k == 0:
            @pl.when(is_inner)
            def _():
                remote(pair.at[c, 0], zq.at[c, 2], q_s, qc_r.at[c - first], near).start()

        @pl.when(is_outer)
        def _():
            remote(pair.at[c, k], zq.at[c, k], q_s, (qc_r if k == 2 else qa_r).at[c - first], near).start()

    def far_copy(c, i):
        return remote(comb.at[c, i], zin.at[c], far_s, far_r.at[c - first], far_inner if i else far_outer)

    def half_x(v):
        return x if v else 1 - x

    def start_qb(c):
        def start(v, k, slot):
            remote(
                deltas.at[0, rows_of(c), columns(k, half_x(v))], qb.at[c, slot, v],
                qb_s, qb_r.at[c, slot // 2], near,
            ).start()

        @pl.when(is_inner)
        def _():
            for v in range(2):
                start(v, 0, 2)

        @pl.when(is_outer)
        def _():
            for k in range(Z - 1):
                for v in range(2):
                    start(v, k, k)

    def farb_copy(c, v, i):
        return remote(combb.at[c, v, i], zinb.at[c, v], farb_s, farb_r.at[c], far_inner if i else far_outer)

    def xb_copy(c):
        return remote(part_b.at[c], xin_b.at[c], xb_s, xb_r.at[c], x_peer)

    def c_copy(c):
        return remote(mine.at[c], sums.at[me_s, c], c_s, c_r, twin_device)

    def y_copy(c):
        return remote(mine.at[c], sums.at[me_s, c], y_s, y_r.at[c], y_device)

    def f_copy(c):
        return remote(sums.at[y_shard, c], sums.at[y_shard, c], f_s, f_r, twin_device)

    def by_copy():
        return remote(base, bases.at[me_s], by_s, by_r, y_device)

    def bf_copy():
        return remote(bases.at[y_shard], bases.at[y_shard], bf_s, bf_r, twin_device)

    def b3_copy():
        return remote(b3, b3_in, b3_s, b3_r, twin_device)

    def base_twin():
        return remote(base, bases.at[me_s], bc_s, bc_r, twin_device)

    def third_copy(h):
        return remote(
            deltas.at[0, pl.ds((SLOTS - 1) * BLOCK_ROWS + h * half, half), :],
            p3.at[pl.ds(h * half, half), :], p3_s, p3_r.at[h], twin_device,
        )

    def t_copy():
        return remote(dv.at[pl.ds(top + half, half), :], yt, t_s, t_r, y_device)

    def start_x(source, low, high):
        @pl.loop(low, high)
        def _(c):
            for k in range(Z):
                x_copy(source, c, k).start()

    def pick(condition, other, start, other_start):
        @pl.loop(0, half // 16)
        def _(r):
            keep = spread(condition, (16, 1024))
            for q in range(width // 1024):
                at = (pl.ds(pl.multiple_of(start + r * 16, 16), 16), pl.ds(q * 1024, 1024))
                there = (pl.ds(pl.multiple_of(other_start + r * 16, 16), 16), pl.ds(q * 1024, 1024))
                dv[at] = jnp.where(keep, dv[at].astype(F32), other[there].astype(F32)).astype(BF16)

    third_copy(1).start()
    third_copy(0).start()
    start_x(deltas.at[0], first, first + 1)

    @pl.loop(0, first)
    def _(c):
        start_qb(c)

    start_x(deltas.at[0], first + 1, direct)

    def send_third():
        load(whole).wait()
        third_copy(1).wait_recv()
        pick(mine_count >= SLOTS, p3, top + half, half)
        t_copy().start()

    def start_base(low, high, target, target_start):
        @pl.loop(low * BLOCK_ROWS // 16, high * BLOCK_ROWS // 16)
        def _(r):
            at = pl.ds(pl.multiple_of(r * 16, 16), 16)
            to = pl.ds(pl.multiple_of(r * 16 - target_start, 16), 16)
            target[to, :] = (ms[at, :] - 0.567 * mm[at, :]).astype(BF16)

    def make_base():
        load_master.wait()
        load_momentum.wait()
        start_base(SLOTS - 1, SLOTS, b3, (SLOTS - 1) * BLOCK_ROWS)
        b3_copy().start()
        start_base(0, SLOTS - 1, base, 0)

    def send_base():
        b3_copy().wait_recv()

        @pl.loop(0, BLOCK_ROWS // 16)
        def _(r):
            at = pl.ds(pl.multiple_of(top + r * 16, 16), 16)
            there = pl.ds(pl.multiple_of(r * 16, 16), 16)
            keep = spread(mine_count >= SLOTS, (16, cols))
            base[at, :] = jnp.where(keep, base[at, :].astype(F32), b3_in[there, :].astype(F32)).astype(BF16)

        by_copy().start()
        base_twin().start()

    def add_pair(c):
        @pl.when(jnp.logical_and(c % per == 0, c < direct))
        def _():
            load(c // per).wait()

        arrived(xin.at[c], x_r.at[c - first])
        for k in range(Z):
            pair[c, k] = (xin[c, k].astype(F32) + dv[rows_of(c), columns(k, x)].astype(F32)).astype(BF16)
            if k < Z - 1:
                start_q(c, k)

    def add_mid(c):
        arrived(zq.at[c, pl.ds(0, 2)], qa_r.at[c - first])
        for i in range(2):
            comb[c, i] = (pair[c, 1 + i].astype(F32) + zq[c, i].astype(F32)).astype(BF16)
            far_copy(c, i).start()

    def add_mid_b(c):
        arrived(qb.at[c, pl.ds(0, 2)], qb_r.at[c, 0])
        for v in range(2):
            for i in range(2):
                own = dv[rows_of(c), columns(1 + i, half_x(v))].astype(F32)
                combb[c, v, i] = (own + qb[c, i, v].astype(F32)).astype(BF16)
                farb_copy(c, v, i).start()

    def add_line_b(c):
        arrived(qb.at[c, 2], qb_r.at[c, 1])
        arrived(zinb.at[c], farb_r.at[c])
        for v in range(2):
            own = dv[rows_of(c), columns(Z - 1, half_x(v))].astype(F32)
            value = own + qb[c, 2, v].astype(F32) + zinb[c, v].astype(F32)
            if v:
                keep_b[c] = value
            else:
                part_b[c] = value.astype(BF16)

    def emit(c, get):
        place = jnp.where(c >= direct, -1, c // per)
        live = spread(place < mine_count, (8, 128))
        part = jnp.zeros((8, 128), F32)
        for r in range(0, rc, 16):
            total = get(r) / R
            mine[c, r:r + 16, :] = total.astype(BF16)
            for h in range(0, 16, 8):
                for q in range(0, cols, 128):
                    v = total[h:h + 8, q:q + 128]
                    part = part + v * v
        norm[...] = norm[...] + jnp.where(live, part, 0.0)
        y_copy(c).start()
        c_copy(c).start()

    def add_line(c):
        arrived(zq.at[c, 2], qc_r.at[c - first])
        arrived(zin.at[c], far_r.at[c - first])
        emit(c, lambda r: (
            pair[c, Z - 1, r:r + 16, :].astype(F32) + zq[c, 2, r:r + 16, :].astype(F32)
            + zin[c, r:r + 16, :].astype(F32)
        ))

    def add_last_b(c):
        xb_copy(c).wait_recv()
        emit(c, lambda r: keep_b[c, r:r + 16, :] + xin_b[c, r:r + 16, :].astype(F32))

    def forward(c):
        y_copy(c).wait_recv()
        f_copy(c).start()

    load_owner.wait()
    mine_count = jnp.sum(jnp.where(owner[...] == me_s, 1, 0), axis=1, keepdims=True)
    twin_count = jnp.sum(jnp.where(owner[...] == twin, 1, 0), axis=1, keepdims=True)
    heavy = jnp.maximum(mine_count, twin_count) >= SLOTS
    make_base()
    send_third()
    send_base()
    load(0).wait()

    mid_lag, line_lag = 2, 4
    steps = chunks - first
    quad_at = (direct - first) * 2 // 3

    @pl.loop(0, steps + line_lag)
    def _(t):
        @pl.when(t < steps)
        def _():
            add_pair(first + t)

        @pl.when(jnp.logical_and(is_inner, t < first))
        def _():
            add_mid_b(t)

        @pl.when(jnp.logical_and(t >= 2, t < 2 + first))
        def _():
            add_line_b(t - 2)

        @pl.when(jnp.logical_and(is_inner, jnp.logical_and(t >= mid_lag, t < steps + mid_lag)))
        def _():
            add_mid(first + t - mid_lag)

        @pl.when(t >= line_lag)
        def _():
            add_line(first + t - line_lag)

        @pl.when(t == steps)
        def _():
            @pl.loop(0, first)
            def _(c):
                add_last_b(c)

        @pl.when(t == quad_at)
        def _():
            third_copy(0).wait_recv()
            pick(mine_count >= SLOTS, p3, top, 0)
            t_copy().wait_recv()
            pick(heavy, yt, top, 0)
            start_x(dv, direct, chunks)

            @pl.loop(0, first)
            def _(c):
                xb_copy(c).start()

    total_row[...] = jnp.sum(norm[...], axis=0, keepdims=True)

    def n_copy(i):
        return remote(total_row, nbuf.at[i - 1], n_s, n_r, peer(i))

    for i in range(1, R * S):
        n_copy(i).start()
    by_copy().wait_recv()
    bf_copy().start()

    @pl.loop(first, chunks - 2)
    def _(c):
        forward(c)

    @pl.loop(0, first)
    def _(c):
        forward(c)

    @pl.loop(chunks - 2, chunks)
    def _(c):
        forward(c)

    sent(p3, p3_s)
    t_copy().wait_send()
    b3_copy().wait_send()
    base_twin().wait()
    ours = pl.ds(first, steps)
    sent(xin.at[ours], x_s)
    sent(xin_b, xb_s)

    @pl.when(is_outer)
    def _():
        sent(zq.at[ours], q_s)
        sent(qb, qb_s)

    @pl.when(is_inner)
    def _():
        sent(zin.at[ours], q_s)
        sent(zinb, qb_s)
        sent(comb.at[ours], far_s)
        sent(combb, farb_s)

    sent(mine, c_s)
    sent(mine, y_s)
    sent(mine, f_s)
    arrived(sums.at[twin], c_r)
    arrived(mine, f_r)
    by_copy().wait_send()
    bf_copy().wait()
    arrived(nbuf, n_r)
    sent(nbuf, n_s)
    total = total_row[...]
    for i in range(1, R * S):
        total = total + nbuf[i - 1]
    tot[...] = jnp.broadcast_to(total, (8, 128)) * jnp.where(
        lax.broadcasted_iota(jnp.int32, (8, 128), 0) == 0, 1.0, 0.0
    )


def finish_kernel(
    R, units,
    owner_in, tot, master, momentum, sums, bases,
    master_out, momentum_out, params,
    owner, owner_s, ms, mm, su, pb, ps,
    a_s, b_s, u_s, p_s, q_s, oa_s, ob_s, op_s,
):
    blocks = owner.shape[1]
    cols = master.shape[1]
    half = BLOCK_ROWS // 2
    me_s = lax.axis_index("shard")
    get_owner = pltpu.make_async_copy(owner_in, owner, owner_s)
    get_owner.start()

    def unit(shard, place, h):
        if units == 2 * SLOTS:
            return shard * units + 2 * place + h
        moved = shard + jnp.where(place == SLOTS - 1, 1 - 2 * (shard % 2), 0)
        if h:
            moved = moved + jnp.where(moved // 2 == 0, 2, -2)
        return jnp.where(place < 2, shard * units + 2 * place + h, moved * units + units - 1)

    def slot_rows(j):
        return pl.ds(pl.multiple_of(j * BLOCK_ROWS, BLOCK_ROWS), BLOCK_ROWS)

    def get_slot(j):
        return [
            pltpu.make_async_copy(master.at[slot_rows(j)], ms.at[slot_rows(j)], a_s.at[j]),
            pltpu.make_async_copy(momentum.at[slot_rows(j)], mm.at[slot_rows(j)], b_s.at[j]),
        ] + [
            pltpu.make_async_copy(sums.at[unit(me_s, j, h)], su.at[2 * j + h], u_s.at[2 * j + h]) for h in range(2)
        ]

    def put_slot(j):
        return [
            pltpu.make_async_copy(ms.at[slot_rows(j)], master_out.at[slot_rows(j)], oa_s.at[j]),
            pltpu.make_async_copy(mm.at[slot_rows(j)], momentum_out.at[slot_rows(j)], ob_s.at[j]),
        ]

    def get_block(b):
        shard = owner[0, b]
        place = sum(jnp.where(jnp.logical_and(owner[0, k] == shard, k < b), 1, 0) for k in range(blocks))
        return [pltpu.make_async_copy(bases.at[shard * SLOTS + place], pb.at[b], p_s.at[b])] + [
            pltpu.make_async_copy(sums.at[unit(shard, place, h)], ps.at[2 * b + h], q_s.at[2 * b + h])
            for h in range(2)
        ]

    def put_block(b):
        return pltpu.make_async_copy(pb.at[b], params.at[slot_rows(b)], op_s.at[b])

    @pl.loop(0, SLOTS)
    def _(j):
        for copy in get_slot(j):
            copy.start()

    get_owner.wait()
    count = shard_count(owner, me_s)

    @pl.loop(0, blocks)
    def _(b):
        for copy in get_block(b):
            copy.start()

    total = jnp.sum(jnp.sum(tot[...], axis=1, keepdims=True), axis=0, keepdims=True)
    limit = 0.5 * jnp.sqrt(jnp.full((1, 1), blocks * BLOCK_ROWS * R * cols, F32))
    factor = jnp.minimum(1.0, limit / (jnp.sqrt(total) + 1e-06))

    @pl.loop(0, SLOTS)
    def _(j):
        for copy in get_slot(j):
            copy.wait()

        @pl.when(j < count)
        def _():
            for h in range(2):
                @pl.loop(0, half // 16)
                def _(r):
                    at = pl.ds(pl.multiple_of(j * BLOCK_ROWS + h * half + r * 16, 16), 16)
                    grad = factor * su[2 * j + h, pl.ds(pl.multiple_of(r * 16, 16), 16), :].astype(F32)
                    fresh = 0.9 * mm[at, :] + grad
                    mm[at, :] = fresh
                    ms[at, :] = ms[at, :] - 0.7 * (grad + 0.9 * fresh)

        for copy in put_slot(j):
            copy.start()

    @pl.loop(0, blocks)
    def _(b):
        for copy in get_block(b):
            copy.wait()
        for h in range(2):
            @pl.loop(0, half // 16)
            def _(r):
                at = pl.ds(pl.multiple_of(h * half + r * 16, 16), 16)
                grad = factor * ps[2 * b + h, pl.ds(pl.multiple_of(r * 16, 16), 16), :].astype(F32)
                pb[b, at, :] = (pb[b, at, :].astype(F32) - 1.33 * grad).astype(BF16)

        put_block(b).start()

    @pl.loop(0, SLOTS)
    def _(j):
        for copy in put_slot(j):
            copy.wait()

    @pl.loop(0, blocks)
    def _(b):
        put_block(b).wait()


def close_kernel(
    R, units, held,
    owner_in, tot, master, momentum, sums, bases,
    master_out, momentum_out, params,
    owner, ms, mm, pb, owner_s, a_s, b_s, p_s,
):
    blocks = owner.shape[1]
    cols = master.shape[1]
    half = BLOCK_ROWS // 2
    me_s = lax.axis_index("shard")
    get_owner = pltpu.make_async_copy(owner_in, owner, owner_s)
    get_owner.start()

    def unit(shard, place, h):
        moved = shard + jnp.where(place == SLOTS - 1, 1 - 2 * (shard % 2), 0)
        if h:
            moved = moved + jnp.where(moved // 2 == 0, 2, -2)
        return jnp.where(place < 2, shard * units + 2 * place + h, moved * units + units - 1)

    def slot_rows(j):
        return pl.ds(pl.multiple_of(j * BLOCK_ROWS, BLOCK_ROWS), BLOCK_ROWS)

    def put_slot(j):
        return [
            pltpu.make_async_copy(ms.at[slot_rows(j)], master_out.at[slot_rows(j)], a_s.at[j]),
            pltpu.make_async_copy(mm.at[slot_rows(j)], momentum_out.at[slot_rows(j)], b_s.at[j]),
        ]

    def put_block(b):
        return pltpu.make_async_copy(pb.at[b], params.at[slot_rows(b)], p_s.at[b])

    total = jnp.sum(jnp.sum(tot[...], axis=1, keepdims=True), axis=0, keepdims=True)
    limit = 0.5 * jnp.sqrt(jnp.full((1, 1), blocks * BLOCK_ROWS * R * cols, F32))
    factor = jnp.minimum(1.0, limit / (jnp.sqrt(total) + 1e-06))
    get_owner.wait()
    count = shard_count(owner, me_s)

    @pl.loop(0, SLOTS)
    def _(j):
        for h in range(2):
            source = unit(me_s, j, h)

            @pl.loop(0, half // 16)
            def _(r):
                at = pl.ds(pl.multiple_of(j * BLOCK_ROWS + h * half + r * 16, 16), 16)
                old, before = master[at, :], momentum[at, :]
                grad = factor * sums[source, pl.ds(pl.multiple_of(r * 16, 16), 16), :].astype(F32)
                fresh = 0.9 * before + grad
                live = spread(j < count, old.shape)
                mm[at, :] = jnp.where(live, fresh, before)
                ms[at, :] = jnp.where(live, old - 0.7 * (grad + 0.9 * fresh), old)

        for copy in put_slot(j):
            copy.start()

    @pl.loop(0, blocks)
    def _(b):
        shard = owner[0, b]
        place = sum(jnp.where(jnp.logical_and(owner[0, k] == shard, k < b), 1, 0) for k in range(blocks))
        kept = jnp.where(place < held, shard * held + place, (shard + 1 - 2 * (shard % 2)) * held + held - 1)
        for h in range(2):
            source = unit(shard, place, h)

            @pl.loop(0, half // 16)
            def _(r):
                at = pl.ds(pl.multiple_of(h * half + r * 16, 16), 16)
                grad = factor * sums[source, pl.ds(pl.multiple_of(r * 16, 16), 16), :].astype(F32)
                pb[b, at, :] = (bases[kept, at, :].astype(F32) - 1.33 * grad).astype(BF16)

        put_block(b).start()

    @pl.loop(0, SLOTS)
    def _(j):
        for copy in put_slot(j):
            copy.wait()

    @pl.loop(0, blocks)
    def _(b):
        put_block(b).wait()


def on_device(deltas, master, momentum, block_owner):
    R, S = lax.axis_size("replica"), lax.axis_size("shard")
    width, cols = deltas.shape[2], master.shape[1]
    blocks = block_owner.shape[0]
    block_owner = block_owner.reshape(1, blocks)
    half = BLOCK_ROWS // 2
    quad = S == 4 and blocks - SLOTS - (S - 2) <= 2
    rows = 2 * BLOCK_ROWS + half if quad else SLOTS * BLOCK_ROWS
    rc = half
    while rc > 16 and (rows // (rc // 2)) * R <= 160:
        rc //= 2
    chunks = rows // rc
    units = rows // half
    Z, O = R // 2, S // 2
    loads = rows // BLOCK_ROWS + (1 if quad else 0)

    dma = pltpu.SemaphoreType.DMA
    vmem = pltpu.VMEM
    anywhere = pl.BlockSpec(memory_space=pl.ANY)
    in_vmem = pl.BlockSpec(memory_space=pltpu.VMEM)
    in_hbm = pl.BlockSpec(memory_space=pltpu.HBM)
    in_smem = pl.BlockSpec(memory_space=pltpu.SMEM)
    tree = quad and Z == 4 and O == 2
    if tree:
        held = SLOTS - 1
        first = chunks // 5
        steps = chunks - first
        piece = (rc, cols)
        sums, bases, tot, ms, mm = pl.pallas_call(
            functools.partial(tree_kernel, R, S, rows, rc, first),
            out_shape=(
                jax.ShapeDtypeStruct((S, chunks, rc, cols), BF16),
                jax.ShapeDtypeStruct((S, held * BLOCK_ROWS, cols), BF16),
                jax.ShapeDtypeStruct((8, 128), F32),
                jax.ShapeDtypeStruct(master.shape, F32),
                jax.ShapeDtypeStruct(master.shape, F32),
            ),
            in_specs=[in_hbm] * 4,
            out_specs=(in_vmem,) * 5,
            scratch_shapes=[
                vmem(block_owner.shape, jnp.int32),
                vmem((loads * BLOCK_ROWS, width), BF16),
                vmem((BLOCK_ROWS, width), BF16),
                vmem((half, width), BF16),
                vmem((BLOCK_ROWS, cols), BF16),
                vmem((BLOCK_ROWS, cols), BF16),
                vmem((chunks, Z) + piece, BF16),
                vmem((chunks, Z) + piece, BF16),
                vmem((chunks, 3) + piece, BF16),
                vmem((chunks, 2) + piece, BF16),
                vmem((chunks,) + piece, BF16),
                vmem((first, 3, 2) + piece, BF16),
                vmem((first, 2, 2) + piece, BF16),
                vmem((first, 2) + piece, BF16),
                vmem((first,) + piece, BF16),
                vmem((first,) + piece, F32),
                vmem((first,) + piece, BF16),
                vmem((8, 128), F32),
                vmem((1, 128), F32),
                vmem((R * S - 1, 1, 128), F32),
                dma, dma((loads,)), dma((2,)), dma, dma((2,)), dma, dma,
                dma, dma((steps,)), dma, dma((steps,)), dma((steps,)), dma, dma((steps,)),
                dma, dma((first, 2)), dma, dma((first,)), dma, dma((first,)),
                dma, dma, dma, dma((chunks,)), dma, dma,
                dma, dma, dma, dma, dma, dma, dma, dma, dma, dma,
            ],
            compiler_params=pltpu.CompilerParams(
                collective_id=0, has_side_effects=True, vmem_limit_bytes=SYNC_VMEM
            ),
            name="sync",
        )(*(pltpu.with_memory_space_constraint(a, pltpu.HBM) for a in (block_owner, deltas, master, momentum)))
        return tuple(pl.pallas_call(
            functools.partial(close_kernel, R, units, held),
            out_shape=(
                jax.ShapeDtypeStruct(master.shape, F32),
                jax.ShapeDtypeStruct(master.shape, F32),
                jax.ShapeDtypeStruct((blocks * BLOCK_ROWS, cols), BF16),
            ),
            in_specs=[in_vmem] * 6,
            out_specs=(in_hbm,) * 3,
            scratch_shapes=[
                pltpu.SMEM((1, blocks), jnp.int32),
                vmem(master.shape, F32),
                vmem(master.shape, F32),
                vmem((blocks, BLOCK_ROWS, cols), BF16),
                dma, dma((SLOTS,)), dma((SLOTS,)), dma((blocks,)),
            ],
            compiler_params=pltpu.CompilerParams(vmem_limit_bytes=CLOSE_VMEM),
            name="close",
        )(block_owner, tot, ms, mm, sums.reshape(S * units, half, cols),
          bases.reshape(S * held, BLOCK_ROWS, cols)))

    ys, zs = max(O - 1, 1), max(Z - 1, 1)
    sums, bases, tot = pl.pallas_call(
        functools.partial(sync_kernel, R, S, rows, rc),
        out_shape=(
            jax.ShapeDtypeStruct((S, chunks, rc, cols), BF16),
            jax.ShapeDtypeStruct((S,) + master.shape, BF16),
            jax.ShapeDtypeStruct((8, 128), F32),
        ),
        in_specs=[in_vmem, anywhere, anywhere, anywhere],
        out_specs=(anywhere, anywhere, in_vmem),
        scratch_shapes=[
            vmem((loads * BLOCK_ROWS, width), BF16),
            vmem((BLOCK_ROWS, width) if quad else (16, 128), BF16),
            vmem((half, width) if quad else (16, 128), BF16),
            vmem(master.shape, F32),
            vmem(master.shape, F32),
            vmem(master.shape, BF16),
            vmem((chunks, Z, rc, cols), BF16),
            vmem((chunks, Z, rc, cols), BF16),
            vmem((chunks, zs, rc, cols), BF16),
            vmem((chunks, rc, cols), BF16),
            vmem((2, 8, 128), F32),
            vmem((R - 1, 8, 128), F32),
            vmem((S - 1, 8, 128), F32),
            dma((loads,)), dma((2,)), dma((2,)), dma((2,)), dma, dma,
            dma((chunks, Z)), dma((chunks, Z)),
            dma((chunks, zs)), dma((chunks, zs)),
            dma((chunks,)), dma((chunks,)), dma((chunks,)),
            dma((ys, chunks)), dma((ys, chunks)), dma((ys, chunks)), dma((ys, chunks)),
            dma, dma, dma,
            dma((ys,)), dma((ys,)), dma((ys,)), dma((ys,)),
            dma((R - 1,)), dma((R - 1,)), dma((S - 1,)), dma((S - 1,)),
        ],
        compiler_params=pltpu.CompilerParams(
            collective_id=0, has_side_effects=True, vmem_limit_bytes=VMEM_LIMIT
        ),
        name="sync",
    )(block_owner, deltas, master, momentum)

    return tuple(pl.pallas_call(
        functools.partial(finish_kernel, R, units),
        out_shape=(
            jax.ShapeDtypeStruct(master.shape, F32),
            jax.ShapeDtypeStruct(master.shape, F32),
            jax.ShapeDtypeStruct((blocks * BLOCK_ROWS, cols), BF16),
        ),
        in_specs=[in_vmem, in_vmem] + [anywhere] * 4,
        out_specs=(anywhere,) * 3,
        scratch_shapes=[
            pltpu.SMEM((1, blocks), jnp.int32), dma,
            vmem(master.shape, F32),
            vmem(master.shape, F32),
            vmem((2 * SLOTS, half, cols), BF16),
            vmem((blocks, BLOCK_ROWS, cols), BF16),
            vmem((2 * blocks, half, cols), BF16),
            dma((SLOTS,)), dma((SLOTS,)), dma((2 * SLOTS,)), dma((blocks,)), dma((2 * blocks,)),
            dma((SLOTS,)), dma((SLOTS,)), dma((blocks,)),
        ],
        compiler_params=pltpu.CompilerParams(vmem_limit_bytes=VMEM_LIMIT),
        name="finish",
    )(block_owner, tot, master, momentum, sums.reshape(S * units, half, cols),
      bases.reshape(S * SLOTS, BLOCK_ROWS, cols)))


def solution(mesh):
    return jax.shard_map(
        on_device,
        mesh=mesh,
        in_specs=(P("replica", "shard", None), P("shard", "replica"), P("shard", "replica"), P()),
        out_specs=(P("shard", "replica"), P("shard", "replica"), P(None, "replica")),
        check_vma=False,
    )
```

```python
import functools

import jax
import jax.numpy as jnp
from jax import lax
from jax.experimental import pallas as pl
from jax.experimental.pallas import tpu as pltpu
from jax.sharding import PartitionSpec as P

BLOCK_ROWS = 128
SLOTS = 4
F32 = jnp.float32
BF16 = jnp.bfloat16
VMEM_LIMIT = 56 * 1024 * 1024
SYNC_VMEM = 26 * 1024 * 1024
CLOSE_VMEM = 12 * 1024 * 1024


def remote(src, dst, send, recv, device):
    return pltpu.make_async_remote_copy(
        src_ref=src, dst_ref=dst, send_sem=send, recv_sem=recv,
        device_id=device, device_id_type=pl.DeviceIdType.MESH,
    )


def shard_count(owner, shard):
    return sum(jnp.where(owner[0, b] == shard, 1, 0) for b in range(owner.shape[1]))


def spread(condition, shape):
    return jnp.broadcast_to(jnp.where(condition, 1, 0), shape) != 0


def sync_kernel(
    R, S, rows, rc,
    owner, deltas, master, momentum,
    sums, bases, tot,
    dv, p3, yt, ms, mm, base, xin, pair, zin, mine, norm, nbuf, sbuf,
    ld, lm, p3_s, p3_r, t_s, t_r, x_s, x_r, z_s, z_r, l_s, c_s, c_r, y_s, y_r, f_s, f_r,
    bl_s, bc_s, bc_r, by_s, by_r, bf_s, bf_r, n_s, n_r, m_s, m_r,
):
    width = deltas.shape[2]
    cols = width // R
    Z, O = R // 2, S // 2
    per = BLOCK_ROWS // rc
    half = BLOCK_ROWS // 2
    chunks = rows // rc
    quad = rows < SLOTS * BLOCK_ROWS
    whole = rows // BLOCK_ROWS
    direct = whole * per
    top = whole * BLOCK_ROWS
    me_r, me_s = lax.axis_index("replica"), lax.axis_index("shard")
    z, x = me_r // 2, me_r % 2
    o, core = me_s // 2, me_s % 2
    x_peer = z * 2 + 1 - x
    twin = o * 2 + 1 - core

    barrier = pltpu.get_barrier_semaphore()
    for i in range(1, R):
        pl.semaphore_signal(barrier, inc=1, device_id=((me_r + i) % R, me_s), device_id_type=pl.DeviceIdType.MESH)
    for i in range(1, S):
        pl.semaphore_signal(barrier, inc=1, device_id=(me_r, (me_s + i) % S), device_id_type=pl.DeviceIdType.MESH)

    def load(k):
        part = pl.ds(k * BLOCK_ROWS, BLOCK_ROWS)
        return pltpu.make_async_copy(deltas.at[0, part, :], dv.at[part, :], ld.at[k])

    if quad:
        load(whole).start()
    for k in range(whole):
        load(k).start()
    load_master = pltpu.make_async_copy(master, ms, lm.at[0])
    load_momentum = pltpu.make_async_copy(momentum, mm, lm.at[1])
    load_master.start()
    load_momentum.start()
    mine_count = jnp.sum(jnp.where(owner[...] == me_s, 1, 0), axis=1, keepdims=True)
    twin_count = jnp.sum(jnp.where(owner[...] == twin, 1, 0), axis=1, keepdims=True)
    heavy = jnp.maximum(mine_count, twin_count) >= SLOTS
    pl.semaphore_wait(barrier, R + S - 2)

    def rows_of(c):
        return pl.ds(pl.multiple_of(c * rc, rc), rc)

    def columns(c, j, side):
        return pl.ds(pl.multiple_of((((z + 1 + j) % Z) * 2 + side) * cols, cols), cols)

    def x_copy(source, c, j):
        return remote(
            source.at[rows_of(c), columns(c, j, 1 - x)], xin.at[c, j], x_s.at[c, j], x_r.at[c, j], (x_peer, me_s)
        )

    def z_copy(c, j):
        return remote(
            pair.at[c, j], zin.at[c, j], z_s.at[c, j], z_r.at[c, j], (((z + 1 + j) % Z) * 2 + x, me_s)
        )

    def c_copy(c):
        return remote(mine.at[c], sums.at[me_s, c], c_s.at[c], c_r.at[c], (me_r, twin))

    def l_copy(c):
        return pltpu.make_async_copy(mine.at[c], sums.at[me_s, c], l_s.at[c])

    def y_copy(i, c):
        return remote(
            mine.at[c], sums.at[me_s, c], y_s.at[i - 1, c], y_r.at[i - 1, c], (me_r, ((o + i) % O) * 2 + core)
        )

    def f_copy(i, c):
        source = ((o + O - i) % O) * 2 + core
        return remote(sums.at[source, c], sums.at[source, c], f_s.at[i - 1, c], f_r.at[i - 1, c], (me_r, twin))

    def by_copy(i):
        return remote(base, bases.at[me_s], by_s.at[i - 1], by_r.at[i - 1], (me_r, ((o + i) % O) * 2 + core))

    def bf_copy(i):
        source = ((o + O - i) % O) * 2 + core
        return remote(bases.at[source], bases.at[source], bf_s.at[i - 1], bf_r.at[i - 1], (me_r, twin))

    def third_copy(h):
        return remote(
            deltas.at[0, pl.ds((SLOTS - 1) * BLOCK_ROWS + h * half, half), :],
            p3.at[pl.ds(h * half, half), :], p3_s.at[h], p3_r.at[h], (me_r, twin),
        )

    def t_copy():
        return remote(dv.at[pl.ds(top + half, half), :], yt, t_s, t_r, (me_r, ((o + 1) % O) * 2 + core))

    def base_twin():
        return remote(base, bases.at[me_s], bc_s, bc_r, (me_r, twin))

    def base_local():
        return pltpu.make_async_copy(base, bases.at[me_s], bl_s)

    def start_x(source, low, high):
        @pl.loop(low, high)
        def _(c):
            for j in range(Z):
                x_copy(source, c, j).start()

    def pick(condition, other, start, other_start):
        @pl.loop(0, half // 16)
        def _(r):
            keep = spread(condition, (16, 1024))
            for q in range(width // 1024):
                at = (pl.ds(pl.multiple_of(start + r * 16, 16), 16), pl.ds(q * 1024, 1024))
                there = (pl.ds(pl.multiple_of(other_start + r * 16, 16), 16), pl.ds(q * 1024, 1024))
                dv[at] = jnp.where(keep, dv[at].astype(F32), other[there].astype(F32)).astype(BF16)

    if quad:
        third_copy(1).start()
        third_copy(0).start()
    start_x(deltas.at[0], 0, direct)
    norm[0] = jnp.zeros((8, 128), F32)

    def send_third():
        load(whole).wait()
        third_copy(1).wait_recv()
        pick(mine_count >= SLOTS, p3, top + half, half)
        t_copy().start()

    def make_base():
        load_master.wait()
        load_momentum.wait()

        @pl.loop(0, SLOTS * BLOCK_ROWS // 16)
        def _(r):
            at = pl.ds(pl.multiple_of(r * 16, 16), 16)
            base[at, :] = (ms[at, :] - 0.567 * mm[at, :]).astype(BF16)

        for i in range(1, O):
            by_copy(i).start()
        base_twin().start()
        base_local().start()

    def add_pair(c):
        @pl.when(c % per == 0)
        def _():
            @pl.when(c < direct)
            def _():
                load(c // per).wait()

        for j in range(Z):
            x_copy(deltas.at[0], c, j).wait_recv()
            pair[c, j] = (xin[c, j].astype(F32) + dv[rows_of(c), columns(c, j, x)].astype(F32)).astype(BF16)
            if j < Z - 1:
                z_copy(c, j).start()

    def add_line(c):
        for j in range(Z - 1):
            z_copy(c, j).wait_recv()
        place = jnp.where(c >= direct, -1, c // per) if quad else c // per
        live = spread(place < mine_count, (8, 128))
        part = jnp.zeros((8, 128), F32)
        for r in range(0, rc, 16):
            total = pair[c, Z - 1, r:r + 16, :].astype(F32)
            for j in range(Z - 1):
                total = total + zin[c, j, r:r + 16, :].astype(F32)
            total = total / R
            mine[c, r:r + 16, :] = total.astype(BF16)
            for h in range(0, 16, 8):
                for q in range(0, cols, 128):
                    v = total[h:h + 8, q:q + 128]
                    part = part + v * v
        norm[0] = norm[0] + jnp.where(live, part, 0.0)
        for i in range(1, O):
            y_copy(i, c).start()
        c_copy(c).start()
        l_copy(c).start()

    def forward(c):
        for i in range(1, O):
            y_copy(i, c).wait_recv()
            f_copy(i, c).start()

    lag = 4

    @pl.loop(0, chunks + lag)
    def _(t):
        @pl.when(t < chunks)
        def _():
            add_pair(t)

        @pl.when(t >= lag)
        def _():
            add_line(t - lag)

        @pl.when(t == 2)
        def _():
            make_base()

        if quad:
            @pl.when(t == 0)
            def _():
                send_third()

            @pl.when(t == direct - direct // 4)
            def _():
                third_copy(0).wait_recv()
                pick(mine_count >= SLOTS, p3, top, 0)
                t_copy().wait_recv()
                pick(heavy, yt, top, 0)
                start_x(dv, direct, chunks)

    def n_copy(i):
        return remote(norm.at[0], nbuf.at[i - 1], n_s.at[i - 1], n_r.at[i - 1], ((me_r + i) % R, me_s))

    def m_copy(i):
        return remote(norm.at[1], sbuf.at[i - 1], m_s.at[i - 1], m_r.at[i - 1], (me_r, (me_s + i) % S))

    for i in range(1, R):
        n_copy(i).start()
    for i in range(1, O):
        by_copy(i).wait_recv()
        bf_copy(i).start()

    @pl.loop(0, chunks - 2)
    def _(c):
        forward(c)
        for j in range(Z):
            x_copy(deltas.at[0], c, j).wait_send()
        for j in range(Z - 1):
            z_copy(c, j).wait_send()

    total = norm[0]
    for i in range(1, R):
        n_copy(i).wait_recv()
        total = total + nbuf[i - 1]
    norm[1] = total
    for i in range(1, S):
        m_copy(i).start()

    @pl.loop(chunks - 2, chunks)
    def _(c):
        forward(c)

    for i in range(1, S):
        m_copy(i).wait_recv()
        total = total + sbuf[i - 1]
    tot[...] = total

    if quad:
        third_copy(0).wait_send()
        third_copy(1).wait_send()
        t_copy().wait_send()
    base_local().wait()
    base_twin().wait()
    for i in range(1, O):
        by_copy(i).wait_send()
        bf_copy(i).wait()
    for i in range(1, R):
        n_copy(i).wait_send()
    for i in range(1, S):
        m_copy(i).wait_send()

    @pl.loop(chunks - 2, chunks)
    def _(c):
        for j in range(Z):
            x_copy(deltas.at[0], c, j).wait_send()
        for j in range(Z - 1):
            z_copy(c, j).wait_send()

    @pl.loop(0, chunks)
    def _(c):
        l_copy(c).wait()
        c_copy(c).wait()
        for i in range(1, O):
            y_copy(i, c).wait_send()
            f_copy(i, c).wait()


def tree_kernel(
    R, S, rows, rc, first,
    owner_in, deltas, master, momentum,
    sums, bases, tot, ms, mm,
    owner, dv, p3, yt, b3, b3_in,
    xin, pair, zq, comb, zin, qb, combb, zinb, part_b, keep_b, xin_b, norm, total_row, nbuf,
    lo, ld, lm, p3_s, p3_r, t_s, t_r, x_s, x_r, q_s, qa_r, qc_r, far_s, far_r,
    qb_s, qb_r, farb_s, farb_r, xb_s, xb_r,
    c_s, c_r, y_s, y_r, f_s, f_r,
    b3_s, b3_r, bc_s, bc_r, by_s, by_r, bf_s, bf_r, n_s, n_r, go,
):
    width = deltas.shape[2]
    cols = width // R
    Z = R // 2
    per = BLOCK_ROWS // rc
    half = BLOCK_ROWS // 2
    chunks = rows // rc
    whole = rows // BLOCK_ROWS
    direct = whole * per
    top = whole * BLOCK_ROWS
    mid_lag, line_lag, late = 2, 4, 6
    last = max(line_lag, late)
    steps = chunks - first
    me_r, me_s = lax.axis_index("replica"), lax.axis_index("shard")
    z, x = me_r // 2, me_r % 2
    o, core = me_s // 2, me_s % 2
    side = z // 2
    inner = (z + side) % 2
    outer = 1 - inner
    is_inner, is_outer = inner == 1, inner == 0
    x_peer = (z * 2 + 1 - x, me_s)
    near = ((side * 2 + 1 - z % 2) * 2 + x, me_s)
    far_outer = ((Z - 1) * (1 - side) * 2 + x, me_s)
    far_inner = ((Z - 1 - z) * 2 + x, me_s)
    twin = o * 2 + 1 - core
    twin_device = (me_r, twin)
    y_shard = (1 - o) * 2 + core
    y_device = (me_r, y_shard)

    barrier = pltpu.get_barrier_semaphore()
    me = me_r * S + me_s

    def peer(i):
        other = (me + i) % (R * S)
        return (other // S, other % S)

    def greet(device):
        pl.semaphore_signal(barrier, inc=1, device_id=device, device_id_type=pl.DeviceIdType.MESH)

    for device in (x_peer, near, twin_device, y_device):
        greet(device)

    @pl.when(is_inner)
    def _():
        greet(far_inner)

    def load(k):
        part = pl.ds(k * BLOCK_ROWS, BLOCK_ROWS)
        return pltpu.make_async_copy(deltas.at[0, part, :], dv.at[part, :], ld.at[k])

    load(whole).start()
    load_owner = pltpu.make_async_copy(owner_in, owner, lo)
    load_owner.start()
    load_master = pltpu.make_async_copy(master, ms, lm.at[0])
    load_momentum = pltpu.make_async_copy(momentum, mm, lm.at[1])
    load_master.start()
    load_momentum.start()
    for k in range(whole):
        load(k).start()
    norm[...] = jnp.zeros((8, 128), F32)
    pl.semaphore_wait(barrier, 4 + inner)

    @pl.when(is_inner)
    def _():
        pl.semaphore_signal(go, inc=1, device_id=far_inner, device_id_type=pl.DeviceIdType.MESH)

    mine, base = sums.at[me_s], bases.at[me_s]

    def rows_of(c):
        return pl.ds(pl.multiple_of(c * rc, rc), rc)

    def columns(k, side_x):
        e = (Z - k - outer) % Z
        d = e + side * (Z - 1 - 2 * e)
        return pl.ds(pl.multiple_of((d * 2 + side_x) * cols, cols), cols)

    def arrived(ref, sem):
        remote(ref, ref, n_s, sem, twin_device).wait_recv()

    def sent(ref, sem):
        remote(ref, ref, sem, n_r, twin_device).wait_send()

    def x_copy(source, c, k):
        return remote(source.at[rows_of(c), columns(k, 1 - x)], xin.at[c, k], x_s, x_r.at[c - first, k // 2], x_peer)

    def start_q(c, k):
        if k == 0:
            @pl.when(is_inner)
            def _():
                remote(pair.at[c, 0], zq.at[c, 2], q_s, qc_r.at[c - first], near).start()

        @pl.when(is_outer)
        def _():
            remote(pair.at[c, k], zq.at[c, k], q_s, (qc_r if k == 2 else qa_r).at[c - first], near).start()

    def far_copy(c, i):
        return remote(comb.at[c, i], zin.at[c], far_s, far_r.at[c - first], far_inner if i else far_outer)

    def half_x(v):
        return x if v else 1 - x

    def start_qb(c):
        def start(v, k, slot):
            remote(
                deltas.at[0, rows_of(c), columns(k, half_x(v))], qb.at[c, slot, v],
                qb_s, qb_r.at[c, slot // 2], near,
            ).start()

        @pl.when(is_inner)
        def _():
            for v in range(2):
                start(v, 0, 2)

        @pl.when(is_outer)
        def _():
            for k in range(Z - 1):
                for v in range(2):
                    start(v, k, k)

    def farb_copy(c, v, i):
        return remote(combb.at[c, v, i], zinb.at[c, v], farb_s, farb_r.at[c], far_inner if i else far_outer)

    def xb_copy(c):
        return remote(part_b.at[c], xin_b.at[c], xb_s, xb_r.at[c], x_peer)

    def c_copy(c):
        return remote(mine.at[c], sums.at[me_s, c], c_s, c_r, twin_device)

    def y_copy(c):
        return remote(mine.at[c], sums.at[me_s, c], y_s, y_r.at[c], y_device)

    def f_copy(c):
        return remote(sums.at[y_shard, c], sums.at[y_shard, c], f_s, f_r, twin_device)

    def by_copy(i):
        part = pl.ds(i * BLOCK_ROWS, BLOCK_ROWS * (SLOTS - 2 if i else 1))
        return remote(base.at[part], bases.at[me_s, part], by_s.at[i], by_r.at[i], y_device)

    def bf_copy():
        return remote(bases.at[y_shard], bases.at[y_shard], bf_s, bf_r, twin_device)

    def b3_copy():
        return remote(b3, b3_in, b3_s, b3_r, twin_device)

    def base_twin():
        return remote(base, bases.at[me_s], bc_s, bc_r, twin_device)

    def third_copy(h):
        return remote(
            deltas.at[0, pl.ds((SLOTS - 1) * BLOCK_ROWS + h * half, half), :],
            p3.at[pl.ds(h * half, half), :], p3_s, p3_r.at[h], twin_device,
        )

    def t_copy():
        return remote(dv.at[pl.ds(top + half, half), :], yt, t_s, t_r, y_device)

    def start_x(source, low, high):
        @pl.loop(low, high)
        def _(c):
            for k in range(Z):
                x_copy(source, c, k).start()

    def pick(condition, other, start, other_start):
        @pl.loop(0, half // 16)
        def _(r):
            keep = spread(condition, (16, 1024))
            for q in range(width // 1024):
                at = (pl.ds(pl.multiple_of(start + r * 16, 16), 16), pl.ds(q * 1024, 1024))
                there = (pl.ds(pl.multiple_of(other_start + r * 16, 16), 16), pl.ds(q * 1024, 1024))
                dv[at] = jnp.where(keep, dv[at].astype(F32), other[there].astype(F32)).astype(BF16)

    third_copy(1).start()
    third_copy(0).start()
    start_x(deltas.at[0], first, first + 1)

    @pl.loop(0, first)
    def _(c):
        start_qb(c)

    start_x(deltas.at[0], first + 1, direct)

    def send_third():
        load(whole).wait()
        third_copy(1).wait_recv()
        pick(mine_count >= SLOTS, p3, top + half, half)
        t_copy().start()

    def start_base(low, high, target, target_start):
        @pl.loop(low * BLOCK_ROWS // 16, high * BLOCK_ROWS // 16)
        def _(r):
            at = pl.ds(pl.multiple_of(r * 16, 16), 16)
            to = pl.ds(pl.multiple_of(r * 16 - target_start, 16), 16)
            target[to, :] = (ms[at, :] - 0.567 * mm[at, :]).astype(BF16)

    def make_base():
        load_master.wait()
        load_momentum.wait()
        start_base(SLOTS - 1, SLOTS, b3, (SLOTS - 1) * BLOCK_ROWS)
        b3_copy().start()
        start_base(0, 1, base, 0)
        by_copy(0).start()
        start_base(1, SLOTS - 1, base, 0)

    def send_base():
        b3_copy().wait_recv()

        @pl.loop(0, BLOCK_ROWS // 16)
        def _(r):
            at = pl.ds(pl.multiple_of(top + r * 16, 16), 16)
            there = pl.ds(pl.multiple_of(r * 16, 16), 16)
            keep = spread(mine_count >= SLOTS, (16, cols))
            base[at, :] = jnp.where(keep, base[at, :].astype(F32), b3_in[there, :].astype(F32)).astype(BF16)

        by_copy(1).start()
        base_twin().start()

    def ready():
        @pl.loop(0, SLOTS * per)
        def _(r):
            at = pl.ds(pl.multiple_of(r * rc, rc), rc)
            old, before = ms[at, :], mm[at, :]
            live = spread(r // per < mine_count, old.shape)
            ms[at, :] = jnp.where(live, old - 0.567 * before, old)
            mm[at, :] = jnp.where(live, 0.9 * before, before)

    def add_pair(c):
        @pl.when(jnp.logical_and(c % per == 0, c < direct))
        def _():
            load(c // per).wait()

        for k in range(Z):
            if k % 2 == 0:
                arrived(xin.at[c, pl.ds(k, 2)], x_r.at[c - first, k // 2])
            pair[c, k] = (xin[c, k].astype(F32) + dv[rows_of(c), columns(k, x)].astype(F32)).astype(BF16)
            if k < 2:
                start_q(c, k)
            elif k == 2:
                @pl.when(c < chunks - late)
                def _():
                    start_q(c, k)

    def add_mid(c):
        arrived(zq.at[c, pl.ds(0, 2)], qa_r.at[c - first])
        for i in range(2):
            comb[c, i] = (pair[c, 1 + i].astype(F32) + zq[c, i].astype(F32)).astype(BF16)
            far_copy(c, i).start()

    def add_mid_b(c):
        arrived(qb.at[c, pl.ds(0, 2)], qb_r.at[c, 0])
        for v in range(2):
            for i in range(2):
                own = dv[rows_of(c), columns(1 + i, half_x(v))].astype(F32)
                combb[c, v, i] = (own + qb[c, i, v].astype(F32)).astype(BF16)
                farb_copy(c, v, i).start()

    def add_line_b(c):
        arrived(qb.at[c, 2], qb_r.at[c, 1])
        arrived(zinb.at[c], farb_r.at[c])
        for v in range(2):
            own = dv[rows_of(c), columns(Z - 1, half_x(v))].astype(F32)
            value = own + qb[c, 2, v].astype(F32) + zinb[c, v].astype(F32)
            if v:
                keep_b[c] = value
            else:
                part_b[c] = value.astype(BF16)

    def emit(c, get):
        place = jnp.where(c >= direct, -1, c // per)
        live = spread(place < mine_count, (8, 128))
        part = jnp.zeros((8, 128), F32)
        for r in range(0, rc, 16):
            total = get(r) / R
            mine[c, r:r + 16, :] = total.astype(BF16)
            for h in range(0, 16, 8):
                for q in range(0, cols, 128):
                    v = total[h:h + 8, q:q + 128]
                    part = part + v * v
        norm[...] = norm[...] + jnp.where(live, part, 0.0)
        y_copy(c).start()
        c_copy(c).start()

    def add_line(c):
        arrived(zq.at[c, 2], qc_r.at[c - first])
        arrived(zin.at[c], far_r.at[c - first])
        emit(c, lambda r: (
            pair[c, Z - 1, r:r + 16, :].astype(F32) + zq[c, 2, r:r + 16, :].astype(F32)
            + zin[c, r:r + 16, :].astype(F32)
        ))

    def add_last_b(c):
        xb_copy(c).wait_recv()
        emit(c, lambda r: keep_b[c, r:r + 16, :] + xin_b[c, r:r + 16, :].astype(F32))

    def forward(c):
        y_copy(c).wait_recv()
        f_copy(c).start()

    load_owner.wait()
    mine_count = jnp.sum(jnp.where(owner[...] == me_s, 1, 0), axis=1, keepdims=True)
    twin_count = jnp.sum(jnp.where(owner[...] == twin, 1, 0), axis=1, keepdims=True)
    heavy = jnp.maximum(mine_count, twin_count) >= SLOTS
    make_base()
    send_third()
    send_base()
    load(0).wait()

    quad_at = (direct - first) * 2 // 3

    @pl.when(is_inner)
    def _():
        pl.semaphore_wait(go, 1)

    @pl.loop(0, steps)
    def _(t):
        add_pair(first + t)

        @pl.when(jnp.logical_and(is_inner, t < first))
        def _():
            add_mid_b(t)

        @pl.when(jnp.logical_and(t >= 2, t < 2 + first))
        def _():
            add_line_b(t - 2)

        @pl.when(jnp.logical_and(is_inner, t >= mid_lag))
        def _():
            add_mid(first + t - mid_lag)

        @pl.when(jnp.logical_and(t >= line_lag, t - line_lag < steps - last))
        def _():
            add_line(first + t - line_lag)

        @pl.when(t == quad_at - 2)
        def _():
            ready()

        @pl.when(t == quad_at)
        def _():
            third_copy(0).wait_recv()
            pick(mine_count >= SLOTS, p3, top, 0)
            t_copy().wait_recv()
            pick(heavy, yt, top, 0)
            start_x(dv, direct, chunks)

            @pl.loop(0, first)
            def _(c):
                xb_copy(c).start()

    @pl.loop(chunks - late, chunks)
    def _(c):
        start_q(c, 2)

    @pl.when(is_inner)
    def _():
        @pl.loop(chunks - mid_lag, chunks)
        def _(c):
            add_mid(c)

    @pl.loop(0, first)
    def _(c):
        add_last_b(c)

    @pl.loop(chunks - last, chunks)
    def _(c):
        add_line(c)

    total_row[...] = jnp.sum(norm[...], axis=0, keepdims=True)

    def n_copy(i):
        return remote(total_row, nbuf.at[i - 1], n_s, n_r, peer(i))

    for i in range(1, R * S):
        n_copy(i).start()
    by_copy(0).wait_recv()
    by_copy(1).wait_recv()
    bf_copy().start()

    @pl.loop(first, chunks - 2)
    def _(c):
        forward(c)

    @pl.loop(0, first)
    def _(c):
        forward(c)

    @pl.loop(chunks - 2, chunks)
    def _(c):
        forward(c)

    sent(p3, p3_s)
    t_copy().wait_send()
    b3_copy().wait_send()
    base_twin().wait()
    ours = pl.ds(first, steps)
    sent(xin.at[ours], x_s)
    sent(xin_b, xb_s)

    @pl.when(is_outer)
    def _():
        sent(zq.at[ours], q_s)
        sent(qb, qb_s)

    @pl.when(is_inner)
    def _():
        sent(zin.at[ours], q_s)
        sent(zinb, qb_s)
        sent(comb.at[ours], far_s)
        sent(combb, farb_s)

    sent(mine, c_s)
    sent(mine, y_s)
    sent(mine, f_s)
    arrived(sums.at[twin], c_r)
    arrived(mine, f_r)
    by_copy(0).wait_send()
    by_copy(1).wait_send()
    bf_copy().wait()
    arrived(nbuf, n_r)
    sent(nbuf, n_s)
    total = total_row[...]
    for i in range(1, R * S):
        total = total + nbuf[i - 1]
    tot[...] = jnp.broadcast_to(total, (8, 128)) * jnp.where(
        lax.broadcasted_iota(jnp.int32, (8, 128), 0) == 0, 1.0, 0.0
    )


def finish_kernel(
    R, units,
    owner_in, tot, master, momentum, sums, bases,
    master_out, momentum_out, params,
    owner, owner_s, ms, mm, su, pb, ps,
    a_s, b_s, u_s, p_s, q_s, oa_s, ob_s, op_s,
):
    blocks = owner.shape[1]
    cols = master.shape[1]
    half = BLOCK_ROWS // 2
    me_s = lax.axis_index("shard")
    get_owner = pltpu.make_async_copy(owner_in, owner, owner_s)
    get_owner.start()

    def unit(shard, place, h):
        if units == 2 * SLOTS:
            return shard * units + 2 * place + h
        moved = shard + jnp.where(place == SLOTS - 1, 1 - 2 * (shard % 2), 0)
        if h:
            moved = moved + jnp.where(moved // 2 == 0, 2, -2)
        return jnp.where(place < 2, shard * units + 2 * place + h, moved * units + units - 1)

    def slot_rows(j):
        return pl.ds(pl.multiple_of(j * BLOCK_ROWS, BLOCK_ROWS), BLOCK_ROWS)

    def get_slot(j):
        return [
            pltpu.make_async_copy(master.at[slot_rows(j)], ms.at[slot_rows(j)], a_s.at[j]),
            pltpu.make_async_copy(momentum.at[slot_rows(j)], mm.at[slot_rows(j)], b_s.at[j]),
        ] + [
            pltpu.make_async_copy(sums.at[unit(me_s, j, h)], su.at[2 * j + h], u_s.at[2 * j + h]) for h in range(2)
        ]

    def put_slot(j):
        return [
            pltpu.make_async_copy(ms.at[slot_rows(j)], master_out.at[slot_rows(j)], oa_s.at[j]),
            pltpu.make_async_copy(mm.at[slot_rows(j)], momentum_out.at[slot_rows(j)], ob_s.at[j]),
        ]

    def get_block(b):
        shard = owner[0, b]
        place = sum(jnp.where(jnp.logical_and(owner[0, k] == shard, k < b), 1, 0) for k in range(blocks))
        return [pltpu.make_async_copy(bases.at[shard * SLOTS + place], pb.at[b], p_s.at[b])] + [
            pltpu.make_async_copy(sums.at[unit(shard, place, h)], ps.at[2 * b + h], q_s.at[2 * b + h])
            for h in range(2)
        ]

    def put_block(b):
        return pltpu.make_async_copy(pb.at[b], params.at[slot_rows(b)], op_s.at[b])

    @pl.loop(0, SLOTS)
    def _(j):
        for copy in get_slot(j):
            copy.start()

    get_owner.wait()
    count = shard_count(owner, me_s)

    @pl.loop(0, blocks)
    def _(b):
        for copy in get_block(b):
            copy.start()

    total = jnp.sum(jnp.sum(tot[...], axis=1, keepdims=True), axis=0, keepdims=True)
    limit = 0.5 * jnp.sqrt(jnp.full((1, 1), blocks * BLOCK_ROWS * R * cols, F32))
    factor = jnp.minimum(1.0, limit / (jnp.sqrt(total) + 1e-06))

    @pl.loop(0, SLOTS)
    def _(j):
        for copy in get_slot(j):
            copy.wait()

        @pl.when(j < count)
        def _():
            for h in range(2):
                @pl.loop(0, half // 16)
                def _(r):
                    at = pl.ds(pl.multiple_of(j * BLOCK_ROWS + h * half + r * 16, 16), 16)
                    grad = factor * su[2 * j + h, pl.ds(pl.multiple_of(r * 16, 16), 16), :].astype(F32)
                    fresh = 0.9 * mm[at, :] + grad
                    mm[at, :] = fresh
                    ms[at, :] = ms[at, :] - 0.7 * (grad + 0.9 * fresh)

        for copy in put_slot(j):
            copy.start()

    @pl.loop(0, blocks)
    def _(b):
        for copy in get_block(b):
            copy.wait()
        for h in range(2):
            @pl.loop(0, half // 16)
            def _(r):
                at = pl.ds(pl.multiple_of(h * half + r * 16, 16), 16)
                grad = factor * ps[2 * b + h, pl.ds(pl.multiple_of(r * 16, 16), 16), :].astype(F32)
                pb[b, at, :] = (pb[b, at, :].astype(F32) - 1.33 * grad).astype(BF16)

        put_block(b).start()

    @pl.loop(0, SLOTS)
    def _(j):
        for copy in put_slot(j):
            copy.wait()

    @pl.loop(0, blocks)
    def _(b):
        put_block(b).wait()


def close_kernel(
    R, units, held,
    owner_in, tot, master, momentum, sums, bases,
    master_out, momentum_out, params,
    owner, ms, mm, pb, owner_s, a_s, b_s, p_s,
):
    blocks = owner.shape[1]
    cols = master.shape[1]
    half = BLOCK_ROWS // 2
    me_s = lax.axis_index("shard")
    get_owner = pltpu.make_async_copy(owner_in, owner, owner_s)
    get_owner.start()

    def unit(shard, place, h):
        moved = shard + jnp.where(place == SLOTS - 1, 1 - 2 * (shard % 2), 0)
        if h:
            moved = moved + jnp.where(moved // 2 == 0, 2, -2)
        return jnp.where(place < 2, shard * units + 2 * place + h, moved * units + units - 1)

    def slot_rows(j):
        return pl.ds(pl.multiple_of(j * BLOCK_ROWS, BLOCK_ROWS), BLOCK_ROWS)

    def put_slot(j):
        return [
            pltpu.make_async_copy(ms.at[slot_rows(j)], master_out.at[slot_rows(j)], a_s.at[j]),
            pltpu.make_async_copy(mm.at[slot_rows(j)], momentum_out.at[slot_rows(j)], b_s.at[j]),
        ]

    def put_block(b):
        return pltpu.make_async_copy(pb.at[b], params.at[slot_rows(b)], p_s.at[b])

    total = jnp.sum(jnp.sum(tot[...], axis=1, keepdims=True), axis=0, keepdims=True)
    limit = 0.5 * jnp.sqrt(jnp.full((1, 1), blocks * BLOCK_ROWS * R * cols, F32))
    factor = jnp.minimum(1.0, limit / (jnp.sqrt(total) + 1e-06))
    get_owner.wait()
    count = shard_count(owner, me_s)

    @pl.loop(0, SLOTS)
    def _(j):
        for h in range(2):
            source = unit(me_s, j, h)

            @pl.loop(0, half // 16)
            def _(r):
                at = pl.ds(pl.multiple_of(j * BLOCK_ROWS + h * half + r * 16, 16), 16)
                part = factor * sums[source, pl.ds(pl.multiple_of(r * 16, 16), 16), :].astype(F32)
                grad = jnp.where(spread(j < count, part.shape), part, 0.0)
                mm[at, :] = momentum[at, :] + grad
                ms[at, :] = master[at, :] - 1.33 * grad

        for copy in put_slot(j):
            copy.start()

    @pl.loop(0, blocks)
    def _(b):
        shard = owner[0, b]
        place = sum(jnp.where(jnp.logical_and(owner[0, k] == shard, k < b), 1, 0) for k in range(blocks))
        kept = jnp.where(place < held, shard * held + place, (shard + 1 - 2 * (shard % 2)) * held + held - 1)
        for h in range(2):
            source = unit(shard, place, h)

            @pl.loop(0, half // 16)
            def _(r):
                at = pl.ds(pl.multiple_of(h * half + r * 16, 16), 16)
                grad = factor * sums[source, pl.ds(pl.multiple_of(r * 16, 16), 16), :].astype(F32)
                pb[b, at, :] = (bases[kept, at, :].astype(F32) - 1.33 * grad).astype(BF16)

        put_block(b).start()

    @pl.loop(0, SLOTS)
    def _(j):
        for copy in put_slot(j):
            copy.wait()

    @pl.loop(0, blocks)
    def _(b):
        put_block(b).wait()


def on_device(deltas, master, momentum, block_owner):
    R, S = lax.axis_size("replica"), lax.axis_size("shard")
    width, cols = deltas.shape[2], master.shape[1]
    blocks = block_owner.shape[0]
    block_owner = block_owner.reshape(1, blocks)
    half = BLOCK_ROWS // 2
    quad = S == 4 and blocks - SLOTS - (S - 2) <= 2
    rows = 2 * BLOCK_ROWS + half if quad else SLOTS * BLOCK_ROWS
    rc = half
    while rc > 16 and (rows // (rc // 2)) * R <= 160:
        rc //= 2
    chunks = rows // rc
    units = rows // half
    Z, O = R // 2, S // 2
    loads = rows // BLOCK_ROWS + (1 if quad else 0)

    dma = pltpu.SemaphoreType.DMA
    vmem = pltpu.VMEM
    anywhere = pl.BlockSpec(memory_space=pl.ANY)
    in_vmem = pl.BlockSpec(memory_space=pltpu.VMEM)
    in_hbm = pl.BlockSpec(memory_space=pltpu.HBM)
    in_smem = pl.BlockSpec(memory_space=pltpu.SMEM)
    tree = quad and Z == 4 and O == 2
    if tree:
        held = SLOTS - 1
        first = chunks // 5
        steps = chunks - first
        piece = (rc, cols)
        sums, bases, tot, ms, mm = pl.pallas_call(
            functools.partial(tree_kernel, R, S, rows, rc, first),
            out_shape=(
                jax.ShapeDtypeStruct((S, chunks, rc, cols), BF16),
                jax.ShapeDtypeStruct((S, held * BLOCK_ROWS, cols), BF16),
                jax.ShapeDtypeStruct((8, 128), F32),
                jax.ShapeDtypeStruct(master.shape, F32),
                jax.ShapeDtypeStruct(master.shape, F32),
            ),
            in_specs=[in_hbm] * 4,
            out_specs=(in_vmem,) * 5,
            scratch_shapes=[
                vmem(block_owner.shape, jnp.int32),
                vmem((loads * BLOCK_ROWS, width), BF16),
                vmem((BLOCK_ROWS, width), BF16),
                vmem((half, width), BF16),
                vmem((BLOCK_ROWS, cols), BF16),
                vmem((BLOCK_ROWS, cols), BF16),
                vmem((chunks, Z) + piece, BF16),
                vmem((chunks, Z) + piece, BF16),
                vmem((chunks, 3) + piece, BF16),
                vmem((chunks, 2) + piece, BF16),
                vmem((chunks,) + piece, BF16),
                vmem((first, 3, 2) + piece, BF16),
                vmem((first, 2, 2) + piece, BF16),
                vmem((first, 2) + piece, BF16),
                vmem((first,) + piece, BF16),
                vmem((first,) + piece, F32),
                vmem((first,) + piece, BF16),
                vmem((8, 128), F32),
                vmem((1, 128), F32),
                vmem((R * S - 1, 1, 128), F32),
                dma, dma((loads,)), dma((2,)), dma, dma((2,)), dma, dma,
                dma, dma((steps, 2)), dma, dma((steps,)), dma((steps,)), dma, dma((steps,)),
                dma, dma((first, 2)), dma, dma((first,)), dma, dma((first,)),
                dma, dma, dma, dma((chunks,)), dma, dma,
                dma, dma, dma, dma, dma((2,)), dma((2,)), dma, dma, dma, dma,
                pltpu.SemaphoreType.REGULAR,
            ],
            compiler_params=pltpu.CompilerParams(
                collective_id=0, has_side_effects=True, vmem_limit_bytes=SYNC_VMEM
            ),
            name="sync",
        )(*(pltpu.with_memory_space_constraint(a, pltpu.HBM) for a in (block_owner, deltas, master, momentum)))
        return tuple(pl.pallas_call(
            functools.partial(close_kernel, R, units, held),
            out_shape=(
                jax.ShapeDtypeStruct(master.shape, F32),
                jax.ShapeDtypeStruct(master.shape, F32),
                jax.ShapeDtypeStruct((blocks * BLOCK_ROWS, cols), BF16),
            ),
            in_specs=[in_vmem] * 6,
            out_specs=(in_hbm,) * 3,
            scratch_shapes=[
                pltpu.SMEM((1, blocks), jnp.int32),
                vmem(master.shape, F32),
                vmem(master.shape, F32),
                vmem((blocks, BLOCK_ROWS, cols), BF16),
                dma, dma((SLOTS,)), dma((SLOTS,)), dma((blocks,)),
            ],
            compiler_params=pltpu.CompilerParams(vmem_limit_bytes=CLOSE_VMEM),
            name="close",
        )(block_owner, tot, ms, mm, sums.reshape(S * units, half, cols),
          bases.reshape(S * held, BLOCK_ROWS, cols)))

    ys, zs = max(O - 1, 1), max(Z - 1, 1)
    sums, bases, tot = pl.pallas_call(
        functools.partial(sync_kernel, R, S, rows, rc),
        out_shape=(
            jax.ShapeDtypeStruct((S, chunks, rc, cols), BF16),
            jax.ShapeDtypeStruct((S,) + master.shape, BF16),
            jax.ShapeDtypeStruct((8, 128), F32),
        ),
        in_specs=[in_vmem, anywhere, anywhere, anywhere],
        out_specs=(anywhere, anywhere, in_vmem),
        scratch_shapes=[
            vmem((loads * BLOCK_ROWS, width), BF16),
            vmem((BLOCK_ROWS, width) if quad else (16, 128), BF16),
            vmem((half, width) if quad else (16, 128), BF16),
            vmem(master.shape, F32),
            vmem(master.shape, F32),
            vmem(master.shape, BF16),
            vmem((chunks, Z, rc, cols), BF16),
            vmem((chunks, Z, rc, cols), BF16),
            vmem((chunks, zs, rc, cols), BF16),
            vmem((chunks, rc, cols), BF16),
            vmem((2, 8, 128), F32),
            vmem((R - 1, 8, 128), F32),
            vmem((S - 1, 8, 128), F32),
            dma((loads,)), dma((2,)), dma((2,)), dma((2,)), dma, dma,
            dma((chunks, Z)), dma((chunks, Z)),
            dma((chunks, zs)), dma((chunks, zs)),
            dma((chunks,)), dma((chunks,)), dma((chunks,)),
            dma((ys, chunks)), dma((ys, chunks)), dma((ys, chunks)), dma((ys, chunks)),
            dma, dma, dma,
            dma((ys,)), dma((ys,)), dma((ys,)), dma((ys,)),
            dma((R - 1,)), dma((R - 1,)), dma((S - 1,)), dma((S - 1,)),
        ],
        compiler_params=pltpu.CompilerParams(
            collective_id=0, has_side_effects=True, vmem_limit_bytes=VMEM_LIMIT
        ),
        name="sync",
    )(block_owner, deltas, master, momentum)

    return tuple(pl.pallas_call(
        functools.partial(finish_kernel, R, units),
        out_shape=(
            jax.ShapeDtypeStruct(master.shape, F32),
            jax.ShapeDtypeStruct(master.shape, F32),
            jax.ShapeDtypeStruct((blocks * BLOCK_ROWS, cols), BF16),
        ),
        in_specs=[in_vmem, in_vmem] + [anywhere] * 4,
        out_specs=(anywhere,) * 3,
        scratch_shapes=[
            pltpu.SMEM((1, blocks), jnp.int32), dma,
            vmem(master.shape, F32),
            vmem(master.shape, F32),
            vmem((2 * SLOTS, half, cols), BF16),
            vmem((blocks, BLOCK_ROWS, cols), BF16),
            vmem((2 * blocks, half, cols), BF16),
            dma((SLOTS,)), dma((SLOTS,)), dma((2 * SLOTS,)), dma((blocks,)), dma((2 * blocks,)),
            dma((SLOTS,)), dma((SLOTS,)), dma((blocks,)),
        ],
        compiler_params=pltpu.CompilerParams(vmem_limit_bytes=VMEM_LIMIT),
        name="finish",
    )(block_owner, tot, master, momentum, sums.reshape(S * units, half, cols),
      bases.reshape(S * SLOTS, BLOCK_ROWS, cols)))


def solution(mesh):
    return jax.shard_map(
        on_device,
        mesh=mesh,
        in_specs=(P("replica", "shard", None), P("shard", "replica"), P("shard", "replica"), P()),
        out_specs=(P("shard", "replica"), P("shard", "replica"), P(None, "replica")),
        check_vma=False,
    )
```

```python
import functools

import jax
import jax.numpy as jnp
from jax import lax
from jax.experimental import pallas as pl
from jax.experimental.pallas import tpu as pltpu
from jax.sharding import PartitionSpec as P

BLOCK_ROWS = 128
SLOTS = 4
F32 = jnp.float32
BF16 = jnp.bfloat16
VMEM_LIMIT = 56 * 1024 * 1024
SYNC_VMEM = 26 * 1024 * 1024
CLOSE_VMEM = 12 * 1024 * 1024


def remote(src, dst, send, recv, device):
    return pltpu.make_async_remote_copy(
        src_ref=src, dst_ref=dst, send_sem=send, recv_sem=recv,
        device_id=device, device_id_type=pl.DeviceIdType.MESH,
    )


def shard_count(owner, shard):
    return sum(jnp.where(owner[0, b] == shard, 1, 0) for b in range(owner.shape[1]))


def spread(condition, shape):
    return jnp.broadcast_to(jnp.where(condition, 1, 0), shape) != 0


def sync_kernel(
    R, S, rows, rc,
    owner, deltas, master, momentum,
    sums, bases, tot,
    dv, p3, yt, ms, mm, base, xin, pair, zin, mine, norm, nbuf, sbuf,
    ld, lm, p3_s, p3_r, t_s, t_r, x_s, x_r, z_s, z_r, l_s, c_s, c_r, y_s, y_r, f_s, f_r,
    bl_s, bc_s, bc_r, by_s, by_r, bf_s, bf_r, n_s, n_r, m_s, m_r,
):
    width = deltas.shape[2]
    cols = width // R
    Z, O = R // 2, S // 2
    per = BLOCK_ROWS // rc
    half = BLOCK_ROWS // 2
    chunks = rows // rc
    quad = rows < SLOTS * BLOCK_ROWS
    whole = rows // BLOCK_ROWS
    direct = whole * per
    top = whole * BLOCK_ROWS
    me_r, me_s = lax.axis_index("replica"), lax.axis_index("shard")
    z, x = me_r // 2, me_r % 2
    o, core = me_s // 2, me_s % 2
    x_peer = z * 2 + 1 - x
    twin = o * 2 + 1 - core

    barrier = pltpu.get_barrier_semaphore()
    for i in range(1, R):
        pl.semaphore_signal(barrier, inc=1, device_id=((me_r + i) % R, me_s), device_id_type=pl.DeviceIdType.MESH)
    for i in range(1, S):
        pl.semaphore_signal(barrier, inc=1, device_id=(me_r, (me_s + i) % S), device_id_type=pl.DeviceIdType.MESH)

    def load(k):
        part = pl.ds(k * BLOCK_ROWS, BLOCK_ROWS)
        return pltpu.make_async_copy(deltas.at[0, part, :], dv.at[part, :], ld.at[k])

    if quad:
        load(whole).start()
    for k in range(whole):
        load(k).start()
    load_master = pltpu.make_async_copy(master, ms, lm.at[0])
    load_momentum = pltpu.make_async_copy(momentum, mm, lm.at[1])
    load_master.start()
    load_momentum.start()
    mine_count = jnp.sum(jnp.where(owner[...] == me_s, 1, 0), axis=1, keepdims=True)
    twin_count = jnp.sum(jnp.where(owner[...] == twin, 1, 0), axis=1, keepdims=True)
    heavy = jnp.maximum(mine_count, twin_count) >= SLOTS
    pl.semaphore_wait(barrier, R + S - 2)

    def rows_of(c):
        return pl.ds(pl.multiple_of(c * rc, rc), rc)

    def columns(c, j, side):
        return pl.ds(pl.multiple_of((((z + 1 + j) % Z) * 2 + side) * cols, cols), cols)

    def x_copy(source, c, j):
        return remote(
            source.at[rows_of(c), columns(c, j, 1 - x)], xin.at[c, j], x_s.at[c, j], x_r.at[c, j], (x_peer, me_s)
        )

    def z_copy(c, j):
        return remote(
            pair.at[c, j], zin.at[c, j], z_s.at[c, j], z_r.at[c, j], (((z + 1 + j) % Z) * 2 + x, me_s)
        )

    def c_copy(c):
        return remote(mine.at[c], sums.at[me_s, c], c_s.at[c], c_r.at[c], (me_r, twin))

    def l_copy(c):
        return pltpu.make_async_copy(mine.at[c], sums.at[me_s, c], l_s.at[c])

    def y_copy(i, c):
        return remote(
            mine.at[c], sums.at[me_s, c], y_s.at[i - 1, c], y_r.at[i - 1, c], (me_r, ((o + i) % O) * 2 + core)
        )

    def f_copy(i, c):
        source = ((o + O - i) % O) * 2 + core
        return remote(sums.at[source, c], sums.at[source, c], f_s.at[i - 1, c], f_r.at[i - 1, c], (me_r, twin))

    def by_copy(i):
        return remote(base, bases.at[me_s], by_s.at[i - 1], by_r.at[i - 1], (me_r, ((o + i) % O) * 2 + core))

    def bf_copy(i):
        source = ((o + O - i) % O) * 2 + core
        return remote(bases.at[source], bases.at[source], bf_s.at[i - 1], bf_r.at[i - 1], (me_r, twin))

    def third_copy(h):
        return remote(
            deltas.at[0, pl.ds((SLOTS - 1) * BLOCK_ROWS + h * half, half), :],
            p3.at[pl.ds(h * half, half), :], p3_s.at[h], p3_r.at[h], (me_r, twin),
        )

    def t_copy():
        return remote(dv.at[pl.ds(top + half, half), :], yt, t_s, t_r, (me_r, ((o + 1) % O) * 2 + core))

    def base_twin():
        return remote(base, bases.at[me_s], bc_s, bc_r, (me_r, twin))

    def base_local():
        return pltpu.make_async_copy(base, bases.at[me_s], bl_s)

    def start_x(source, low, high):
        @pl.loop(low, high)
        def _(c):
            for j in range(Z):
                x_copy(source, c, j).start()

    def pick(condition, other, start, other_start):
        @pl.loop(0, half // 16)
        def _(r):
            keep = spread(condition, (16, 1024))
            for q in range(width // 1024):
                at = (pl.ds(pl.multiple_of(start + r * 16, 16), 16), pl.ds(q * 1024, 1024))
                there = (pl.ds(pl.multiple_of(other_start + r * 16, 16), 16), pl.ds(q * 1024, 1024))
                dv[at] = jnp.where(keep, dv[at].astype(F32), other[there].astype(F32)).astype(BF16)

    if quad:
        third_copy(1).start()
        third_copy(0).start()
    start_x(deltas.at[0], 0, direct)
    norm[0] = jnp.zeros((8, 128), F32)

    def send_third():
        load(whole).wait()
        third_copy(1).wait_recv()
        pick(mine_count >= SLOTS, p3, top + half, half)
        t_copy().start()

    def make_base():
        load_master.wait()
        load_momentum.wait()

        @pl.loop(0, SLOTS * BLOCK_ROWS // 16)
        def _(r):
            at = pl.ds(pl.multiple_of(r * 16, 16), 16)
            base[at, :] = (ms[at, :] - 0.567 * mm[at, :]).astype(BF16)

        for i in range(1, O):
            by_copy(i).start()
        base_twin().start()
        base_local().start()

    def add_pair(c):
        @pl.when(c % per == 0)
        def _():
            @pl.when(c < direct)
            def _():
                load(c // per).wait()

        for j in range(Z):
            x_copy(deltas.at[0], c, j).wait_recv()
            pair[c, j] = (xin[c, j].astype(F32) + dv[rows_of(c), columns(c, j, x)].astype(F32)).astype(BF16)
            if j < Z - 1:
                z_copy(c, j).start()

    def add_line(c):
        for j in range(Z - 1):
            z_copy(c, j).wait_recv()
        place = jnp.where(c >= direct, -1, c // per) if quad else c // per
        live = spread(place < mine_count, (8, 128))
        part = jnp.zeros((8, 128), F32)
        for r in range(0, rc, 16):
            total = pair[c, Z - 1, r:r + 16, :].astype(F32)
            for j in range(Z - 1):
                total = total + zin[c, j, r:r + 16, :].astype(F32)
            total = total / R
            mine[c, r:r + 16, :] = total.astype(BF16)
            for h in range(0, 16, 8):
                for q in range(0, cols, 128):
                    v = total[h:h + 8, q:q + 128]
                    part = part + v * v
        norm[0] = norm[0] + jnp.where(live, part, 0.0)
        for i in range(1, O):
            y_copy(i, c).start()
        c_copy(c).start()
        l_copy(c).start()

    def forward(c):
        for i in range(1, O):
            y_copy(i, c).wait_recv()
            f_copy(i, c).start()

    lag = 4

    @pl.loop(0, chunks + lag)
    def _(t):
        @pl.when(t < chunks)
        def _():
            add_pair(t)

        @pl.when(t >= lag)
        def _():
            add_line(t - lag)

        @pl.when(t == 2)
        def _():
            make_base()

        if quad:
            @pl.when(t == 0)
            def _():
                send_third()

            @pl.when(t == direct - direct // 4)
            def _():
                third_copy(0).wait_recv()
                pick(mine_count >= SLOTS, p3, top, 0)
                t_copy().wait_recv()
                pick(heavy, yt, top, 0)
                start_x(dv, direct, chunks)

    def n_copy(i):
        return remote(norm.at[0], nbuf.at[i - 1], n_s.at[i - 1], n_r.at[i - 1], ((me_r + i) % R, me_s))

    def m_copy(i):
        return remote(norm.at[1], sbuf.at[i - 1], m_s.at[i - 1], m_r.at[i - 1], (me_r, (me_s + i) % S))

    for i in range(1, R):
        n_copy(i).start()
    for i in range(1, O):
        by_copy(i).wait_recv()
        bf_copy(i).start()

    @pl.loop(0, chunks - 2)
    def _(c):
        forward(c)
        for j in range(Z):
            x_copy(deltas.at[0], c, j).wait_send()
        for j in range(Z - 1):
            z_copy(c, j).wait_send()

    total = norm[0]
    for i in range(1, R):
        n_copy(i).wait_recv()
        total = total + nbuf[i - 1]
    norm[1] = total
    for i in range(1, S):
        m_copy(i).start()

    @pl.loop(chunks - 2, chunks)
    def _(c):
        forward(c)

    for i in range(1, S):
        m_copy(i).wait_recv()
        total = total + sbuf[i - 1]
    tot[...] = total

    if quad:
        third_copy(0).wait_send()
        third_copy(1).wait_send()
        t_copy().wait_send()
    base_local().wait()
    base_twin().wait()
    for i in range(1, O):
        by_copy(i).wait_send()
        bf_copy(i).wait()
    for i in range(1, R):
        n_copy(i).wait_send()
    for i in range(1, S):
        m_copy(i).wait_send()

    @pl.loop(chunks - 2, chunks)
    def _(c):
        for j in range(Z):
            x_copy(deltas.at[0], c, j).wait_send()
        for j in range(Z - 1):
            z_copy(c, j).wait_send()

    @pl.loop(0, chunks)
    def _(c):
        l_copy(c).wait()
        c_copy(c).wait()
        for i in range(1, O):
            y_copy(i, c).wait_send()
            f_copy(i, c).wait()


def tree_kernel(
    R, S, rows, rc, first,
    owner_in, deltas, master, momentum,
    sums, bases, tot, ms, mm,
    owner, dv, p3, yt, b3, b3_in,
    xin, pair, zq, comb, zin, qb, combb, zinb, part_b, keep_b, xin_b, norm, total_row, nbuf,
    lo, ld, lm, p3_s, p3_r, t_s, t_r, x_s, x_r, xl_r, q_s, qa_r, qc_r, far_s, far_r,
    qb_s, qb_r, farb_s, farb_r, xb_s, xb_r,
    c_s, c_r, y_s, y_r, f_s, f_r,
    b3_s, b3_r, bc_s, bc_r, by_s, by_r, bf_s, bf_r, n_s, n_r, go,
):
    width = deltas.shape[2]
    cols = width // R
    Z = R // 2
    per = BLOCK_ROWS // rc
    half = BLOCK_ROWS // 2
    chunks = rows // rc
    whole = rows // BLOCK_ROWS
    direct = whole * per
    top = whole * BLOCK_ROWS
    mid_lag, line_lag = 2, 4
    steps = chunks - first
    late = chunks - direct
    last = max(line_lag, late)
    group = late
    me_r, me_s = lax.axis_index("replica"), lax.axis_index("shard")
    z, x = me_r // 2, me_r % 2
    o, core = me_s // 2, me_s % 2
    side = z // 2
    inner = (z + side) % 2
    outer = 1 - inner
    is_inner, is_outer = inner == 1, inner == 0
    x_peer = (z * 2 + 1 - x, me_s)
    near = ((side * 2 + 1 - z % 2) * 2 + x, me_s)
    far_outer = ((Z - 1) * (1 - side) * 2 + x, me_s)
    far_inner = ((Z - 1 - z) * 2 + x, me_s)
    twin = o * 2 + 1 - core
    twin_device = (me_r, twin)
    y_shard = (1 - o) * 2 + core
    y_device = (me_r, y_shard)

    barrier = pltpu.get_barrier_semaphore()
    me = me_r * S + me_s

    def peer(i):
        other = (me + i) % (R * S)
        return (other // S, other % S)

    def greet(device):
        pl.semaphore_signal(barrier, inc=1, device_id=device, device_id_type=pl.DeviceIdType.MESH)

    for device in (x_peer, near, twin_device, y_device):
        greet(device)

    @pl.when(is_inner)
    def _():
        greet(far_inner)

    def load(k):
        part = pl.ds(k * BLOCK_ROWS, BLOCK_ROWS)
        return pltpu.make_async_copy(deltas.at[0, part, :], dv.at[part, :], ld.at[k])

    load_owner = pltpu.make_async_copy(owner_in, owner, lo)
    load_owner.start()
    load_master = pltpu.make_async_copy(master, ms, lm.at[0])
    load_momentum = pltpu.make_async_copy(momentum, mm, lm.at[1])
    load_master.start()
    load_momentum.start()
    load(whole).start()
    for k in range(whole):
        load(k).start()
    norm[...] = jnp.zeros((8, 128), F32)
    pl.semaphore_wait(barrier, 4 + inner)

    @pl.when(is_inner)
    def _():
        pl.semaphore_signal(go, inc=1, device_id=far_inner, device_id_type=pl.DeviceIdType.MESH)

    mine, base = sums.at[me_s], bases.at[me_s]

    def rows_of(c):
        return pl.ds(pl.multiple_of(c * rc, rc), rc)

    def columns(k, side_x):
        e = (Z - 1 - k) if k < 2 else (outer if k == 2 else inner)
        d = e + side * (Z - 1 - 2 * e)
        return pl.ds(pl.multiple_of((d * 2 + side_x) * cols, cols), cols)

    def arrived(ref, sem):
        remote(ref, ref, n_s, sem, twin_device).wait_recv()

    def sent(ref, sem):
        remote(ref, ref, sem, n_r, twin_device).wait_send()

    def x_copy(source, c, k, sem):
        return remote(source.at[rows_of(c), columns(k, 1 - x)], xin.at[c, k], x_s, sem, x_peer)

    def start_q(c, k):
        if k == 2:
            remote(pair.at[c, k], zq.at[c, k], q_s, qc_r.at[c - first], near).start()
        else:
            @pl.when(is_outer)
            def _():
                remote(pair.at[c, k], zq.at[c, k], q_s, qa_r.at[c - first], near).start()

    def far_copy(c, i):
        return remote(comb.at[c, i], zin.at[c], far_s, far_r.at[c - first], far_inner if i else far_outer)

    def half_x(v):
        return x if v else 1 - x

    def start_qb(c):
        def start(v, k):
            remote(
                deltas.at[0, rows_of(c), columns(k, half_x(v))], qb.at[c, k, v], qb_s, qb_r.at[c, k // 2], near
            ).start()

        @pl.when(is_outer)
        def _():
            for k in range(2):
                for v in range(2):
                    start(v, k)

        for v in range(2):
            start(v, 2)

    def farb_copy(c, v, i):
        return remote(combb.at[c, v, i], zinb.at[c, v], farb_s, farb_r.at[c], far_inner if i else far_outer)

    def xb_copy(c):
        return remote(part_b.at[c], xin_b.at[c], xb_s, xb_r.at[c], x_peer)

    def c_copy(c):
        return remote(mine.at[c], sums.at[me_s, c], c_s, c_r, twin_device)

    def y_copy(c):
        return remote(mine.at[c], sums.at[me_s, c], y_s, y_r.at[c // group], y_device)

    def f_copy(g):
        part = sums.at[y_shard, pl.ds(g * group, group)]
        return remote(part, part, f_s, f_r, twin_device)

    def by_copy(i):
        part = pl.ds(i * BLOCK_ROWS, BLOCK_ROWS * (SLOTS - 2 if i else 1))
        return remote(base.at[part], bases.at[me_s, part], by_s.at[i], by_r.at[i], y_device)

    def bf_copy():
        return remote(bases.at[y_shard], bases.at[y_shard], bf_s, bf_r, twin_device)

    def b3_copy():
        return remote(b3, b3_in, b3_s, b3_r, twin_device)

    def base_twin():
        return remote(base, bases.at[me_s], bc_s, bc_r, twin_device)

    def third_copy(h):
        return remote(
            deltas.at[0, pl.ds((SLOTS - 1) * BLOCK_ROWS + h * half, half), :],
            p3.at[pl.ds(h * half, half), :], p3_s, p3_r.at[h], twin_device,
        )

    def t_copy():
        return remote(dv.at[pl.ds(top + half, half), :], yt, t_s, t_r, y_device)

    def start_x(low, high):
        @pl.loop(low, high)
        def _(c):
            for k in range(Z):
                x_copy(deltas.at[0], c, k, x_r.at[c - first]).start()

    def start_late(pieces):
        @pl.loop(direct, chunks)
        def _(c):
            for k in pieces:
                x_copy(dv, c, k, x_r.at[c - first] if k < 2 else xl_r.at[c - direct, k - 2]).start()

    def pick(condition, other, start, other_start):
        @pl.loop(0, half // 16)
        def _(r):
            keep = spread(condition, (16, 1024))
            for q in range(width // 1024):
                at = (pl.ds(pl.multiple_of(start + r * 16, 16), 16), pl.ds(q * 1024, 1024))
                there = (pl.ds(pl.multiple_of(other_start + r * 16, 16), 16), pl.ds(q * 1024, 1024))
                dv[at] = jnp.where(keep, dv[at].astype(F32), other[there].astype(F32)).astype(BF16)

    third_copy(1).start()
    start_x(first, first + 2)
    third_copy(0).start()
    start_qb(0)

    def send_third():
        load(whole).wait()
        third_copy(1).wait_recv()
        pick(mine_count >= SLOTS, p3, top + half, half)
        t_copy().start()

    def start_base(low, high, target, target_start):
        @pl.loop(low * BLOCK_ROWS // 16, high * BLOCK_ROWS // 16)
        def _(r):
            at = pl.ds(pl.multiple_of(r * 16, 16), 16)
            to = pl.ds(pl.multiple_of(r * 16 - target_start, 16), 16)
            target[to, :] = (ms[at, :] - 0.567 * mm[at, :]).astype(BF16)

    def make_base():
        start_base(SLOTS - 1, SLOTS, b3, (SLOTS - 1) * BLOCK_ROWS)
        b3_copy().start()
        start_base(1, SLOTS - 1, base, 0)

    def send_base():
        b3_copy().wait_recv()

        @pl.loop(0, BLOCK_ROWS // 16)
        def _(r):
            at = pl.ds(pl.multiple_of(top + r * 16, 16), 16)
            there = pl.ds(pl.multiple_of(r * 16, 16), 16)
            keep = spread(mine_count >= SLOTS, (16, cols))
            base[at, :] = jnp.where(keep, base[at, :].astype(F32), b3_in[there, :].astype(F32)).astype(BF16)

        by_copy(1).start()
        base_twin().start()

    def ready():
        @pl.loop(0, SLOTS * per)
        def _(r):
            at = pl.ds(pl.multiple_of(r * rc, rc), rc)
            old, before = ms[at, :], mm[at, :]
            live = spread(r // per < mine_count, old.shape)
            ms[at, :] = jnp.where(live, old - 0.567 * before, old)
            mm[at, :] = jnp.where(live, 0.9 * before, before)

    def add_pair(c, pieces):
        for k in pieces:
            pair[c, k] = (xin[c, k].astype(F32) + dv[rows_of(c), columns(k, x)].astype(F32)).astype(BF16)
            if k < Z - 1:
                start_q(c, k)

    def add_mid(c):
        arrived(zq.at[c, pl.ds(0, 2)], qa_r.at[c - first])
        for i in range(2):
            comb[c, i] = (pair[c, i].astype(F32) + zq[c, i].astype(F32)).astype(BF16)
            far_copy(c, i).start()

    def add_mid_b(c):
        arrived(qb.at[c, pl.ds(0, 2)], qb_r.at[c, 0])
        for v in range(2):
            for i in range(2):
                own = dv[rows_of(c), columns(i, half_x(v))].astype(F32)
                combb[c, v, i] = (own + qb[c, i, v].astype(F32)).astype(BF16)
                farb_copy(c, v, i).start()

    def add_line_b(c):
        arrived(qb.at[c, 2], qb_r.at[c, 1])
        arrived(zinb.at[c], farb_r.at[c])
        for v in range(2):
            own = dv[rows_of(c), columns(Z - 1, half_x(v))].astype(F32)
            value = own + qb[c, 2, v].astype(F32) + zinb[c, v].astype(F32)
            if v:
                keep_b[c] = value
            else:
                part_b[c] = value.astype(BF16)

    def emit(c, get):
        place = jnp.where(c >= direct, -1, c // per)
        live = spread(place < mine_count, (8, 128))
        part = jnp.zeros((8, 128), F32)
        for r in range(0, rc, 16):
            total = get(r) / R
            mine[c, r:r + 16, :] = total.astype(BF16)
            for h in range(0, 16, 8):
                for q in range(0, cols, 128):
                    v = total[h:h + 8, q:q + 128]
                    part = part + v * v
        norm[...] = norm[...] + jnp.where(live, part, 0.0)
        y_copy(c).start()
        c_copy(c).start()

    def add_line(c):
        arrived(zq.at[c, 2], qc_r.at[c - first])
        arrived(zin.at[c], far_r.at[c - first])
        emit(c, lambda r: (
            pair[c, Z - 1, r:r + 16, :].astype(F32) + zq[c, 2, r:r + 16, :].astype(F32)
            + zin[c, r:r + 16, :].astype(F32)
        ))

    def add_last_b(c):
        xb_copy(c).wait_recv()
        emit(c, lambda r: keep_b[c, r:r + 16, :] + xin_b[c, r:r + 16, :].astype(F32))

    def forward(g):
        arrived(sums.at[y_shard, pl.ds(g * group, group)], y_r.at[g])
        f_copy(g).start()

    load_owner.wait()
    mine_count = jnp.sum(jnp.where(owner[...] == me_s, 1, 0), axis=1, keepdims=True)
    twin_count = jnp.sum(jnp.where(owner[...] == twin, 1, 0), axis=1, keepdims=True)
    heavy = jnp.maximum(mine_count, twin_count) >= SLOTS
    load_master.wait()
    load_momentum.wait()
    start_base(0, 1, base, 0)
    by_copy(0).start()

    @pl.loop(1, first)
    def _(c):
        start_qb(c)

    start_x(first + 2, direct)
    make_base()
    send_third()
    send_base()
    load(0).wait()

    quad_at = (direct - first) * 2 // 3

    @pl.when(is_inner)
    def _():
        pl.semaphore_wait(go, 1)

    @pl.loop(0, steps)
    def _(t):
        c = first + t

        @pl.when(jnp.logical_and(c % per == 0, c < direct))
        def _():
            load(c // per).wait()

        @pl.when(c < direct)
        def _():
            arrived(xin.at[c], x_r.at[c - first])
            add_pair(c, range(Z))

        @pl.when(c >= direct)
        def _():
            arrived(xin.at[c, pl.ds(0, 2)], x_r.at[c - first])
            add_pair(c, range(2))

        @pl.when(jnp.logical_and(is_inner, t < first))
        def _():
            add_mid_b(t)

        @pl.when(jnp.logical_and(t >= 2, t < 2 + first))
        def _():
            add_line_b(t - 2)

        @pl.when(jnp.logical_and(is_inner, t >= mid_lag))
        def _():
            add_mid(first + t - mid_lag)

        @pl.when(jnp.logical_and(t >= line_lag, t - line_lag < steps - last))
        def _():
            add_line(first + t - line_lag)

        @pl.when(t == quad_at - 2)
        def _():
            ready()

        @pl.when(t == quad_at)
        def _():
            third_copy(0).wait_recv()
            pick(mine_count >= SLOTS, p3, top, 0)
            t_copy().wait_recv()
            pick(heavy, yt, top, 0)
            for pieces in ((0, 1), (2,), (3,)):
                start_late(pieces)

            @pl.loop(0, first)
            def _(c):
                xb_copy(c).start()

    @pl.loop(direct, chunks)
    def _(c):
        arrived(xin.at[c, 2], xl_r.at[c - direct, 0])
        add_pair(c, (2,))

    @pl.when(is_inner)
    def _():
        @pl.loop(chunks - mid_lag, chunks)
        def _(c):
            add_mid(c)

    @pl.loop(direct, chunks)
    def _(c):
        arrived(xin.at[c, 3], xl_r.at[c - direct, 1])
        add_pair(c, (3,))

    @pl.loop(0, first)
    def _(c):
        add_last_b(c)

    @pl.loop(chunks - last, chunks)
    def _(c):
        add_line(c)

    total_row[...] = jnp.sum(norm[...], axis=0, keepdims=True)

    def n_copy(i):
        return remote(total_row, nbuf.at[i - 1], n_s, n_r, peer(i))

    for i in range(1, R * S):
        n_copy(i).start()
    by_copy(0).wait_recv()
    by_copy(1).wait_recv()
    bf_copy().start()

    @pl.loop(1, chunks // group)
    def _(g):
        forward(g % (chunks // group - 1))

    forward(chunks // group - 1)

    sent(p3, p3_s)
    t_copy().wait_send()
    b3_copy().wait_send()
    base_twin().wait()
    ours = pl.ds(first, steps)
    sent(xin.at[ours], x_s)
    sent(xin_b, xb_s)

    @pl.when(is_outer)
    def _():
        sent(zq.at[ours], q_s)
        sent(qb, qb_s)

    @pl.when(is_inner)
    def _():
        sent(zin.at[ours], q_s)
        sent(zinb, qb_s)
        sent(comb.at[ours], far_s)
        sent(combb, farb_s)

    sent(mine, c_s)
    sent(mine, y_s)
    sent(mine, f_s)
    arrived(sums.at[twin], c_r)
    arrived(mine, f_r)
    by_copy(0).wait_send()
    by_copy(1).wait_send()
    bf_copy().wait()
    arrived(nbuf, n_r)
    sent(nbuf, n_s)
    total = total_row[...]
    for i in range(1, R * S):
        total = total + nbuf[i - 1]
    tot[...] = jnp.broadcast_to(total, (8, 128)) * jnp.where(
        lax.broadcasted_iota(jnp.int32, (8, 128), 0) == 0, 1.0, 0.0
    )


def finish_kernel(
    R, units,
    owner_in, tot, master, momentum, sums, bases,
    master_out, momentum_out, params,
    owner, owner_s, ms, mm, su, pb, ps,
    a_s, b_s, u_s, p_s, q_s, oa_s, ob_s, op_s,
):
    blocks = owner.shape[1]
    cols = master.shape[1]
    half = BLOCK_ROWS // 2
    me_s = lax.axis_index("shard")
    get_owner = pltpu.make_async_copy(owner_in, owner, owner_s)
    get_owner.start()

    def unit(shard, place, h):
        if units == 2 * SLOTS:
            return shard * units + 2 * place + h
        moved = shard + jnp.where(place == SLOTS - 1, 1 - 2 * (shard % 2), 0)
        if h:
            moved = moved + jnp.where(moved // 2 == 0, 2, -2)
        return jnp.where(place < 2, shard * units + 2 * place + h, moved * units + units - 1)

    def slot_rows(j):
        return pl.ds(pl.multiple_of(j * BLOCK_ROWS, BLOCK_ROWS), BLOCK_ROWS)

    def get_slot(j):
        return [
            pltpu.make_async_copy(master.at[slot_rows(j)], ms.at[slot_rows(j)], a_s.at[j]),
            pltpu.make_async_copy(momentum.at[slot_rows(j)], mm.at[slot_rows(j)], b_s.at[j]),
        ] + [
            pltpu.make_async_copy(sums.at[unit(me_s, j, h)], su.at[2 * j + h], u_s.at[2 * j + h]) for h in range(2)
        ]

    def put_slot(j):
        return [
            pltpu.make_async_copy(ms.at[slot_rows(j)], master_out.at[slot_rows(j)], oa_s.at[j]),
            pltpu.make_async_copy(mm.at[slot_rows(j)], momentum_out.at[slot_rows(j)], ob_s.at[j]),
        ]

    def get_block(b):
        shard = owner[0, b]
        place = sum(jnp.where(jnp.logical_and(owner[0, k] == shard, k < b), 1, 0) for k in range(blocks))
        return [pltpu.make_async_copy(bases.at[shard * SLOTS + place], pb.at[b], p_s.at[b])] + [
            pltpu.make_async_copy(sums.at[unit(shard, place, h)], ps.at[2 * b + h], q_s.at[2 * b + h])
            for h in range(2)
        ]

    def put_block(b):
        return pltpu.make_async_copy(pb.at[b], params.at[slot_rows(b)], op_s.at[b])

    @pl.loop(0, SLOTS)
    def _(j):
        for copy in get_slot(j):
            copy.start()

    get_owner.wait()
    count = shard_count(owner, me_s)

    @pl.loop(0, blocks)
    def _(b):
        for copy in get_block(b):
            copy.start()

    total = jnp.sum(jnp.sum(tot[...], axis=1, keepdims=True), axis=0, keepdims=True)
    limit = 0.5 * jnp.sqrt(jnp.full((1, 1), blocks * BLOCK_ROWS * R * cols, F32))
    factor = jnp.minimum(1.0, limit / (jnp.sqrt(total) + 1e-06))

    @pl.loop(0, SLOTS)
    def _(j):
        for copy in get_slot(j):
            copy.wait()

        @pl.when(j < count)
        def _():
            for h in range(2):
                @pl.loop(0, half // 16)
                def _(r):
                    at = pl.ds(pl.multiple_of(j * BLOCK_ROWS + h * half + r * 16, 16), 16)
                    grad = factor * su[2 * j + h, pl.ds(pl.multiple_of(r * 16, 16), 16), :].astype(F32)
                    fresh = 0.9 * mm[at, :] + grad
                    mm[at, :] = fresh
                    ms[at, :] = ms[at, :] - 0.7 * (grad + 0.9 * fresh)

        for copy in put_slot(j):
            copy.start()

    @pl.loop(0, blocks)
    def _(b):
        for copy in get_block(b):
            copy.wait()
        for h in range(2):
            @pl.loop(0, half // 16)
            def _(r):
                at = pl.ds(pl.multiple_of(h * half + r * 16, 16), 16)
                grad = factor * ps[2 * b + h, pl.ds(pl.multiple_of(r * 16, 16), 16), :].astype(F32)
                pb[b, at, :] = (pb[b, at, :].astype(F32) - 1.33 * grad).astype(BF16)

        put_block(b).start()

    @pl.loop(0, SLOTS)
    def _(j):
        for copy in put_slot(j):
            copy.wait()

    @pl.loop(0, blocks)
    def _(b):
        put_block(b).wait()


def close_kernel(
    R, units, held,
    owner_in, tot, master, momentum, sums, bases,
    master_out, momentum_out, params,
    owner, ms, mm, pb, owner_s, a_s, b_s, p_s,
):
    blocks = owner.shape[1]
    cols = master.shape[1]
    half = BLOCK_ROWS // 2
    me_s = lax.axis_index("shard")
    get_owner = pltpu.make_async_copy(owner_in, owner, owner_s)
    get_owner.start()

    def unit(shard, place, h):
        moved = shard + jnp.where(place == SLOTS - 1, 1 - 2 * (shard % 2), 0)
        if h:
            moved = moved + jnp.where(moved // 2 == 0, 2, -2)
        return jnp.where(place < 2, shard * units + 2 * place + h, moved * units + units - 1)

    def slot_rows(j):
        return pl.ds(pl.multiple_of(j * BLOCK_ROWS, BLOCK_ROWS), BLOCK_ROWS)

    def put_slot(j):
        return [
            pltpu.make_async_copy(ms.at[slot_rows(j)], master_out.at[slot_rows(j)], a_s.at[j]),
            pltpu.make_async_copy(mm.at[slot_rows(j)], momentum_out.at[slot_rows(j)], b_s.at[j]),
        ]

    def put_block(b):
        return pltpu.make_async_copy(pb.at[b], params.at[slot_rows(b)], p_s.at[b])

    total = jnp.sum(jnp.sum(tot[...], axis=1, keepdims=True), axis=0, keepdims=True)
    limit = 0.5 * jnp.sqrt(jnp.full((1, 1), blocks * BLOCK_ROWS * R * cols, F32))
    factor = jnp.minimum(1.0, limit / (jnp.sqrt(total) + 1e-06))
    count = jnp.sum(jnp.where(owner_in[...] == me_s, 1, 0), axis=1, keepdims=True)

    @pl.loop(0, SLOTS)
    def _(j):
        for h in range(2):
            source = unit(me_s, j, h)

            @pl.loop(0, half // 16)
            def _(r):
                at = pl.ds(pl.multiple_of(j * BLOCK_ROWS + h * half + r * 16, 16), 16)
                part = factor * sums[source, pl.ds(pl.multiple_of(r * 16, 16), 16), :].astype(F32)
                grad = jnp.where(spread(j < count, part.shape), part, 0.0)
                mm[at, :] = momentum[at, :] + grad
                ms[at, :] = master[at, :] - 1.33 * grad

        for copy in put_slot(j):
            copy.start()

    get_owner.wait()

    @pl.loop(0, blocks)
    def _(b):
        shard = owner[0, b]
        place = sum(jnp.where(jnp.logical_and(owner[0, k] == shard, k < b), 1, 0) for k in range(blocks))
        kept = jnp.where(place < held, shard * held + place, (shard + 1 - 2 * (shard % 2)) * held + held - 1)
        for h in range(2):
            source = unit(shard, place, h)

            @pl.loop(0, half // 16)
            def _(r):
                at = pl.ds(pl.multiple_of(h * half + r * 16, 16), 16)
                grad = factor * sums[source, pl.ds(pl.multiple_of(r * 16, 16), 16), :].astype(F32)
                pb[b, at, :] = (bases[kept, at, :].astype(F32) - 1.33 * grad).astype(BF16)

        put_block(b).start()

    @pl.loop(0, SLOTS)
    def _(j):
        for copy in put_slot(j):
            copy.wait()

    @pl.loop(0, blocks)
    def _(b):
        put_block(b).wait()


def on_device(deltas, master, momentum, block_owner):
    R, S = lax.axis_size("replica"), lax.axis_size("shard")
    width, cols = deltas.shape[2], master.shape[1]
    blocks = block_owner.shape[0]
    block_owner = block_owner.reshape(1, blocks)
    half = BLOCK_ROWS // 2
    quad = S == 4 and blocks - SLOTS - (S - 2) <= 2
    rows = 2 * BLOCK_ROWS + half if quad else SLOTS * BLOCK_ROWS
    rc = half
    while rc > 16 and (rows // (rc // 2)) * R <= 160:
        rc //= 2
    chunks = rows // rc
    units = rows // half
    Z, O = R // 2, S // 2
    loads = rows // BLOCK_ROWS + (1 if quad else 0)

    dma = pltpu.SemaphoreType.DMA
    vmem = pltpu.VMEM
    anywhere = pl.BlockSpec(memory_space=pl.ANY)
    in_vmem = pl.BlockSpec(memory_space=pltpu.VMEM)
    in_hbm = pl.BlockSpec(memory_space=pltpu.HBM)
    in_smem = pl.BlockSpec(memory_space=pltpu.SMEM)
    tree = quad and Z == 4 and O == 2
    if tree:
        held = SLOTS - 1
        first = chunks * 3 // 20
        steps = chunks - first
        piece = (rc, cols)
        sums, bases, tot, ms, mm = pl.pallas_call(
            functools.partial(tree_kernel, R, S, rows, rc, first),
            out_shape=(
                jax.ShapeDtypeStruct((S, chunks, rc, cols), BF16),
                jax.ShapeDtypeStruct((S, held * BLOCK_ROWS, cols), BF16),
                jax.ShapeDtypeStruct((8, 128), F32),
                jax.ShapeDtypeStruct(master.shape, F32),
                jax.ShapeDtypeStruct(master.shape, F32),
            ),
            in_specs=[in_hbm] * 4,
            out_specs=(in_vmem,) * 5,
            scratch_shapes=[
                vmem(block_owner.shape, jnp.int32),
                vmem((loads * BLOCK_ROWS, width), BF16),
                vmem((BLOCK_ROWS, width), BF16),
                vmem((half, width), BF16),
                vmem((BLOCK_ROWS, cols), BF16),
                vmem((BLOCK_ROWS, cols), BF16),
                vmem((chunks, Z) + piece, BF16),
                vmem((chunks, Z) + piece, BF16),
                vmem((chunks, 3) + piece, BF16),
                vmem((chunks, 2) + piece, BF16),
                vmem((chunks,) + piece, BF16),
                vmem((first, 3, 2) + piece, BF16),
                vmem((first, 2, 2) + piece, BF16),
                vmem((first, 2) + piece, BF16),
                vmem((first,) + piece, BF16),
                vmem((first,) + piece, F32),
                vmem((first,) + piece, BF16),
                vmem((8, 128), F32),
                vmem((1, 128), F32),
                vmem((R * S - 1, 1, 128), F32),
                dma, dma((loads,)), dma((2,)), dma, dma((2,)), dma, dma,
                dma, dma((steps,)), dma((half // rc, 2)), dma, dma((steps,)), dma((steps,)), dma, dma((steps,)),
                dma, dma((first, 2)), dma, dma((first,)), dma, dma((first,)),
                dma, dma, dma, dma((chunks * rc // half,)), dma, dma,
                dma, dma, dma, dma, dma((2,)), dma((2,)), dma, dma, dma, dma,
                pltpu.SemaphoreType.REGULAR,
            ],
            compiler_params=pltpu.CompilerParams(
                collective_id=0, has_side_effects=True, vmem_limit_bytes=SYNC_VMEM
            ),
            name="sync",
        )(*(pltpu.with_memory_space_constraint(a, pltpu.HBM) for a in (block_owner, deltas, master, momentum)))
        return tuple(pl.pallas_call(
            functools.partial(close_kernel, R, units, held),
            out_shape=(
                jax.ShapeDtypeStruct(master.shape, F32),
                jax.ShapeDtypeStruct(master.shape, F32),
                jax.ShapeDtypeStruct((blocks * BLOCK_ROWS, cols), BF16),
            ),
            in_specs=[in_vmem] * 6,
            out_specs=(in_hbm,) * 3,
            scratch_shapes=[
                pltpu.SMEM((1, blocks), jnp.int32),
                vmem(master.shape, F32),
                vmem(master.shape, F32),
                vmem((blocks, BLOCK_ROWS, cols), BF16),
                dma, dma((SLOTS,)), dma((SLOTS,)), dma((blocks,)),
            ],
            compiler_params=pltpu.CompilerParams(vmem_limit_bytes=CLOSE_VMEM),
            name="close",
        )(block_owner, tot, ms, mm, sums.reshape(S * units, half, cols),
          bases.reshape(S * held, BLOCK_ROWS, cols)))

    ys, zs = max(O - 1, 1), max(Z - 1, 1)
    sums, bases, tot = pl.pallas_call(
        functools.partial(sync_kernel, R, S, rows, rc),
        out_shape=(
            jax.ShapeDtypeStruct((S, chunks, rc, cols), BF16),
            jax.ShapeDtypeStruct((S,) + master.shape, BF16),
            jax.ShapeDtypeStruct((8, 128), F32),
        ),
        in_specs=[in_vmem, anywhere, anywhere, anywhere],
        out_specs=(anywhere, anywhere, in_vmem),
        scratch_shapes=[
            vmem((loads * BLOCK_ROWS, width), BF16),
            vmem((BLOCK_ROWS, width) if quad else (16, 128), BF16),
            vmem((half, width) if quad else (16, 128), BF16),
            vmem(master.shape, F32),
            vmem(master.shape, F32),
            vmem(master.shape, BF16),
            vmem((chunks, Z, rc, cols), BF16),
            vmem((chunks, Z, rc, cols), BF16),
            vmem((chunks, zs, rc, cols), BF16),
            vmem((chunks, rc, cols), BF16),
            vmem((2, 8, 128), F32),
            vmem((R - 1, 8, 128), F32),
            vmem((S - 1, 8, 128), F32),
            dma((loads,)), dma((2,)), dma((2,)), dma((2,)), dma, dma,
            dma((chunks, Z)), dma((chunks, Z)),
            dma((chunks, zs)), dma((chunks, zs)),
            dma((chunks,)), dma((chunks,)), dma((chunks,)),
            dma((ys, chunks)), dma((ys, chunks)), dma((ys, chunks)), dma((ys, chunks)),
            dma, dma, dma,
            dma((ys,)), dma((ys,)), dma((ys,)), dma((ys,)),
            dma((R - 1,)), dma((R - 1,)), dma((S - 1,)), dma((S - 1,)),
        ],
        compiler_params=pltpu.CompilerParams(
            collective_id=0, has_side_effects=True, vmem_limit_bytes=VMEM_LIMIT
        ),
        name="sync",
    )(block_owner, deltas, master, momentum)

    return tuple(pl.pallas_call(
        functools.partial(finish_kernel, R, units),
        out_shape=(
            jax.ShapeDtypeStruct(master.shape, F32),
            jax.ShapeDtypeStruct(master.shape, F32),
            jax.ShapeDtypeStruct((blocks * BLOCK_ROWS, cols), BF16),
        ),
        in_specs=[in_vmem, in_vmem] + [anywhere] * 4,
        out_specs=(anywhere,) * 3,
        scratch_shapes=[
            pltpu.SMEM((1, blocks), jnp.int32), dma,
            vmem(master.shape, F32),
            vmem(master.shape, F32),
            vmem((2 * SLOTS, half, cols), BF16),
            vmem((blocks, BLOCK_ROWS, cols), BF16),
            vmem((2 * blocks, half, cols), BF16),
            dma((SLOTS,)), dma((SLOTS,)), dma((2 * SLOTS,)), dma((blocks,)), dma((2 * blocks,)),
            dma((SLOTS,)), dma((SLOTS,)), dma((blocks,)),
        ],
        compiler_params=pltpu.CompilerParams(vmem_limit_bytes=VMEM_LIMIT),
        name="finish",
    )(block_owner, tot, master, momentum, sums.reshape(S * units, half, cols),
      bases.reshape(S * SLOTS, BLOCK_ROWS, cols)))


def solution(mesh):
    return jax.shard_map(
        on_device,
        mesh=mesh,
        in_specs=(P("replica", "shard", None), P("shard", "replica"), P("shard", "replica"), P()),
        out_specs=(P("shard", "replica"), P("shard", "replica"), P(None, "replica")),
        check_vma=False,
    )
```

```python
import functools

import jax
import jax.numpy as jnp
from jax import lax
from jax.experimental import pallas as pl
from jax.experimental.pallas import tpu as pltpu
from jax.sharding import PartitionSpec as P

BLOCK_ROWS = 128
SLOTS = 4
F32 = jnp.float32
BF16 = jnp.bfloat16
VMEM_LIMIT = 56 * 1024 * 1024
SYNC_VMEM = 26 * 1024 * 1024
CLOSE_VMEM = 12 * 1024 * 1024


def remote(src, dst, send, recv, device):
    return pltpu.make_async_remote_copy(
        src_ref=src, dst_ref=dst, send_sem=send, recv_sem=recv,
        device_id=device, device_id_type=pl.DeviceIdType.MESH,
    )


def shard_count(owner, shard):
    return sum(jnp.where(owner[0, b] == shard, 1, 0) for b in range(owner.shape[1]))


def spread(condition, shape):
    return jnp.broadcast_to(jnp.where(condition, 1, 0), shape) != 0


def sync_kernel(
    R, S, rows, rc,
    owner, deltas, master, momentum,
    sums, bases, tot,
    dv, p3, yt, ms, mm, base, xin, pair, zin, mine, norm, nbuf, sbuf,
    ld, lm, p3_s, p3_r, t_s, t_r, x_s, x_r, z_s, z_r, l_s, c_s, c_r, y_s, y_r, f_s, f_r,
    bl_s, bc_s, bc_r, by_s, by_r, bf_s, bf_r, n_s, n_r, m_s, m_r,
):
    width = deltas.shape[2]
    cols = width // R
    Z, O = R // 2, S // 2
    per = BLOCK_ROWS // rc
    half = BLOCK_ROWS // 2
    chunks = rows // rc
    quad = rows < SLOTS * BLOCK_ROWS
    whole = rows // BLOCK_ROWS
    direct = whole * per
    top = whole * BLOCK_ROWS
    me_r, me_s = lax.axis_index("replica"), lax.axis_index("shard")
    z, x = me_r // 2, me_r % 2
    o, core = me_s // 2, me_s % 2
    x_peer = z * 2 + 1 - x
    twin = o * 2 + 1 - core

    barrier = pltpu.get_barrier_semaphore()
    for i in range(1, R):
        pl.semaphore_signal(barrier, inc=1, device_id=((me_r + i) % R, me_s), device_id_type=pl.DeviceIdType.MESH)
    for i in range(1, S):
        pl.semaphore_signal(barrier, inc=1, device_id=(me_r, (me_s + i) % S), device_id_type=pl.DeviceIdType.MESH)

    def load(k):
        part = pl.ds(k * BLOCK_ROWS, BLOCK_ROWS)
        return pltpu.make_async_copy(deltas.at[0, part, :], dv.at[part, :], ld.at[k])

    if quad:
        load(whole).start()
    for k in range(whole):
        load(k).start()
    load_master = pltpu.make_async_copy(master, ms, lm.at[0])
    load_momentum = pltpu.make_async_copy(momentum, mm, lm.at[1])
    load_master.start()
    load_momentum.start()
    mine_count = jnp.sum(jnp.where(owner[...] == me_s, 1, 0), axis=1, keepdims=True)
    twin_count = jnp.sum(jnp.where(owner[...] == twin, 1, 0), axis=1, keepdims=True)
    heavy = jnp.maximum(mine_count, twin_count) >= SLOTS
    pl.semaphore_wait(barrier, R + S - 2)

    def rows_of(c):
        return pl.ds(pl.multiple_of(c * rc, rc), rc)

    def columns(c, j, side):
        return pl.ds(pl.multiple_of((((z + 1 + j) % Z) * 2 + side) * cols, cols), cols)

    def x_copy(source, c, j):
        return remote(
            source.at[rows_of(c), columns(c, j, 1 - x)], xin.at[c, j], x_s.at[c, j], x_r.at[c, j], (x_peer, me_s)
        )

    def z_copy(c, j):
        return remote(
            pair.at[c, j], zin.at[c, j], z_s.at[c, j], z_r.at[c, j], (((z + 1 + j) % Z) * 2 + x, me_s)
        )

    def c_copy(c):
        return remote(mine.at[c], sums.at[me_s, c], c_s.at[c], c_r.at[c], (me_r, twin))

    def l_copy(c):
        return pltpu.make_async_copy(mine.at[c], sums.at[me_s, c], l_s.at[c])

    def y_copy(i, c):
        return remote(
            mine.at[c], sums.at[me_s, c], y_s.at[i - 1, c], y_r.at[i - 1, c], (me_r, ((o + i) % O) * 2 + core)
        )

    def f_copy(i, c):
        source = ((o + O - i) % O) * 2 + core
        return remote(sums.at[source, c], sums.at[source, c], f_s.at[i - 1, c], f_r.at[i - 1, c], (me_r, twin))

    def by_copy(i):
        return remote(base, bases.at[me_s], by_s.at[i - 1], by_r.at[i - 1], (me_r, ((o + i) % O) * 2 + core))

    def bf_copy(i):
        source = ((o + O - i) % O) * 2 + core
        return remote(bases.at[source], bases.at[source], bf_s.at[i - 1], bf_r.at[i - 1], (me_r, twin))

    def third_copy(h):
        return remote(
            deltas.at[0, pl.ds((SLOTS - 1) * BLOCK_ROWS + h * half, half), :],
            p3.at[pl.ds(h * half, half), :], p3_s.at[h], p3_r.at[h], (me_r, twin),
        )

    def t_copy():
        return remote(dv.at[pl.ds(top + half, half), :], yt, t_s, t_r, (me_r, ((o + 1) % O) * 2 + core))

    def base_twin():
        return remote(base, bases.at[me_s], bc_s, bc_r, (me_r, twin))

    def base_local():
        return pltpu.make_async_copy(base, bases.at[me_s], bl_s)

    def start_x(source, low, high):
        @pl.loop(low, high)
        def _(c):
            for j in range(Z):
                x_copy(source, c, j).start()

    def pick(condition, other, start, other_start):
        @pl.loop(0, half // 16)
        def _(r):
            keep = spread(condition, (16, 1024))
            for q in range(width // 1024):
                at = (pl.ds(pl.multiple_of(start + r * 16, 16), 16), pl.ds(q * 1024, 1024))
                there = (pl.ds(pl.multiple_of(other_start + r * 16, 16), 16), pl.ds(q * 1024, 1024))
                dv[at] = jnp.where(keep, dv[at].astype(F32), other[there].astype(F32)).astype(BF16)

    if quad:
        third_copy(1).start()
        third_copy(0).start()
    start_x(deltas.at[0], 0, direct)
    norm[0] = jnp.zeros((8, 128), F32)

    def send_third():
        load(whole).wait()
        third_copy(1).wait_recv()
        pick(mine_count >= SLOTS, p3, top + half, half)
        t_copy().start()

    def make_base():
        load_master.wait()
        load_momentum.wait()

        @pl.loop(0, SLOTS * BLOCK_ROWS // 16)
        def _(r):
            at = pl.ds(pl.multiple_of(r * 16, 16), 16)
            base[at, :] = (ms[at, :] - 0.567 * mm[at, :]).astype(BF16)

        for i in range(1, O):
            by_copy(i).start()
        base_twin().start()
        base_local().start()

    def add_pair(c):
        @pl.when(c % per == 0)
        def _():
            @pl.when(c < direct)
            def _():
                load(c // per).wait()

        for j in range(Z):
            x_copy(deltas.at[0], c, j).wait_recv()
            pair[c, j] = (xin[c, j].astype(F32) + dv[rows_of(c), columns(c, j, x)].astype(F32)).astype(BF16)
            if j < Z - 1:
                z_copy(c, j).start()

    def add_line(c):
        for j in range(Z - 1):
            z_copy(c, j).wait_recv()
        place = jnp.where(c >= direct, -1, c // per) if quad else c // per
        live = spread(place < mine_count, (8, 128))
        part = jnp.zeros((8, 128), F32)
        for r in range(0, rc, 16):
            total = pair[c, Z - 1, r:r + 16, :].astype(F32)
            for j in range(Z - 1):
                total = total + zin[c, j, r:r + 16, :].astype(F32)
            total = total / R
            mine[c, r:r + 16, :] = total.astype(BF16)
            for h in range(0, 16, 8):
                for q in range(0, cols, 128):
                    v = total[h:h + 8, q:q + 128]
                    part = part + v * v
        norm[0] = norm[0] + jnp.where(live, part, 0.0)
        for i in range(1, O):
            y_copy(i, c).start()
        c_copy(c).start()
        l_copy(c).start()

    def forward(c):
        for i in range(1, O):
            y_copy(i, c).wait_recv()
            f_copy(i, c).start()

    lag = 4

    @pl.loop(0, chunks + lag)
    def _(t):
        @pl.when(t < chunks)
        def _():
            add_pair(t)

        @pl.when(t >= lag)
        def _():
            add_line(t - lag)

        @pl.when(t == 2)
        def _():
            make_base()

        if quad:
            @pl.when(t == 0)
            def _():
                send_third()

            @pl.when(t == direct - direct // 4)
            def _():
                third_copy(0).wait_recv()
                pick(mine_count >= SLOTS, p3, top, 0)
                t_copy().wait_recv()
                pick(heavy, yt, top, 0)
                start_x(dv, direct, chunks)

    def n_copy(i):
        return remote(norm.at[0], nbuf.at[i - 1], n_s.at[i - 1], n_r.at[i - 1], ((me_r + i) % R, me_s))

    def m_copy(i):
        return remote(norm.at[1], sbuf.at[i - 1], m_s.at[i - 1], m_r.at[i - 1], (me_r, (me_s + i) % S))

    for i in range(1, R):
        n_copy(i).start()
    for i in range(1, O):
        by_copy(i).wait_recv()
        bf_copy(i).start()

    @pl.loop(0, chunks - 2)
    def _(c):
        forward(c)
        for j in range(Z):
            x_copy(deltas.at[0], c, j).wait_send()
        for j in range(Z - 1):
            z_copy(c, j).wait_send()

    total = norm[0]
    for i in range(1, R):
        n_copy(i).wait_recv()
        total = total + nbuf[i - 1]
    norm[1] = total
    for i in range(1, S):
        m_copy(i).start()

    @pl.loop(chunks - 2, chunks)
    def _(c):
        forward(c)

    for i in range(1, S):
        m_copy(i).wait_recv()
        total = total + sbuf[i - 1]
    tot[...] = total

    if quad:
        third_copy(0).wait_send()
        third_copy(1).wait_send()
        t_copy().wait_send()
    base_local().wait()
    base_twin().wait()
    for i in range(1, O):
        by_copy(i).wait_send()
        bf_copy(i).wait()
    for i in range(1, R):
        n_copy(i).wait_send()
    for i in range(1, S):
        m_copy(i).wait_send()

    @pl.loop(chunks - 2, chunks)
    def _(c):
        for j in range(Z):
            x_copy(deltas.at[0], c, j).wait_send()
        for j in range(Z - 1):
            z_copy(c, j).wait_send()

    @pl.loop(0, chunks)
    def _(c):
        l_copy(c).wait()
        c_copy(c).wait()
        for i in range(1, O):
            y_copy(i, c).wait_send()
            f_copy(i, c).wait()


def tree_kernel(
    R, S, rows, rc, first,
    owner_in, deltas, master, momentum,
    sums, bases, tot, ms, mm,
    owner, dv, p3, yt, b3, b3_in,
    xin, pair, zq, comb, zin, qb, combb, zinb, part_b, keep_b, xin_b, norm, total_row, nbuf,
    lo, ld, lm, p3_s, p3_r, t_s, t_r, x_s, x_r, xl_r, q_s, qa_r, qc_r, far_s, far_r,
    qb_s, qb_r, farb_s, farb_r, xb_s, xb_r,
    c_s, c_r, y_s, y_r, f_s, f_r,
    b3_s, b3_r, bc_s, bc_r, by_s, by_r, bf_s, bf_r, n_s, n_r, go,
):
    width = deltas.shape[2]
    cols = width // R
    Z = R // 2
    per = BLOCK_ROWS // rc
    half = BLOCK_ROWS // 2
    chunks = rows // rc
    whole = rows // BLOCK_ROWS
    direct = whole * per
    top = whole * BLOCK_ROWS
    mid_lag, line_lag = 2, 4
    steps = chunks - first
    late = chunks - direct
    last = max(line_lag, late)
    group = late
    me_r, me_s = lax.axis_index("replica"), lax.axis_index("shard")
    z, x = me_r // 2, me_r % 2
    o, core = me_s // 2, me_s % 2
    side = z // 2
    inner = (z + side) % 2
    outer = 1 - inner
    is_inner, is_outer = inner == 1, inner == 0
    x_peer = (z * 2 + 1 - x, me_s)
    near = ((side * 2 + 1 - z % 2) * 2 + x, me_s)
    far_outer = ((Z - 1) * (1 - side) * 2 + x, me_s)
    far_inner = ((Z - 1 - z) * 2 + x, me_s)
    twin = o * 2 + 1 - core
    twin_device = (me_r, twin)
    y_shard = (1 - o) * 2 + core
    y_device = (me_r, y_shard)

    barrier = pltpu.get_barrier_semaphore()
    me = me_r * S + me_s

    def peer(i):
        other = (me + i) % (R * S)
        return (other // S, other % S)

    def greet(device):
        pl.semaphore_signal(barrier, inc=1, device_id=device, device_id_type=pl.DeviceIdType.MESH)

    for device in (x_peer, near, twin_device, y_device):
        greet(device)

    @pl.when(is_inner)
    def _():
        greet(far_inner)

    def load(k):
        part = pl.ds(k * BLOCK_ROWS, BLOCK_ROWS)
        return pltpu.make_async_copy(deltas.at[0, part, :], dv.at[part, :], ld.at[k])

    load_owner = pltpu.make_async_copy(owner_in, owner, lo)
    load_owner.start()
    load_master = pltpu.make_async_copy(master, ms, lm.at[0])
    load_momentum = pltpu.make_async_copy(momentum, mm, lm.at[1])
    load_master.start()
    load_momentum.start()
    load(whole).start()
    for k in range(whole):
        load(k).start()
    norm[...] = jnp.zeros((8, 128), F32)
    pl.semaphore_wait(barrier, 4 + inner)

    @pl.when(is_inner)
    def _():
        pl.semaphore_signal(go, inc=1, device_id=far_inner, device_id_type=pl.DeviceIdType.MESH)

    mine, base = sums.at[me_s], bases.at[me_s]

    def rows_of(c):
        return pl.ds(pl.multiple_of(c * rc, rc), rc)

    def columns(k, side_x):
        e = (Z - 1 - k) if k < 2 else (outer if k == 2 else inner)
        d = e + side * (Z - 1 - 2 * e)
        return pl.ds(pl.multiple_of((d * 2 + side_x) * cols, cols), cols)

    def arrived(ref, sem):
        remote(ref, ref, n_s, sem, twin_device).wait_recv()

    def sent(ref, sem):
        remote(ref, ref, sem, n_r, twin_device).wait_send()

    def x_copy(source, c, k, sem):
        return remote(source.at[rows_of(c), columns(k, 1 - x)], xin.at[c, k], x_s, sem, x_peer)

    def start_q(c, k):
        if k == 2:
            remote(pair.at[c, k], zq.at[c, k], q_s, qc_r.at[c - first], near).start()
        else:
            @pl.when(is_outer)
            def _():
                remote(pair.at[c, k], zq.at[c, k], q_s, qa_r.at[c - first], near).start()

    def far_copy(c, i):
        return remote(comb.at[c, i], zin.at[c], far_s, far_r.at[c - first], far_inner if i else far_outer)

    def half_x(v):
        return x if v else 1 - x

    def start_qb(c):
        def start(v, k):
            remote(
                deltas.at[0, rows_of(c), columns(k, half_x(v))], qb.at[c, k, v], qb_s, qb_r.at[c, k // 2], near
            ).start()

        @pl.when(is_outer)
        def _():
            for k in range(2):
                for v in range(2):
                    start(v, k)

        for v in range(2):
            start(v, 2)

    def farb_copy(c, v, i):
        return remote(combb.at[c, v, i], zinb.at[c, v], farb_s, farb_r.at[c], far_inner if i else far_outer)

    def xb_copy(c):
        return remote(part_b.at[c], xin_b.at[c], xb_s, xb_r.at[c], x_peer)

    def c_copy(c):
        return remote(mine.at[c], sums.at[me_s, c], c_s, c_r, twin_device)

    def y_copy(c):
        return remote(mine.at[c], sums.at[me_s, c], y_s, y_r.at[c // group], y_device)

    def f_copy(g):
        part = sums.at[y_shard, pl.ds(g * group, group)]
        return remote(part, part, f_s, f_r, twin_device)

    def by_copy(i):
        part = pl.ds(i * BLOCK_ROWS, BLOCK_ROWS * (SLOTS - 2 if i else 1))
        return remote(base.at[part], bases.at[me_s, part], by_s.at[i], by_r.at[i], y_device)

    def bf_copy():
        return remote(bases.at[y_shard], bases.at[y_shard], bf_s, bf_r, twin_device)

    def b3_copy():
        return remote(b3, b3_in, b3_s, b3_r, twin_device)

    def base_twin():
        return remote(base, bases.at[me_s], bc_s, bc_r, twin_device)

    def third_copy(h):
        return remote(
            deltas.at[0, pl.ds((SLOTS - 1) * BLOCK_ROWS + h * half, half), :],
            p3.at[pl.ds(h * half, half), :], p3_s, p3_r.at[h], twin_device,
        )

    def t_copy():
        return remote(dv.at[pl.ds(top + half, half), :], yt, t_s, t_r, y_device)

    def start_x(low, high):
        @pl.loop(low, high)
        def _(c):
            for k in range(Z):
                x_copy(deltas.at[0], c, k, x_r.at[c - first]).start()

    def start_late(pieces):
        @pl.loop(direct, chunks)
        def _(c):
            for k in pieces:
                x_copy(dv, c, k, x_r.at[c - first] if k < 2 else xl_r.at[c - direct, k - 2]).start()

    def pick(condition, other, start, other_start):
        @pl.loop(0, half // 16)
        def _(r):
            keep = spread(condition, (16, 1024))
            for q in range(width // 1024):
                at = (pl.ds(pl.multiple_of(start + r * 16, 16), 16), pl.ds(q * 1024, 1024))
                there = (pl.ds(pl.multiple_of(other_start + r * 16, 16), 16), pl.ds(q * 1024, 1024))
                dv[at] = jnp.where(keep, dv[at].astype(F32), other[there].astype(F32)).astype(BF16)

    third_copy(1).start()
    start_x(first, first + 2)
    third_copy(0).start()
    start_qb(0)

    def send_third():
        load(whole).wait()
        third_copy(1).wait_recv()
        pick(mine_count >= SLOTS, p3, top + half, half)
        t_copy().start()

    def start_base(low, high, target, target_start):
        @pl.loop(low * BLOCK_ROWS // 16, high * BLOCK_ROWS // 16)
        def _(r):
            at = pl.ds(pl.multiple_of(r * 16, 16), 16)
            to = pl.ds(pl.multiple_of(r * 16 - target_start, 16), 16)
            target[to, :] = (ms[at, :] - 0.567 * mm[at, :]).astype(BF16)

    def make_base():
        start_base(SLOTS - 1, SLOTS, b3, (SLOTS - 1) * BLOCK_ROWS)
        b3_copy().start()
        start_base(1, SLOTS - 1, base, 0)

    def send_base():
        b3_copy().wait_recv()

        @pl.loop(0, BLOCK_ROWS // 16)
        def _(r):
            at = pl.ds(pl.multiple_of(top + r * 16, 16), 16)
            there = pl.ds(pl.multiple_of(r * 16, 16), 16)
            keep = spread(mine_count >= SLOTS, (16, cols))
            base[at, :] = jnp.where(keep, base[at, :].astype(F32), b3_in[there, :].astype(F32)).astype(BF16)

        by_copy(1).start()
        base_twin().start()

    def ready():
        @pl.loop(0, SLOTS * per)
        def _(r):
            at = pl.ds(pl.multiple_of(r * rc, rc), rc)
            old, before = ms[at, :], mm[at, :]
            live = spread(r // per < mine_count, old.shape)
            ms[at, :] = jnp.where(live, old - 0.567 * before, old)
            mm[at, :] = jnp.where(live, 0.9 * before, before)

    def add_pair(c, pieces):
        for k in pieces:
            pair[c, k] = (xin[c, k].astype(F32) + dv[rows_of(c), columns(k, x)].astype(F32)).astype(BF16)
            if k < Z - 1:
                start_q(c, k)

    def add_mid(c):
        arrived(zq.at[c, pl.ds(0, 2)], qa_r.at[c - first])
        for i in range(2):
            comb[c, i] = (pair[c, i].astype(F32) + zq[c, i].astype(F32)).astype(BF16)
            far_copy(c, i).start()

    def add_mid_b(c):
        arrived(qb.at[c, pl.ds(0, 2)], qb_r.at[c, 0])
        for v in range(2):
            for i in range(2):
                own = dv[rows_of(c), columns(i, half_x(v))].astype(F32)
                combb[c, v, i] = (own + qb[c, i, v].astype(F32)).astype(BF16)
                farb_copy(c, v, i).start()

    def add_line_b(c):
        arrived(qb.at[c, 2], qb_r.at[c, 1])
        arrived(zinb.at[c], farb_r.at[c])
        for v in range(2):
            own = dv[rows_of(c), columns(Z - 1, half_x(v))].astype(F32)
            value = own + qb[c, 2, v].astype(F32) + zinb[c, v].astype(F32)
            if v:
                keep_b[c] = value
            else:
                part_b[c] = value.astype(BF16)

    def emit(c, get):
        place = jnp.where(c >= direct, -1, c // per)
        live = spread(place < mine_count, (8, 128))
        part = jnp.zeros((8, 128), F32)
        for r in range(0, rc, 16):
            total = get(r) / R
            mine[c, r:r + 16, :] = total.astype(BF16)
            for h in range(0, 16, 8):
                for q in range(0, cols, 128):
                    v = total[h:h + 8, q:q + 128]
                    part = part + v * v
        norm[...] = norm[...] + jnp.where(live, part, 0.0)
        y_copy(c).start()
        c_copy(c).start()

    def add_line(c):
        arrived(zq.at[c, 2], qc_r.at[c - first])
        arrived(zin.at[c], far_r.at[c - first])
        emit(c, lambda r: (
            pair[c, Z - 1, r:r + 16, :].astype(F32) + zq[c, 2, r:r + 16, :].astype(F32)
            + zin[c, r:r + 16, :].astype(F32)
        ))

    def add_last_b(c):
        xb_copy(c).wait_recv()
        emit(c, lambda r: keep_b[c, r:r + 16, :] + xin_b[c, r:r + 16, :].astype(F32))

    def forward(g):
        arrived(sums.at[y_shard, pl.ds(g * group, group)], y_r.at[g])
        f_copy(g).start()

    load_owner.wait()
    mine_count = jnp.sum(jnp.where(owner[...] == me_s, 1, 0), axis=1, keepdims=True)
    twin_count = jnp.sum(jnp.where(owner[...] == twin, 1, 0), axis=1, keepdims=True)
    heavy = jnp.maximum(mine_count, twin_count) >= SLOTS
    load_master.wait()
    load_momentum.wait()
    start_base(0, 1, base, 0)
    by_copy(0).start()

    @pl.loop(1, first)
    def _(c):
        start_qb(c)

    start_x(first + 2, direct)
    make_base()
    send_third()
    send_base()
    load(0).wait()

    quad_at = (direct - first) * 5 // 7

    @pl.when(is_inner)
    def _():
        pl.semaphore_wait(go, 1)

    @pl.loop(0, steps)
    def _(t):
        c = first + t

        @pl.when(jnp.logical_and(c % per == 0, c < direct))
        def _():
            load(c // per).wait()

        @pl.when(c < direct)
        def _():
            arrived(xin.at[c], x_r.at[c - first])
            add_pair(c, range(Z))

        @pl.when(c >= direct)
        def _():
            arrived(xin.at[c, pl.ds(0, 2)], x_r.at[c - first])
            add_pair(c, range(2))

        @pl.when(jnp.logical_and(is_inner, t < first))
        def _():
            add_mid_b(t)

        @pl.when(jnp.logical_and(t >= 2, t < 2 + first))
        def _():
            add_line_b(t - 2)

        @pl.when(jnp.logical_and(is_inner, t >= mid_lag))
        def _():
            add_mid(first + t - mid_lag)

        @pl.when(jnp.logical_and(t >= line_lag, t - line_lag < steps - last))
        def _():
            add_line(first + t - line_lag)

        @pl.when(t == quad_at - 2)
        def _():
            ready()

        @pl.when(t == quad_at)
        def _():
            third_copy(0).wait_recv()
            pick(mine_count >= SLOTS, p3, top, 0)
            t_copy().wait_recv()
            pick(heavy, yt, top, 0)
            for pieces in ((0, 1), (2,), (3,)):
                start_late(pieces)

            @pl.loop(0, first)
            def _(c):
                xb_copy(c).start()

    @pl.loop(direct, chunks)
    def _(c):
        arrived(xin.at[c, 2], xl_r.at[c - direct, 0])
        add_pair(c, (2,))

    @pl.when(is_inner)
    def _():
        @pl.loop(chunks - mid_lag, chunks)
        def _(c):
            add_mid(c)

    @pl.loop(direct, chunks)
    def _(c):
        arrived(xin.at[c, 3], xl_r.at[c - direct, 1])
        add_pair(c, (3,))

    @pl.loop(chunks - last, chunks - 1)
    def _(c):
        add_line(c)

    @pl.loop(0, first)
    def _(c):
        add_last_b(c)

    add_line(chunks - 1)

    total_row[...] = jnp.sum(norm[...], axis=0, keepdims=True)

    def n_copy(i):
        return remote(total_row, nbuf.at[i - 1], n_s, n_r, peer(i))

    for i in range(1, R * S):
        n_copy(i).start()
    by_copy(0).wait_recv()
    by_copy(1).wait_recv()
    bf_copy().start()

    @pl.loop(1, chunks // group)
    def _(g):
        forward(g % (chunks // group - 1))

    forward(chunks // group - 1)

    sent(p3, p3_s)
    t_copy().wait_send()
    b3_copy().wait_send()
    base_twin().wait()
    ours = pl.ds(first, steps)
    sent(xin.at[ours], x_s)
    sent(xin_b, xb_s)

    @pl.when(is_outer)
    def _():
        sent(zq.at[ours], q_s)
        sent(qb, qb_s)

    @pl.when(is_inner)
    def _():
        sent(zin.at[ours], q_s)
        sent(zinb, qb_s)
        sent(comb.at[ours], far_s)
        sent(combb, farb_s)

    sent(mine, c_s)
    sent(mine, y_s)
    sent(mine, f_s)
    arrived(sums.at[twin], c_r)
    arrived(mine, f_r)
    by_copy(0).wait_send()
    by_copy(1).wait_send()
    bf_copy().wait()
    arrived(nbuf, n_r)
    sent(nbuf, n_s)
    total = total_row[...]
    for i in range(1, R * S):
        total = total + nbuf[i - 1]
    tot[...] = jnp.broadcast_to(total, (8, 128)) * jnp.where(
        lax.broadcasted_iota(jnp.int32, (8, 128), 0) == 0, 1.0, 0.0
    )


def finish_kernel(
    R, units,
    owner_in, tot, master, momentum, sums, bases,
    master_out, momentum_out, params,
    owner, owner_s, ms, mm, su, pb, ps,
    a_s, b_s, u_s, p_s, q_s, oa_s, ob_s, op_s,
):
    blocks = owner.shape[1]
    cols = master.shape[1]
    half = BLOCK_ROWS // 2
    me_s = lax.axis_index("shard")
    get_owner = pltpu.make_async_copy(owner_in, owner, owner_s)
    get_owner.start()

    def unit(shard, place, h):
        if units == 2 * SLOTS:
            return shard * units + 2 * place + h
        moved = shard + jnp.where(place == SLOTS - 1, 1 - 2 * (shard % 2), 0)
        if h:
            moved = moved + jnp.where(moved // 2 == 0, 2, -2)
        return jnp.where(place < 2, shard * units + 2 * place + h, moved * units + units - 1)

    def slot_rows(j):
        return pl.ds(pl.multiple_of(j * BLOCK_ROWS, BLOCK_ROWS), BLOCK_ROWS)

    def get_slot(j):
        return [
            pltpu.make_async_copy(master.at[slot_rows(j)], ms.at[slot_rows(j)], a_s.at[j]),
            pltpu.make_async_copy(momentum.at[slot_rows(j)], mm.at[slot_rows(j)], b_s.at[j]),
        ] + [
            pltpu.make_async_copy(sums.at[unit(me_s, j, h)], su.at[2 * j + h], u_s.at[2 * j + h]) for h in range(2)
        ]

    def put_slot(j):
        return [
            pltpu.make_async_copy(ms.at[slot_rows(j)], master_out.at[slot_rows(j)], oa_s.at[j]),
            pltpu.make_async_copy(mm.at[slot_rows(j)], momentum_out.at[slot_rows(j)], ob_s.at[j]),
        ]

    def get_block(b):
        shard = owner[0, b]
        place = sum(jnp.where(jnp.logical_and(owner[0, k] == shard, k < b), 1, 0) for k in range(blocks))
        return [pltpu.make_async_copy(bases.at[shard * SLOTS + place], pb.at[b], p_s.at[b])] + [
            pltpu.make_async_copy(sums.at[unit(shard, place, h)], ps.at[2 * b + h], q_s.at[2 * b + h])
            for h in range(2)
        ]

    def put_block(b):
        return pltpu.make_async_copy(pb.at[b], params.at[slot_rows(b)], op_s.at[b])

    @pl.loop(0, SLOTS)
    def _(j):
        for copy in get_slot(j):
            copy.start()

    get_owner.wait()
    count = shard_count(owner, me_s)

    @pl.loop(0, blocks)
    def _(b):
        for copy in get_block(b):
            copy.start()

    total = jnp.sum(jnp.sum(tot[...], axis=1, keepdims=True), axis=0, keepdims=True)
    limit = 0.5 * jnp.sqrt(jnp.full((1, 1), blocks * BLOCK_ROWS * R * cols, F32))
    factor = jnp.minimum(1.0, limit / (jnp.sqrt(total) + 1e-06))

    @pl.loop(0, SLOTS)
    def _(j):
        for copy in get_slot(j):
            copy.wait()

        @pl.when(j < count)
        def _():
            for h in range(2):
                @pl.loop(0, half // 16)
                def _(r):
                    at = pl.ds(pl.multiple_of(j * BLOCK_ROWS + h * half + r * 16, 16), 16)
                    grad = factor * su[2 * j + h, pl.ds(pl.multiple_of(r * 16, 16), 16), :].astype(F32)
                    fresh = 0.9 * mm[at, :] + grad
                    mm[at, :] = fresh
                    ms[at, :] = ms[at, :] - 0.7 * (grad + 0.9 * fresh)

        for copy in put_slot(j):
            copy.start()

    @pl.loop(0, blocks)
    def _(b):
        for copy in get_block(b):
            copy.wait()
        for h in range(2):
            @pl.loop(0, half // 16)
            def _(r):
                at = pl.ds(pl.multiple_of(h * half + r * 16, 16), 16)
                grad = factor * ps[2 * b + h, pl.ds(pl.multiple_of(r * 16, 16), 16), :].astype(F32)
                pb[b, at, :] = (pb[b, at, :].astype(F32) - 1.33 * grad).astype(BF16)

        put_block(b).start()

    @pl.loop(0, SLOTS)
    def _(j):
        for copy in put_slot(j):
            copy.wait()

    @pl.loop(0, blocks)
    def _(b):
        put_block(b).wait()


def close_kernel(
    R, units, held,
    owner_in, tot, master, momentum, sums, bases,
    master_out, momentum_out, params,
    owner, ms, mm, pb, owner_s, a_s, b_s, p_s,
):
    blocks = owner.shape[1]
    cols = master.shape[1]
    half = BLOCK_ROWS // 2
    me_s = lax.axis_index("shard")
    get_owner = pltpu.make_async_copy(owner_in, owner, owner_s)
    get_owner.start()

    def unit(shard, place, h):
        moved = shard + jnp.where(place == SLOTS - 1, 1 - 2 * (shard % 2), 0)
        if h:
            moved = moved + jnp.where(moved // 2 == 0, 2, -2)
        return jnp.where(place < 2, shard * units + 2 * place + h, moved * units + units - 1)

    def slot_rows(j):
        return pl.ds(pl.multiple_of(j * BLOCK_ROWS, BLOCK_ROWS), BLOCK_ROWS)

    def put_slot(j):
        return [
            pltpu.make_async_copy(ms.at[slot_rows(j)], master_out.at[slot_rows(j)], a_s.at[j]),
            pltpu.make_async_copy(mm.at[slot_rows(j)], momentum_out.at[slot_rows(j)], b_s.at[j]),
        ]

    def put_block(b):
        return pltpu.make_async_copy(pb.at[b], params.at[slot_rows(b)], p_s.at[b])

    total = jnp.sum(jnp.sum(tot[...], axis=1, keepdims=True), axis=0, keepdims=True)
    limit = 0.5 * jnp.sqrt(jnp.full((1, 1), blocks * BLOCK_ROWS * R * cols, F32))
    factor = jnp.minimum(1.0, limit / (jnp.sqrt(total) + 1e-06))
    count = jnp.sum(jnp.where(owner_in[...] == me_s, 1, 0), axis=1, keepdims=True)

    @pl.loop(0, SLOTS)
    def _(j):
        for h in range(2):
            source = unit(me_s, j, h)

            @pl.loop(0, half // 16, unroll=4)
            def _(r):
                at = pl.ds(pl.multiple_of(j * BLOCK_ROWS + h * half + r * 16, 16), 16)
                part = factor * sums[source, pl.ds(pl.multiple_of(r * 16, 16), 16), :].astype(F32)
                grad = jnp.where(spread(j < count, part.shape), part, 0.0)
                mm[at, :] = momentum[at, :] + grad
                ms[at, :] = master[at, :] - 1.33 * grad

        for copy in put_slot(j):
            copy.start()

    get_owner.wait()

    @pl.loop(0, blocks)
    def _(b):
        shard = owner[0, b]
        place = sum(jnp.where(jnp.logical_and(owner[0, k] == shard, k < b), 1, 0) for k in range(blocks))
        kept = jnp.where(place < held, shard * held + place, (shard + 1 - 2 * (shard % 2)) * held + held - 1)
        for h in range(2):
            source = unit(shard, place, h)

            @pl.loop(0, half // 16, unroll=4)
            def _(r):
                at = pl.ds(pl.multiple_of(h * half + r * 16, 16), 16)
                grad = factor * sums[source, pl.ds(pl.multiple_of(r * 16, 16), 16), :].astype(F32)
                pb[b, at, :] = (bases[kept, at, :].astype(F32) - 1.33 * grad).astype(BF16)

        put_block(b).start()

    @pl.loop(0, SLOTS)
    def _(j):
        for copy in put_slot(j):
            copy.wait()

    @pl.loop(0, blocks)
    def _(b):
        put_block(b).wait()


def on_device(deltas, master, momentum, block_owner):
    R, S = lax.axis_size("replica"), lax.axis_size("shard")
    width, cols = deltas.shape[2], master.shape[1]
    blocks = block_owner.shape[0]
    block_owner = block_owner.reshape(1, blocks)
    half = BLOCK_ROWS // 2
    quad = S == 4 and blocks - SLOTS - (S - 2) <= 2
    rows = 2 * BLOCK_ROWS + half if quad else SLOTS * BLOCK_ROWS
    rc = half
    while rc > 16 and (rows // (rc // 2)) * R <= 160:
        rc //= 2
    chunks = rows // rc
    units = rows // half
    Z, O = R // 2, S // 2
    loads = rows // BLOCK_ROWS + (1 if quad else 0)

    dma = pltpu.SemaphoreType.DMA
    vmem = pltpu.VMEM
    anywhere = pl.BlockSpec(memory_space=pl.ANY)
    in_vmem = pl.BlockSpec(memory_space=pltpu.VMEM)
    in_hbm = pl.BlockSpec(memory_space=pltpu.HBM)
    in_smem = pl.BlockSpec(memory_space=pltpu.SMEM)
    tree = quad and Z == 4 and O == 2
    if tree:
        held = SLOTS - 1
        first = chunks * 3 // 20
        steps = chunks - first
        piece = (rc, cols)
        sums, bases, tot, ms, mm = pl.pallas_call(
            functools.partial(tree_kernel, R, S, rows, rc, first),
            out_shape=(
                jax.ShapeDtypeStruct((S, chunks, rc, cols), BF16),
                jax.ShapeDtypeStruct((S, held * BLOCK_ROWS, cols), BF16),
                jax.ShapeDtypeStruct((8, 128), F32),
                jax.ShapeDtypeStruct(master.shape, F32),
                jax.ShapeDtypeStruct(master.shape, F32),
            ),
            in_specs=[in_hbm] * 4,
            out_specs=(in_vmem,) * 5,
            scratch_shapes=[
                vmem(block_owner.shape, jnp.int32),
                vmem((loads * BLOCK_ROWS, width), BF16),
                vmem((BLOCK_ROWS, width), BF16),
                vmem((half, width), BF16),
                vmem((BLOCK_ROWS, cols), BF16),
                vmem((BLOCK_ROWS, cols), BF16),
                vmem((chunks, Z) + piece, BF16),
                vmem((chunks, Z) + piece, BF16),
                vmem((chunks, 3) + piece, BF16),
                vmem((chunks, 2) + piece, BF16),
                vmem((chunks,) + piece, BF16),
                vmem((first, 3, 2) + piece, BF16),
                vmem((first, 2, 2) + piece, BF16),
                vmem((first, 2) + piece, BF16),
                vmem((first,) + piece, BF16),
                vmem((first,) + piece, F32),
                vmem((first,) + piece, BF16),
                vmem((8, 128), F32),
                vmem((1, 128), F32),
                vmem((R * S - 1, 1, 128), F32),
                dma, dma((loads,)), dma((2,)), dma, dma((2,)), dma, dma,
                dma, dma((steps,)), dma((half // rc, 2)), dma, dma((steps,)), dma((steps,)), dma, dma((steps,)),
                dma, dma((first, 2)), dma, dma((first,)), dma, dma((first,)),
                dma, dma, dma, dma((chunks * rc // half,)), dma, dma,
                dma, dma, dma, dma, dma((2,)), dma((2,)), dma, dma, dma, dma,
                pltpu.SemaphoreType.REGULAR,
            ],
            compiler_params=pltpu.CompilerParams(
                collective_id=0, has_side_effects=True, vmem_limit_bytes=SYNC_VMEM
            ),
            name="sync",
        )(*(pltpu.with_memory_space_constraint(a, pltpu.HBM) for a in (block_owner, deltas, master, momentum)))
        return tuple(pl.pallas_call(
            functools.partial(close_kernel, R, units, held),
            out_shape=(
                jax.ShapeDtypeStruct(master.shape, F32),
                jax.ShapeDtypeStruct(master.shape, F32),
                jax.ShapeDtypeStruct((blocks * BLOCK_ROWS, cols), BF16),
            ),
            in_specs=[in_vmem] * 6,
            out_specs=(in_hbm,) * 3,
            scratch_shapes=[
                pltpu.SMEM((1, blocks), jnp.int32),
                vmem(master.shape, F32),
                vmem(master.shape, F32),
                vmem((blocks, BLOCK_ROWS, cols), BF16),
                dma, dma((SLOTS,)), dma((SLOTS,)), dma((blocks,)),
            ],
            compiler_params=pltpu.CompilerParams(vmem_limit_bytes=CLOSE_VMEM),
            name="close",
        )(block_owner, tot, ms, mm, sums.reshape(S * units, half, cols),
          bases.reshape(S * held, BLOCK_ROWS, cols)))

    ys, zs = max(O - 1, 1), max(Z - 1, 1)
    sums, bases, tot = pl.pallas_call(
        functools.partial(sync_kernel, R, S, rows, rc),
        out_shape=(
            jax.ShapeDtypeStruct((S, chunks, rc, cols), BF16),
            jax.ShapeDtypeStruct((S,) + master.shape, BF16),
            jax.ShapeDtypeStruct((8, 128), F32),
        ),
        in_specs=[in_vmem, anywhere, anywhere, anywhere],
        out_specs=(anywhere, anywhere, in_vmem),
        scratch_shapes=[
            vmem((loads * BLOCK_ROWS, width), BF16),
            vmem((BLOCK_ROWS, width) if quad else (16, 128), BF16),
            vmem((half, width) if quad else (16, 128), BF16),
            vmem(master.shape, F32),
            vmem(master.shape, F32),
            vmem(master.shape, BF16),
            vmem((chunks, Z, rc, cols), BF16),
            vmem((chunks, Z, rc, cols), BF16),
            vmem((chunks, zs, rc, cols), BF16),
            vmem((chunks, rc, cols), BF16),
            vmem((2, 8, 128), F32),
            vmem((R - 1, 8, 128), F32),
            vmem((S - 1, 8, 128), F32),
            dma((loads,)), dma((2,)), dma((2,)), dma((2,)), dma, dma,
            dma((chunks, Z)), dma((chunks, Z)),
            dma((chunks, zs)), dma((chunks, zs)),
            dma((chunks,)), dma((chunks,)), dma((chunks,)),
            dma((ys, chunks)), dma((ys, chunks)), dma((ys, chunks)), dma((ys, chunks)),
            dma, dma, dma,
            dma((ys,)), dma((ys,)), dma((ys,)), dma((ys,)),
            dma((R - 1,)), dma((R - 1,)), dma((S - 1,)), dma((S - 1,)),
        ],
        compiler_params=pltpu.CompilerParams(
            collective_id=0, has_side_effects=True, vmem_limit_bytes=VMEM_LIMIT
        ),
        name="sync",
    )(block_owner, deltas, master, momentum)

    return tuple(pl.pallas_call(
        functools.partial(finish_kernel, R, units),
        out_shape=(
            jax.ShapeDtypeStruct(master.shape, F32),
            jax.ShapeDtypeStruct(master.shape, F32),
            jax.ShapeDtypeStruct((blocks * BLOCK_ROWS, cols), BF16),
        ),
        in_specs=[in_vmem, in_vmem] + [anywhere] * 4,
        out_specs=(anywhere,) * 3,
        scratch_shapes=[
            pltpu.SMEM((1, blocks), jnp.int32), dma,
            vmem(master.shape, F32),
            vmem(master.shape, F32),
            vmem((2 * SLOTS, half, cols), BF16),
            vmem((blocks, BLOCK_ROWS, cols), BF16),
            vmem((2 * blocks, half, cols), BF16),
            dma((SLOTS,)), dma((SLOTS,)), dma((2 * SLOTS,)), dma((blocks,)), dma((2 * blocks,)),
            dma((SLOTS,)), dma((SLOTS,)), dma((blocks,)),
        ],
        compiler_params=pltpu.CompilerParams(vmem_limit_bytes=VMEM_LIMIT),
        name="finish",
    )(block_owner, tot, master, momentum, sums.reshape(S * units, half, cols),
      bases.reshape(S * SLOTS, BLOCK_ROWS, cols)))


def solution(mesh):
    return jax.shard_map(
        on_device,
        mesh=mesh,
        in_specs=(P("replica", "shard", None), P("shard", "replica"), P("shard", "replica"), P()),
        out_specs=(P("shard", "replica"), P("shard", "replica"), P(None, "replica")),
        check_vma=False,
    )
```
